16 devices in a mesh: dp: 16 (over z, y, x, core).
Axes of the slice: x: 2, y: 2, z: 2, core: 2. Of those that a mesh axis runs over, the one named last changes fastest.
Arguments:
- g_mat: bfloat16 [16, 25165824], P('dp')
- g_vec: bfloat16 [16, 26624], P('dp')
- p_mat: float32 [25165824], P('dp')
- m_mat: float32 [25165824], P('dp')
- v_mat: float32 [25165824], P('dp')
- p_vec: float32 [26624], replicated
- m_vec: float32 [26624], replicated
- v_vec: float32 [26624], replicated
- learn_rate: float32 [], replicated
Outputs:
- output 1: float32 [25165824], P('dp')
- output 2: float32 [25165824], P('dp')
- output 3: float32 [25165824], P('dp')
- output 4: float32 [26624], replicated
- output 5: float32 [26624], replicated
- output 6: float32 [26624], replicated
- output 7: bfloat16 [25165824], replicated
All inputs are finite; a program needn't handle non-finite values.
Results may differ from the reference program's by a relative error of at most 0.001.
Values are sent between devices in bfloat16 or wider.
A program may use at most 1 GiB of HBM per device.

```python
import jax
import jax.numpy as jnp
from jax import lax

D = 1024
FF = 4096
TP = 1
DP = 16
STEP = 10

N_MAT = (8 * D * D + 4 * D * FF) // TP
N_VEC = 2 * ((3 * D + FF) // TP) + 12 * D
N_ALL = N_MAT + N_VEC
ELEM_SCALE = N_ALL ** -0.5
NOISE_GAIN = 6.0 * DP ** 0.5
ADAM_BETA1 = 0.9
ADAM_BETA2 = 0.98
ADAM_EPS = 1e-8
WEIGHT_DECAY = 0.01
MAX_NORM = 1.0
NORM_EPS = 1e-6
BIAS_ONE = 1.0 - ADAM_BETA1 ** STEP
BIAS_TWO = 1.0 - ADAM_BETA2 ** STEP


def draw_local_grads(draw_key, elem_count):
    key_base, key_dev = jax.random.split(draw_key)
    base_part = 2.0 * jax.random.normal(key_base, (elem_count,), jnp.float32)
    dev_keys = jax.random.split(key_dev, DP)

    def one_device(dev_key):
        noise_part = jax.random.normal(dev_key, (elem_count,), jnp.float32)
        return ((base_part + NOISE_GAIN * noise_part) * ELEM_SCALE).astype(jnp.bfloat16)

    return lax.map(one_device, dev_keys)


def setup_inputs(seed: int = 0) -> dict:
    key_list = jax.random.split(jax.random.key(seed), 9)
    return dict(
        g_mat=draw_local_grads(key_list[0], N_MAT),
        g_vec=draw_local_grads(key_list[1], N_VEC),
        p_mat=0.02 * jax.random.normal(key_list[2], (N_MAT,), jnp.float32),
        m_mat=0.1 * ELEM_SCALE * jax.random.normal(key_list[3], (N_MAT,), jnp.float32),
        v_mat=0.05 * ELEM_SCALE * ELEM_SCALE * jax.random.uniform(key_list[4], (N_MAT,), jnp.float32, minval=0.25, maxval=1.75),
        p_vec=0.05 * jax.random.normal(key_list[5], (N_VEC,), jnp.float32),
        m_vec=0.1 * ELEM_SCALE * jax.random.normal(key_list[6], (N_VEC,), jnp.float32),
        v_vec=0.05 * ELEM_SCALE * ELEM_SCALE * jax.random.uniform(key_list[7], (N_VEC,), jnp.float32, minval=0.25, maxval=1.75),
        learn_rate=jax.random.uniform(key_list[8], (), jnp.float32, minval=0.002, maxval=0.008),
    )


def mean_over_devices(local_grads):
    def add_row(acc_sum, grad_row):
        return acc_sum + grad_row.astype(jnp.float32), None

    total_sum, _ = lax.scan(add_row, jnp.zeros(local_grads.shape[1:], jnp.float32), local_grads)
    return total_sum / local_grads.shape[0]


def adam_update(grad_vals, param_vals, moment_one, moment_two, learn_rate, decay_rate):
    new_one = ADAM_BETA1 * moment_one + (1.0 - ADAM_BETA1) * grad_vals
    new_two = ADAM_BETA2 * moment_two + (1.0 - ADAM_BETA2) * grad_vals * grad_vals
    direction = (new_one / BIAS_ONE) / (jnp.sqrt(new_two / BIAS_TWO) + ADAM_EPS)
    return param_vals - learn_rate * (direction + decay_rate * param_vals), new_one, new_two


def reference(g_mat, g_vec, p_mat, m_mat, v_mat, p_vec, m_vec, v_vec, learn_rate):
    grad_mat = mean_over_devices(g_mat)
    grad_vec = mean_over_devices(g_vec)
    norm_sq = jnp.sum(grad_mat * grad_mat) + jnp.sum(grad_vec * grad_vec)
    clip_scale = jnp.minimum(1.0, MAX_NORM / (jnp.sqrt(norm_sq) + NORM_EPS))
    new_p_mat, new_m_mat, new_v_mat = adam_update(grad_mat * clip_scale, p_mat, m_mat, v_mat, learn_rate, WEIGHT_DECAY)
    new_p_vec, new_m_vec, new_v_vec = adam_update(grad_vec * clip_scale, p_vec, m_vec, v_vec, learn_rate, 0.0)
    return (new_p_mat, new_m_mat, new_v_mat, new_p_vec, new_m_vec, new_v_vec, new_p_mat.astype(jnp.bfloat16))
```

```python
import functools

import jax
import jax.numpy as jnp
from jax import lax
from jax.experimental import pallas as pl
from jax.experimental.pallas import tpu as pltpu
from jax.sharding import PartitionSpec as P

STEP = 10
ADAM_BETA1 = 0.9
ADAM_BETA2 = 0.98
ADAM_EPS = 1e-8
WEIGHT_DECAY = 0.01
MAX_NORM = 1.0
NORM_EPS = 1e-6
BIAS_ONE = 1.0 - ADAM_BETA1 ** STEP
BIAS_TWO = 1.0 - ADAM_BETA2 ** STEP

MESH_ID = pl.DeviceIdType.MESH
COLORS = 3
PARTS = 4
STRIDES = (2, 4, 8)
STEPS = 8 * PARTS


def adam_update(grad_vals, param_vals, moment_one, moment_two, learn_rate, decay_rate):
    new_one = ADAM_BETA1 * moment_one + (1.0 - ADAM_BETA1) * grad_vals
    new_two = ADAM_BETA2 * moment_two + (1.0 - ADAM_BETA2) * grad_vals * grad_vals
    direction = (new_one / BIAS_ONE) / (jnp.sqrt(new_two / BIAS_TWO) + ADAM_EPS)
    return param_vals - learn_rate * (direction + decay_rate * param_vals), new_one, new_two


def scatter_kernel(axis_name, piece, g, out, pg, a_buf, b_buf, stage, r1, r2, r3,
                   a_sem, b_sem, ds_sem, dr_sem, s1_sem, r1_sem, s2_sem, r2_sem, s3_sem, r3_sem, o_sem):
    chunk = piece // (COLORS * PARTS)
    me = lax.axis_index(axis_name)
    core_step = 1 - 2 * lax.rem(me, 2)
    deltas = [s * (1 - 2 * lax.rem(me // s, 2)) for s in STRIDES]
    partner = me + core_step
    peers = [me + d for d in deltas]

    barrier = pltpu.get_barrier_semaphore()
    for dev in (partner, *peers):
        pl.semaphore_signal(barrier, inc=1, device_id=(dev,), device_id_type=MESH_ID)

    def offset(color, t):
        unit = t // PARTS
        f1 = 1 - unit // 4
        f2 = 1 - lax.rem(unit // 2, 2)
        f3 = 1 - lax.rem(unit, 2)
        d1, d2, d3 = (deltas[(color + k) % 3] for k in range(3))
        owner = me + f1 * d1 + f2 * d2 + f3 * d3
        return owner * piece + (color * PARTS + lax.rem(t, PARTS)) * chunk

    def cut(ref, start):
        return ref.at[:, pl.ds(pl.multiple_of(start, 1024), chunk)]

    def swap(color, t):
        return pltpu.make_async_remote_copy(
            src_ref=cut(g, offset(color, t) + core_step * piece),
            dst_ref=cut(pg, (color * STEPS + t) * chunk),
            send_sem=ds_sem.at[color * 4 + lax.rem(t, 4)],
            recv_sem=dr_sem.at[color * STEPS + t],
            device_id=(partner,), device_id_type=MESH_ID)

    def load_a(color, t):
        k = color * 2 + lax.rem(t, 2)
        return pltpu.make_async_copy(cut(g, offset(color, t)), a_buf.at[k], a_sem.at[k])

    def load_b(color, t):
        k = color * 2 + lax.rem(t, 2)
        return pltpu.make_async_copy(cut(pg, (color * STEPS + t) * chunk), b_buf.at[k], b_sem.at[k])

    def push(src, dst, send_sem, recv_sem, axis):
        return pltpu.make_async_remote_copy(
            src_ref=src, dst_ref=dst, send_sem=send_sem, recv_sem=recv_sem,
            device_id=(peers[axis],), device_id_type=MESH_ID)

    def push1(color, t):
        k = color * 3 + lax.rem(t, 3)
        j = color * 4 * PARTS + t
        return push(stage.at[k], r1.at[j], s1_sem.at[k], r1_sem.at[j], color)

    def push2(color, t):
        j = color * 2 * PARTS + t - 4 * PARTS
        return push(r1.at[color * 4 * PARTS + t - 4 * PARTS], r2.at[j], s2_sem.at[j], r2_sem.at[j], (color + 1) % 3)

    def push3(color, t):
        j = color * PARTS + t - 6 * PARTS
        return push(r1.at[color * 4 * PARTS + t - 4 * PARTS], r3.at[j], s3_sem.at[j], r3_sem.at[j], (color + 2) % 3)

    def store(color, t):
        j = color * PARTS + t - 7 * PARTS
        return pltpu.make_async_copy(r3.at[j], cut(out, j * chunk), o_sem.at[j])

    def add_up(color, t, dst, extra):
        k = color * 2 + lax.rem(t, 2)
        width = min(chunk, 4096)

        @pl.loop(0, chunk // width)
        def _(i):
            s = pl.ds(pl.multiple_of(i * width, width), width)
            acc = a_buf[k, :, s].astype(jnp.float32) + b_buf[k, :, s].astype(jnp.float32)
            for ref, j in extra:
                acc = acc + ref[j, :, s]
            dst[0][dst[1], :, s] = acc

    def ready(color, t):
        load_a(color, t).wait()
        load_b(color, t).wait()

    def refill(color, t):
        load_a(color, t).start()
        swap(color, t).wait_recv()
        load_b(color, t).start()

    def more_swap(color, t):
        swap(color, t - 4).wait_send()
        swap(color, t).start()

    for t in range(2):
        for color in range(COLORS):
            load_a(color, t).start()
    pl.semaphore_wait(barrier, 4)
    for t in range(4):
        for color in range(COLORS):
            swap(color, t).start()
    for t in range(2):
        for color in range(COLORS):
            swap(color, t).wait_recv()
            load_b(color, t).start()

    def phase_one(t, first):
        for color in range(COLORS):
            ready(color, t)
            if not first:
                push1(color, t - 3).wait_send()
            add_up(color, t, (stage, color * 3 + lax.rem(t, 3)), ())
            push1(color, t).start()
            more_swap(color, t + 4)
            refill(color, t + 2)

    def run(lo, hi, body):
        lax.fori_loop(lo, hi, lambda t, c: (body(t), c)[1], 0)

    run(0, 3, lambda t: phase_one(t, True))
    run(3, 4 * PARTS, lambda t: phase_one(t, False))

    def phase_two(t):
        for color in range(COLORS):
            ready(color, t)
            j = color * 4 * PARTS + t - 4 * PARTS
            push1(color, t - 4 * PARTS).wait_recv()
            add_up(color, t, (r1, j), ((r1, j),))
            push2(color, t).start()
            more_swap(color, t + 4)
            refill(color, t + 2)

    run(4 * PARTS, 6 * PARTS, phase_two)

    def phase_three(t):
        for color in range(COLORS):
            ready(color, t)
            j = color * 4 * PARTS + t - 4 * PARTS
            push1(color, t - 4 * PARTS).wait_recv()
            push2(color, t - 2 * PARTS).wait_recv()
            add_up(color, t, (r1, j), ((r1, j), (r2, color * 2 * PARTS + t - 6 * PARTS)))
            push3(color, t).start()
            more_swap(color, t + 4)
            refill(color, t + 2)

    run(6 * PARTS, 7 * PARTS, phase_three)

    def phase_four(t, fill):
        for color in range(COLORS):
            ready(color, t)
            push1(color, t - 4 * PARTS).wait_recv()
            push2(color, t - 2 * PARTS).wait_recv()
            push3(color, t - PARTS).wait_recv()
            add_up(color, t, (r3, color * PARTS + t - 7 * PARTS), (
                (r1, color * 4 * PARTS + t - 4 * PARTS),
                (r2, color * 2 * PARTS + t - 6 * PARTS),
                (r3, color * PARTS + t - 7 * PARTS)))
            store(color, t).start()
            if fill:
                refill(color, t + 2)

    run(7 * PARTS, 7 * PARTS + 2, lambda t: phase_four(t, True))
    run(7 * PARTS + 2, STEPS, lambda t: phase_four(t, False))

    def drain(lo, hi, wait):
        def body(t):
            for color in range(COLORS):
                wait(color, t)
        run(lo, hi, body)

    drain(4 * PARTS - 3, 4 * PARTS, lambda c, t: push1(c, t).wait_send())
    drain(4 * PARTS, 6 * PARTS, lambda c, t: push2(c, t).wait_send())
    drain(6 * PARTS, 7 * PARTS, lambda c, t: push3(c, t).wait_send())
    drain(STEPS - 4, STEPS, lambda c, t: swap(c, t).wait_send())
    drain(7 * PARTS, STEPS, lambda c, t: store(c, t).wait())


def scatter_sum(g_mat, axis_name, group_size):
    total = g_mat.shape[1]
    piece = total // group_size
    chunk = piece // (COLORS * PARTS)
    dma = pltpu.SemaphoreType.DMA
    out, _ = pl.pallas_call(
        functools.partial(scatter_kernel, axis_name, piece),
        out_shape=(jax.ShapeDtypeStruct((1, piece), jnp.float32),
                   jax.ShapeDtypeStruct((1, total // 2), jnp.bfloat16)),
        in_specs=[pl.BlockSpec(memory_space=pl.ANY)],
        out_specs=[pl.BlockSpec(memory_space=pl.ANY)] * 2,
        scratch_shapes=[
            pltpu.VMEM((2 * COLORS, 1, chunk), jnp.bfloat16),
            pltpu.VMEM((2 * COLORS, 1, chunk), jnp.bfloat16),
            pltpu.VMEM((3 * COLORS, 1, chunk), jnp.float32),
            pltpu.VMEM((4 * PARTS * COLORS, 1, chunk), jnp.float32),
            pltpu.VMEM((2 * PARTS * COLORS, 1, chunk), jnp.float32),
            pltpu.VMEM((PARTS * COLORS, 1, chunk), jnp.float32),
            dma((2 * COLORS,)), dma((2 * COLORS,)),
            dma((4 * COLORS,)), dma((STEPS * COLORS,)),
            dma((3 * COLORS,)), dma((4 * PARTS * COLORS,)),
            dma((2 * PARTS * COLORS,)), dma((2 * PARTS * COLORS,)),
            dma((PARTS * COLORS,)), dma((PARTS * COLORS,)),
            dma((PARTS * COLORS,)),
        ],
        compiler_params=pltpu.CompilerParams(
            collective_id=0, has_side_effects=True, vmem_limit_bytes=63 * 1024 * 1024),
        name="scatter_sum",
    )(g_mat)
    return out.reshape(piece)


def solution(mesh):
    axis_name = mesh.axis_names[0]
    group_size = mesh.shape[axis_name]

    def local_step(g_mat, g_vec, p_mat, m_mat, v_mat, p_vec, m_vec, v_vec, learn_rate):
        grad_mat = scatter_sum(g_mat, axis_name, group_size) / group_size
        grad_vec = lax.psum(g_vec[0].astype(jnp.float32), axis_name) / group_size
        norm_sq = lax.psum(jnp.sum(grad_mat * grad_mat), axis_name) + jnp.sum(grad_vec * grad_vec)
        clip_scale = jnp.minimum(1.0, MAX_NORM / (jnp.sqrt(norm_sq) + NORM_EPS))
        new_p_mat, new_m_mat, new_v_mat = adam_update(grad_mat * clip_scale, p_mat, m_mat, v_mat, learn_rate, WEIGHT_DECAY)
        new_p_vec, new_m_vec, new_v_vec = adam_update(grad_vec * clip_scale, p_vec, m_vec, v_vec, learn_rate, 0.0)
        full_params = lax.all_gather(new_p_mat.astype(jnp.bfloat16), axis_name, tiled=True)
        return new_p_mat, new_m_mat, new_v_mat, new_p_vec, new_m_vec, new_v_vec, full_params

    return jax.shard_map(
        local_step,
        mesh=mesh,
        in_specs=(P(axis_name, None), P(axis_name, None), P(axis_name), P(axis_name), P(axis_name), P(), P(), P(), P()),
        out_specs=(P(axis_name), P(axis_name), P(axis_name), P(), P(), P(), P()),
        check_vma=False,
    )
```

```python
import functools

import jax
import jax.numpy as jnp
from jax import lax
from jax.experimental import pallas as pl
from jax.experimental.pallas import tpu as pltpu
from jax.sharding import PartitionSpec as P

STEP = 10
ADAM_BETA1 = 0.9
ADAM_BETA2 = 0.98
ADAM_EPS = 1e-8
WEIGHT_DECAY = 0.01
MAX_NORM = 1.0
NORM_EPS = 1e-6
BIAS_ONE = 1.0 - ADAM_BETA1 ** STEP
BIAS_TWO = 1.0 - ADAM_BETA2 ** STEP

MESH_ID = pl.DeviceIdType.MESH
COLORS = 3
PARTS = 4
STRIDES = (2, 4, 8)
STEPS = 8 * PARTS
WIDTH = 4096
WRITES = 16
MEAN_SCALE = 1.0 / 16.0


def adam_update(grad_vals, param_vals, moment_one, moment_two, learn_rate, decay_rate):
    new_one = ADAM_BETA1 * moment_one + (1.0 - ADAM_BETA1) * grad_vals
    new_two = ADAM_BETA2 * moment_two + (1.0 - ADAM_BETA2) * grad_vals * grad_vals
    direction = (new_one / BIAS_ONE) / (jnp.sqrt(new_two / BIAS_TWO) + ADAM_EPS)
    return param_vals - learn_rate * (direction + decay_rate * param_vals), new_one, new_two


def scatter_kernel(axis_name, piece, g, gv, out, pg, vec_out, clip_out,
                   a_buf, b_buf, stage, r1, r2, r3, v_in, v_acc, v_get, n_acc, n_get, squares,
                   a_sem, b_sem, ds_sem, dr_sem, s1_sem, r1_sem, s2_sem, r2_sem, s3_sem, r3_sem, o_sem,
                   vi_sem, vs_sem, vr_sem, ns_sem, nr_sem, vo_sem):
    chunk = piece // (COLORS * PARTS)
    width = min(chunk, WIDTH)
    n_vec = gv.shape[1]
    me = lax.axis_index(axis_name)
    core_step = 1 - 2 * lax.rem(me, 2)
    deltas = [s * (1 - 2 * lax.rem(me // s, 2)) for s in STRIDES]
    partner = me + core_step
    peers = [me + d for d in deltas]

    barrier = pltpu.get_barrier_semaphore()
    for dev in (partner, *peers):
        pl.semaphore_signal(barrier, inc=1, device_id=(dev,), device_id_type=MESH_ID)

    def offset(color, t):
        unit = t // PARTS
        f1 = 1 - unit // 4
        f2 = 1 - lax.rem(unit // 2, 2)
        f3 = 1 - lax.rem(unit, 2)
        d1, d2, d3 = (deltas[(color + k) % 3] for k in range(3))
        owner = me + f1 * d1 + f2 * d2 + f3 * d3
        return owner * piece + (color * PARTS + lax.rem(t, PARTS)) * chunk

    def cut(ref, start):
        return ref.at[:, pl.ds(pl.multiple_of(start, 1024), chunk)]

    def swap(color, t):
        return pltpu.make_async_remote_copy(
            src_ref=cut(g, offset(color, t) + core_step * piece),
            dst_ref=cut(pg, (color * STEPS + t) * chunk),
            send_sem=ds_sem.at[color * 4 + lax.rem(t, 4)],
            recv_sem=dr_sem.at[color * STEPS + t],
            device_id=(partner,), device_id_type=MESH_ID)

    def load_a(color, t):
        k = color * 2 + lax.rem(t, 2)
        return pltpu.make_async_copy(cut(g, offset(color, t)), a_buf.at[k], a_sem.at[k])

    def load_b(color, t):
        k = color * 2 + lax.rem(t, 2)
        return pltpu.make_async_copy(cut(pg, (color * STEPS + t) * chunk), b_buf.at[k], b_sem.at[k])

    def push(src, dst, send_sem, recv_sem, axis):
        return pltpu.make_async_remote_copy(
            src_ref=src, dst_ref=dst, send_sem=send_sem, recv_sem=recv_sem,
            device_id=(peers[axis],), device_id_type=MESH_ID)

    def push1(color, t):
        k = color * 3 + lax.rem(t, 3)
        j = color * 4 * PARTS + t
        return push(stage.at[k], r1.at[j], s1_sem.at[k], r1_sem.at[j], color)

    def push2(color, t):
        j = color * 2 * PARTS + t - 4 * PARTS
        return push(r1.at[color * 4 * PARTS + t - 4 * PARTS], r2.at[j], s2_sem.at[j], r2_sem.at[j], (color + 1) % 3)

    def push3(color, t):
        j = color * PARTS + t - 6 * PARTS
        return push(r1.at[color * 4 * PARTS + t - 4 * PARTS], r3.at[j], s3_sem.at[j], r3_sem.at[j], (color + 2) % 3)

    def store(color, t):
        j = color * PARTS + t - 7 * PARTS
        return pltpu.make_async_copy(r3.at[j], cut(out, j * chunk), o_sem.at[j])

    def add_up(color, t, dst, extra, last=False):
        k = color * 2 + lax.rem(t, 2)

        @pl.loop(0, chunk // width)
        def _(i):
            s = pl.ds(pl.multiple_of(i * width, width), width)
            acc = a_buf[k, :, s].astype(jnp.float32) + b_buf[k, :, s].astype(jnp.float32)
            for ref, j in extra:
                acc = acc + ref[j, :, s]
            if last:
                acc = acc * MEAN_SCALE
                squares[...] += acc * acc
            dst[0][dst[1], :, s] = acc

    def vec_push(k):
        return pltpu.make_async_remote_copy(
            src_ref=v_acc.at[k], dst_ref=v_get.at[k], send_sem=vs_sem.at[k], recv_sem=vr_sem.at[k],
            device_id=((partner, *peers)[k],), device_id_type=MESH_ID)

    def norm_push(k):
        return pltpu.make_async_remote_copy(
            src_ref=n_acc.at[k], dst_ref=n_get.at[k], send_sem=ns_sem.at[k], recv_sem=nr_sem.at[k],
            device_id=((partner, *peers)[k],), device_id_type=MESH_ID)

    def vec_loop(body):
        @pl.loop(0, n_vec // 1024)
        def _(i):
            body(pl.ds(pl.multiple_of(i * 1024, 1024), 1024))

    def vec_turn(k):
        def body(s):
            v_acc[k + 1, :, s] = v_acc[k, :, s] + v_get[k, :, s]
        vec_push(k).wait_recv()
        vec_loop(body)
        if k < 3:
            vec_push(k + 1).start()

    def ready(color, t):
        load_a(color, t).wait()
        load_b(color, t).wait()

    def refill(color, t):
        load_a(color, t).start()
        swap(color, t).wait_recv()
        load_b(color, t).start()

    def more_swap(color, t):
        swap(color, t - 4).wait_send()
        swap(color, t).start()

    for t in range(2):
        for color in range(COLORS):
            load_a(color, t).start()
    vec_load = pltpu.make_async_copy(gv, v_in, vi_sem)
    vec_load.start()
    squares[...] = jnp.zeros_like(squares)
    pl.semaphore_wait(barrier, 4)
    for t in range(4):
        for color in range(COLORS):
            swap(color, t).start()
    for t in range(2):
        for color in range(COLORS):
            swap(color, t).wait_recv()
            load_b(color, t).start()

    def phase_one(t, first):
        for color in range(COLORS):
            ready(color, t)
            if not first:
                push1(color, t - 3).wait_send()
            add_up(color, t, (stage, color * 3 + lax.rem(t, 3)), ())
            push1(color, t).start()
            more_swap(color, t + 4)
            refill(color, t + 2)

    def run(lo, hi, body):
        lax.fori_loop(lo, hi, lambda t, c: (body(t), c)[1], 0)

    run(0, 3, lambda t: phase_one(t, True))
    vec_load.wait()

    def widen(s):
        v_acc[0, :, s] = v_in[:, s].astype(jnp.float32)

    vec_loop(widen)
    vec_push(0).start()
    for k in range(4):
        run(3 * k + 3, 3 * k + 6, lambda t: phase_one(t, False))
        vec_turn(k)
    run(15, 4 * PARTS, lambda t: phase_one(t, False))

    def vec_mean(s):
        mean = v_acc[4, :, s] * MEAN_SCALE
        v_acc[0, :, s] = mean
        v_get[0, :, s] = mean * mean

    vec_push(0).wait_send()
    vec_loop(vec_mean)
    vec_store = pltpu.make_async_copy(v_acc.at[0], vec_out, vo_sem)
    vec_store.start()

    def phase_two(t):
        for color in range(COLORS):
            ready(color, t)
            j = color * 4 * PARTS + t - 4 * PARTS
            push1(color, t - 4 * PARTS).wait_recv()
            add_up(color, t, (r1, j), ((r1, j),))
            push2(color, t).start()
            more_swap(color, t + 4)
            refill(color, t + 2)

    run(4 * PARTS, 6 * PARTS, phase_two)

    def phase_three(t):
        for color in range(COLORS):
            ready(color, t)
            j = color * 4 * PARTS + t - 4 * PARTS
            push1(color, t - 4 * PARTS).wait_recv()
            push2(color, t - 2 * PARTS).wait_recv()
            add_up(color, t, (r1, j), ((r1, j), (r2, color * 2 * PARTS + t - 6 * PARTS)))
            push3(color, t).start()
            more_swap(color, t + 4)
            refill(color, t + 2)

    run(6 * PARTS, 7 * PARTS, phase_three)

    def phase_four(t, fill):
        for color in range(COLORS):
            ready(color, t)
            push1(color, t - 4 * PARTS).wait_recv()
            push2(color, t - 2 * PARTS).wait_recv()
            push3(color, t - PARTS).wait_recv()
            add_up(color, t, (r3, color * PARTS + t - 7 * PARTS), (
                (r1, color * 4 * PARTS + t - 4 * PARTS),
                (r2, color * 2 * PARTS + t - 6 * PARTS),
                (r3, color * PARTS + t - 7 * PARTS)), last=True)
            store(color, t).start()
            if fill:
                refill(color, t + 2)

    run(7 * PARTS, 7 * PARTS + 2, lambda t: phase_four(t, True))
    run(7 * PARTS + 2, STEPS, lambda t: phase_four(t, False))

    n_acc[0] = jnp.broadcast_to(jnp.sum(squares[...], axis=1, keepdims=True), (1, 128))
    for k in range(4):
        norm_push(k).start()
        norm_push(k).wait_recv()
        n_acc[k + 1] = n_acc[k] + n_get[k]
    norm_sq = n_acc[4] + jnp.sum(v_get[0], axis=1, keepdims=True)
    clip_out[...] = jnp.minimum(1.0, MAX_NORM / (jnp.sqrt(norm_sq) + NORM_EPS))

    def drain(lo, hi, wait):
        def body(t):
            for color in range(COLORS):
                wait(color, t)
        run(lo, hi, body)

    drain(4 * PARTS - 3, 4 * PARTS, lambda c, t: push1(c, t).wait_send())
    drain(4 * PARTS, 6 * PARTS, lambda c, t: push2(c, t).wait_send())
    drain(6 * PARTS, 7 * PARTS, lambda c, t: push3(c, t).wait_send())
    drain(STEPS - 4, STEPS, lambda c, t: swap(c, t).wait_send())
    drain(7 * PARTS, STEPS, lambda c, t: store(c, t).wait())
    for k in range(4):
        norm_push(k).wait_send()
        if k:
            vec_push(k).wait_send()
    vec_store.wait()


def scatter_sum(g_mat, g_vec, axis_name, group_size):
    total = g_mat.shape[1]
    n_vec = g_vec.shape[1]
    piece = total // group_size
    chunk = piece // (COLORS * PARTS)
    dma = pltpu.SemaphoreType.DMA
    any_spec = pl.BlockSpec(memory_space=pl.ANY)
    out, _, vec, clip = pl.pallas_call(
        functools.partial(scatter_kernel, axis_name, piece),
        out_shape=(jax.ShapeDtypeStruct((1, piece), jnp.float32),
                   jax.ShapeDtypeStruct((1, total // 2), jnp.bfloat16),
                   jax.ShapeDtypeStruct((1, n_vec), jnp.float32),
                   jax.ShapeDtypeStruct((1, 128), jnp.float32)),
        in_specs=[any_spec, any_spec],
        out_specs=[any_spec, any_spec, any_spec, pl.BlockSpec(memory_space=pltpu.VMEM)],
        scratch_shapes=[
            pltpu.VMEM((2 * COLORS, 1, chunk), jnp.bfloat16),
            pltpu.VMEM((2 * COLORS, 1, chunk), jnp.bfloat16),
            pltpu.VMEM((3 * COLORS, 1, chunk), jnp.float32),
            pltpu.VMEM((4 * PARTS * COLORS, 1, chunk), jnp.float32),
            pltpu.VMEM((2 * PARTS * COLORS, 1, chunk), jnp.float32),
            pltpu.VMEM((PARTS * COLORS, 1, chunk), jnp.float32),
            pltpu.VMEM((1, n_vec), jnp.bfloat16),
            pltpu.VMEM((5, 1, n_vec), jnp.float32),
            pltpu.VMEM((4, 1, n_vec), jnp.float32),
            pltpu.VMEM((5, 1, 128), jnp.float32),
            pltpu.VMEM((4, 1, 128), jnp.float32),
            pltpu.VMEM((1, min(chunk, WIDTH)), jnp.float32),
            dma((2 * COLORS,)), dma((2 * COLORS,)),
            dma((4 * COLORS,)), dma((STEPS * COLORS,)),
            dma((3 * COLORS,)), dma((4 * PARTS * COLORS,)),
            dma((2 * PARTS * COLORS,)), dma((2 * PARTS * COLORS,)),
            dma((PARTS * COLORS,)), dma((PARTS * COLORS,)),
            dma((PARTS * COLORS,)),
            dma, dma((4,)), dma((4,)), dma((4,)), dma((4,)), dma,
        ],
        compiler_params=pltpu.CompilerParams(
            collective_id=0, has_side_effects=True, vmem_limit_bytes=63 * 1024 * 1024),
        name="scatter_sum",
    )(g_mat, g_vec)
    return out.reshape(piece), vec.reshape(n_vec), clip[0, 0]


def gather_kernel(axis_name, x, out, s_sem, r_sem, own_sem, ds_sem, dr_sem):
    own = COLORS * PARTS
    me = lax.axis_index(axis_name)
    deltas = [s * (1 - 2 * lax.rem(me // s, 2)) for s in STRIDES]
    partner = me + 1 - 2 * lax.rem(me, 2)
    peers = [me + d for d in deltas]

    barrier = pltpu.get_barrier_semaphore()
    for dev in (partner, *peers):
        pl.semaphore_signal(barrier, inc=1, device_id=(dev,), device_id_type=MESH_ID)

    def local(i):
        return pltpu.make_async_copy(x.at[i], out.at[me * own + i], own_sem.at[i])

    def across(src, index):
        return pltpu.make_async_remote_copy(
            src_ref=src, dst_ref=out.at[index], send_sem=ds_sem, recv_sem=dr_sem,
            device_id=(partner,), device_id_type=MESH_ID)

    def route(stage, axis):
        b1, b2 = (axis - 2) % 3, (axis - 1) % 3
        color = (axis, b2, b2, b1, b1, b1, b1)[stage]
        flips = ((), (), (b2,), (), (b1,), (b2,), (b1, b2))[stage]
        return color, sum((deltas[f] for f in flips), me), not flips

    def push(stage, axis, q):
        color, owner, mine = route(stage, axis)
        index = owner * own + color * PARTS + q
        k = (stage * 3 + axis) * PARTS + q
        return pltpu.make_async_remote_copy(
            src_ref=x.at[color * PARTS + q] if mine else out.at[index], dst_ref=out.at[index],
            send_sem=s_sem.at[k], recv_sem=r_sem.at[k],
            device_id=(peers[axis],), device_id_type=MESH_ID)

    def land(stage, axis, q):
        color, owner, _ = route(stage, axis)
        index = (owner + deltas[axis]) * own + color * PARTS + q
        push(stage, axis, q).wait_recv()
        across(out.at[index], index).start()

    def each(count, body):
        lax.fori_loop(0, count, lambda i, c: (body(i), c)[1], 0)

    pl.semaphore_wait(barrier, 4)

    for stage in range(8):
        def body(q, stage=stage):
            for axis in range(3):
                if stage < 7:
                    push(stage, axis, q).start()
                if stage:
                    land(stage - 1, axis, q)
                else:
                    i = axis * PARTS + q
                    across(x.at[i], me * own + i).start()
        each(PARTS, body)
        if stage == 0:
            each(own, lambda i: local(i).start())

    half = pltpu.make_async_remote_copy(
        src_ref=out.at[pl.ds(0, 8 * own)], dst_ref=out.at[pl.ds(0, 8 * own)], send_sem=ds_sem, recv_sem=dr_sem,
        device_id=(partner,), device_id_type=MESH_ID)
    each(own, lambda i: local(i).wait())
    for stage in range(7):
        def body(q, stage=stage):
            for axis in range(3):
                push(stage, axis, q).wait_send()
        each(PARTS, body)
    half.wait_recv()
    half.wait_send()


def write_kernel(rows, held, out, sem):
    def cut(ref, i):
        return ref.at[pl.ds(i * rows, rows)]

    copies = [pltpu.make_async_copy(cut(held, i), cut(out, i), sem.at[i]) for i in range(WRITES)]
    for copy in copies:
        copy.start()
    for copy in copies:
        copy.wait()


def gather_params(piece_bf16, axis_name, group_size):
    own = COLORS * PARTS
    piece = piece_bf16.shape[0]
    rows = piece // (own * 128)
    dma = pltpu.SemaphoreType.DMA
    full = pl.pallas_call(
        functools.partial(gather_kernel, axis_name),
        out_shape=pltpu.VMEM((group_size * own, rows, 128), jnp.bfloat16),
        in_specs=[pl.BlockSpec(memory_space=pltpu.HBM)],
        out_specs=pl.BlockSpec(memory_space=pltpu.VMEM),
        scratch_shapes=[dma((7 * 3 * PARTS,)), dma((7 * 3 * PARTS,)), dma((own,)), dma, dma],
        compiler_params=pltpu.CompilerParams(
            collective_id=1, has_side_effects=True, vmem_limit_bytes=2 * 1024 * 1024),
        name="gather_params",
    )(piece_bf16.reshape(own, rows, 128))
    full = pl.pallas_call(
        functools.partial(write_kernel, group_size * own // WRITES),
        out_shape=jax.ShapeDtypeStruct(full.shape, full.dtype),
        in_specs=[pl.BlockSpec(memory_space=pltpu.VMEM)],
        out_specs=pl.BlockSpec(memory_space=pl.ANY),
        scratch_shapes=[dma((WRITES,))],
        compiler_params=pltpu.CompilerParams(vmem_limit_bytes=1024 * 1024),
        name="write_params",
    )(full)
    return full.reshape(group_size * piece)


def solution(mesh):
    axis_name = mesh.axis_names[0]
    group_size = mesh.shape[axis_name]

    def local_step(g_mat, g_vec, p_mat, m_mat, v_mat, p_vec, m_vec, v_vec, learn_rate):
        grad_mat, grad_vec, clip_scale = lax.optimization_barrier(scatter_sum(g_mat, g_vec, axis_name, group_size))
        new_p_mat, new_m_mat, new_v_mat = adam_update(grad_mat * clip_scale, p_mat, m_mat, v_mat, learn_rate, WEIGHT_DECAY)
        new_p_vec, new_m_vec, new_v_vec = adam_update(grad_vec * clip_scale, p_vec, m_vec, v_vec, learn_rate, 0.0)
        full_params = gather_params(new_p_mat.astype(jnp.bfloat16), axis_name, group_size)
        return new_p_mat, new_m_mat, new_v_mat, new_p_vec, new_m_vec, new_v_vec, full_params

    return jax.shard_map(
        local_step,
        mesh=mesh,
        in_specs=(P(axis_name, None), P(axis_name, None), P(axis_name), P(axis_name), P(axis_name), P(), P(), P(), P()),
        out_specs=(P(axis_name), P(axis_name), P(axis_name), P(), P(), P(), P()),
        check_vma=False,
    )
```

```python
import functools

import jax
import jax.numpy as jnp
from jax import lax
from jax.experimental import pallas as pl
from jax.experimental.pallas import tpu as pltpu
from jax.sharding import PartitionSpec as P

STEP = 10
ADAM_BETA1 = 0.9
ADAM_BETA2 = 0.98
ADAM_EPS = 1e-8
WEIGHT_DECAY = 0.01
MAX_NORM = 1.0
NORM_EPS = 1e-6
BIAS_ONE = 1.0 - ADAM_BETA1 ** STEP
BIAS_TWO = 1.0 - ADAM_BETA2 ** STEP

MESH_ID = pl.DeviceIdType.MESH
COLORS = 3
PARTS = 4
STRIDES = (2, 4, 8)
STEPS = 8 * PARTS
DEVICES = 16
WIDTH = 4096
ROWS = 64
SMALL_VMEM = 3400 * 1024
RING = 5
MEAN_SCALE = 1.0 / 16.0


def scatter_kernel(axis_name, piece, g, gv, lr, out, pg, vec_out, scale_out,
                   a_buf, b_buf, stage, r1, r2, r3, v_in, v_acc, v_get, n_put, n_get, squares, lr_smem, scale_buf,
                   a_sem, b_sem, ds_sem, dr_sem, s1_sem, r1_sem, s2_sem, r2_sem, s3_sem, r3_sem, o_sem,
                   vi_sem, vs_sem, vr_sem, ns_sem, nr_sem, vo_sem, lr_sem, so_sem):
    chunk = piece // (COLORS * PARTS)
    width = min(chunk, WIDTH)
    n_vec = gv.shape[1]
    me = lax.axis_index(axis_name)
    core_step = 1 - 2 * lax.rem(me, 2)
    deltas = [s * (1 - 2 * lax.rem(me // s, 2)) for s in STRIDES]
    partner = me + core_step
    peers = [me + d for d in deltas]

    barrier = pltpu.get_barrier_semaphore()
    for dev in (partner, *peers):
        pl.semaphore_signal(barrier, inc=1, device_id=(dev,), device_id_type=MESH_ID)

    def offset(color, t):
        unit = t // PARTS
        f1 = 1 - unit // 4
        f2 = 1 - lax.rem(unit // 2, 2)
        f3 = 1 - lax.rem(unit, 2)
        d1, d2, d3 = (deltas[(color + k) % 3] for k in range(3))
        owner = me + f1 * d1 + f2 * d2 + f3 * d3
        return owner * piece + (color * PARTS + lax.rem(t, PARTS)) * chunk

    def cut(ref, start):
        return ref.at[:, pl.ds(pl.multiple_of(start, 1024), chunk)]

    def swap(color, t):
        return pltpu.make_async_remote_copy(
            src_ref=cut(g, offset(color, t) + core_step * piece),
            dst_ref=cut(pg, (color * STEPS + t) * chunk),
            send_sem=ds_sem.at[color * 4 + lax.rem(t, 4)],
            recv_sem=dr_sem.at[color * STEPS + t],
            device_id=(partner,), device_id_type=MESH_ID)

    def load_a(color, t):
        k = color * 2 + lax.rem(t, 2)
        return pltpu.make_async_copy(cut(g, offset(color, t)), a_buf.at[k], a_sem.at[k])

    def load_b(color, t):
        k = color * 2 + lax.rem(t, 2)
        return pltpu.make_async_copy(cut(pg, (color * STEPS + t) * chunk), b_buf.at[k], b_sem.at[k])

    def push(src, dst, send_sem, recv_sem, axis):
        return pltpu.make_async_remote_copy(
            src_ref=src, dst_ref=dst, send_sem=send_sem, recv_sem=recv_sem,
            device_id=(peers[axis],), device_id_type=MESH_ID)

    def push1(color, t):
        k = color * 3 + lax.rem(t, 3)
        j = color * 4 * PARTS + t
        return push(stage.at[k], r1.at[j], s1_sem.at[k], r1_sem.at[j], color)

    def push2(color, t):
        j = color * 2 * PARTS + t - 4 * PARTS
        return push(r1.at[color * 4 * PARTS + t - 4 * PARTS], r2.at[j], s2_sem.at[j], r2_sem.at[j], (color + 1) % 3)

    def push3(color, t):
        j = color * PARTS + t - 6 * PARTS
        return push(r1.at[color * 4 * PARTS + t - 4 * PARTS], r3.at[j], s3_sem.at[j], r3_sem.at[j], (color + 2) % 3)

    def store(color, t):
        j = color * PARTS + t - 7 * PARTS
        return pltpu.make_async_copy(r3.at[j], cut(out, j * chunk), o_sem.at[j])

    def add_up(color, t, dst, extra, last=False):
        k = color * 2 + lax.rem(t, 2)

        @pl.loop(0, chunk // width)
        def _(i):
            s = pl.ds(pl.multiple_of(i * width, width), width)
            acc = a_buf[k, :, s].astype(jnp.float32) + b_buf[k, :, s].astype(jnp.float32)
            for ref, j in extra:
                acc = acc + ref[j, :, s]
            if last:
                acc = acc * MEAN_SCALE
                squares[...] += acc * acc
            dst[0][dst[1], :, s] = acc

    def vec_push(k):
        return pltpu.make_async_remote_copy(
            src_ref=v_acc.at[k], dst_ref=v_get.at[k], send_sem=vs_sem.at[k], recv_sem=vr_sem.at[k],
            device_id=((partner, *peers)[k],), device_id_type=MESH_ID)

    def norm_push(k):
        return pltpu.make_async_remote_copy(
            src_ref=n_put, dst_ref=n_get.at[me], send_sem=ns_sem, recv_sem=nr_sem,
            device_id=(lax.rem(me + k, DEVICES),), device_id_type=MESH_ID)

    def vec_loop(body):
        @pl.loop(0, n_vec // 1024)
        def _(i):
            body(pl.ds(pl.multiple_of(i * 1024, 1024), 1024))

    def vec_turn(k):
        def body(s):
            v_acc[k + 1, :, s] = v_acc[k, :, s] + v_get[k, :, s]
        vec_push(k).wait_recv()
        vec_loop(body)
        if k < 3:
            vec_push(k + 1).start()

    def ready(color, t):
        load_a(color, t).wait()
        load_b(color, t).wait()

    def refill(color, t):
        load_a(color, t).start()
        swap(color, t).wait_recv()
        load_b(color, t).start()

    def more_swap(color, t):
        swap(color, t - 4).wait_send()
        swap(color, t).start()

    for t in range(2):
        for color in range(COLORS):
            load_a(color, t).start()
    vec_load = pltpu.make_async_copy(gv, v_in, vi_sem)
    vec_load.start()
    lr_load = pltpu.make_async_copy(lr, lr_smem, lr_sem)
    lr_load.start()
    squares[...] = jnp.zeros_like(squares)
    pl.semaphore_wait(barrier, 4)
    for t in range(4):
        for color in range(COLORS):
            swap(color, t).start()
    for t in range(2):
        for color in range(COLORS):
            swap(color, t).wait_recv()
            load_b(color, t).start()

    def phase_one(t, first):
        for color in range(COLORS):
            ready(color, t)
            if not first:
                push1(color, t - 3).wait_send()
            add_up(color, t, (stage, color * 3 + lax.rem(t, 3)), ())
            push1(color, t).start()
            more_swap(color, t + 4)
            refill(color, t + 2)

    def run(lo, hi, body):
        lax.fori_loop(lo, hi, lambda t, c: (body(t), c)[1], 0)

    run(0, 3, lambda t: phase_one(t, True))
    vec_load.wait()

    def widen(s):
        v_acc[0, :, s] = v_in[:, s].astype(jnp.float32)

    vec_loop(widen)
    vec_push(0).start()
    for k in range(4):
        run(3 * k + 3, 3 * k + 6, lambda t: phase_one(t, False))
        vec_turn(k)
    run(15, 4 * PARTS, lambda t: phase_one(t, False))

    def vec_mean(s):
        mean = v_acc[4, :, s] * MEAN_SCALE
        v_acc[0, :, s] = mean
        v_get[0, :, s] = mean * mean

    vec_push(0).wait_send()
    vec_loop(vec_mean)
    vec_store = pltpu.make_async_copy(v_acc.at[0], vec_out, vo_sem)
    vec_store.start()

    def phase_two(t):
        for color in range(COLORS):
            ready(color, t)
            j = color * 4 * PARTS + t - 4 * PARTS
            push1(color, t - 4 * PARTS).wait_recv()
            add_up(color, t, (r1, j), ((r1, j),))
            push2(color, t).start()
            more_swap(color, t + 4)
            refill(color, t + 2)

    run(4 * PARTS, 6 * PARTS, phase_two)

    def phase_three(t):
        for color in range(COLORS):
            ready(color, t)
            j = color * 4 * PARTS + t - 4 * PARTS
            push1(color, t - 4 * PARTS).wait_recv()
            push2(color, t - 2 * PARTS).wait_recv()
            add_up(color, t, (r1, j), ((r1, j), (r2, color * 2 * PARTS + t - 6 * PARTS)))
            push3(color, t).start()
            more_swap(color, t + 4)
            refill(color, t + 2)

    run(6 * PARTS, 7 * PARTS, phase_three)

    def phase_four(t, fill):
        for color in range(COLORS):
            ready(color, t)
            push1(color, t - 4 * PARTS).wait_recv()
            push2(color, t - 2 * PARTS).wait_recv()
            push3(color, t - PARTS).wait_recv()
            add_up(color, t, (r3, color * PARTS + t - 7 * PARTS), (
                (r1, color * 4 * PARTS + t - 4 * PARTS),
                (r2, color * 2 * PARTS + t - 6 * PARTS),
                (r3, color * PARTS + t - 7 * PARTS)), last=True)
            store(color, t).start()
            if fill:
                refill(color, t + 2)

    run(7 * PARTS, 7 * PARTS + 2, lambda t: phase_four(t, True))
    run(7 * PARTS + 2, STEPS, lambda t: phase_four(t, False))

    part = jnp.broadcast_to(jnp.sum(squares[...], axis=1, keepdims=True), (1, 128))
    n_put[...] = part
    n_get[me] = part
    for k in range(1, DEVICES):
        norm_push(k).start()
    rest = pltpu.make_async_remote_copy(
        src_ref=n_get.at[pl.ds(0, DEVICES - 1)], dst_ref=n_get.at[pl.ds(0, DEVICES - 1)],
        send_sem=ns_sem, recv_sem=nr_sem, device_id=(partner,), device_id_type=MESH_ID)
    rest.wait_recv()
    norm_sq = n_get[0]
    for k in range(1, DEVICES):
        norm_sq = norm_sq + n_get[k]
    norm_sq = norm_sq + jnp.sum(v_get[0], axis=1, keepdims=True)
    scale_buf[0:1, :] = jnp.minimum(1.0, MAX_NORM / (jnp.sqrt(norm_sq) + NORM_EPS))
    lr_load.wait()
    scale_buf[1:2, :] = jnp.full((1, 128), lr_smem[0, 0])
    scale_store = pltpu.make_async_copy(scale_buf, scale_out, so_sem)
    scale_store.start()

    def drain(lo, hi, wait):
        def body(t):
            for color in range(COLORS):
                wait(color, t)
        run(lo, hi, body)

    drain(4 * PARTS - 3, 4 * PARTS, lambda c, t: push1(c, t).wait_send())
    drain(4 * PARTS, 6 * PARTS, lambda c, t: push2(c, t).wait_send())
    drain(6 * PARTS, 7 * PARTS, lambda c, t: push3(c, t).wait_send())
    drain(STEPS - 4, STEPS, lambda c, t: swap(c, t).wait_send())
    drain(7 * PARTS, STEPS, lambda c, t: store(c, t).wait())
    for k in range(1, 4):
        vec_push(k).wait_send()
    rest.wait_send()
    vec_store.wait()
    scale_store.wait()


def scatter_sum(g_mat, g_vec, learn_rate, axis_name, group_size):
    total = g_mat.shape[1]
    n_vec = g_vec.shape[1]
    piece = total // group_size
    chunk = piece // (COLORS * PARTS)
    dma = pltpu.SemaphoreType.DMA
    any_spec = pl.BlockSpec(memory_space=pl.ANY)
    out, _, vec, scales = pl.pallas_call(
        functools.partial(scatter_kernel, axis_name, piece),
        out_shape=(jax.ShapeDtypeStruct((1, piece), jnp.float32),
                   jax.ShapeDtypeStruct((1, total // 2), jnp.bfloat16),
                   jax.ShapeDtypeStruct((1, n_vec), jnp.float32),
                   jax.ShapeDtypeStruct((2, 128), jnp.float32)),
        in_specs=[any_spec] * 3,
        out_specs=[any_spec] * 4,
        scratch_shapes=[
            pltpu.VMEM((2 * COLORS, 1, chunk), jnp.bfloat16),
            pltpu.VMEM((2 * COLORS, 1, chunk), jnp.bfloat16),
            pltpu.VMEM((3 * COLORS, 1, chunk), jnp.float32),
            pltpu.VMEM((4 * PARTS * COLORS, 1, chunk), jnp.float32),
            pltpu.VMEM((2 * PARTS * COLORS, 1, chunk), jnp.float32),
            pltpu.VMEM((PARTS * COLORS, 1, chunk), jnp.float32),
            pltpu.VMEM((1, n_vec), jnp.bfloat16),
            pltpu.VMEM((5, 1, n_vec), jnp.float32),
            pltpu.VMEM((4, 1, n_vec), jnp.float32),
            pltpu.VMEM((1, 128), jnp.float32),
            pltpu.VMEM((DEVICES, 1, 128), jnp.float32),
            pltpu.VMEM((1, min(chunk, WIDTH)), jnp.float32),
            pltpu.SMEM((1, 1), jnp.float32),
            pltpu.VMEM((2, 128), jnp.float32),
            dma((2 * COLORS,)), dma((2 * COLORS,)),
            dma((4 * COLORS,)), dma((STEPS * COLORS,)),
            dma((3 * COLORS,)), dma((4 * PARTS * COLORS,)),
            dma((2 * PARTS * COLORS,)), dma((2 * PARTS * COLORS,)),
            dma((PARTS * COLORS,)), dma((PARTS * COLORS,)),
            dma((PARTS * COLORS,)),
            dma, dma((4,)), dma((4,)), dma, dma, dma, dma, dma,
        ],
        compiler_params=pltpu.CompilerParams(
            collective_id=0, has_side_effects=True, vmem_limit_bytes=63 * 1024 * 1024),
        name="scatter_sum",
    )(g_mat, g_vec, learn_rate.reshape(1, 1))
    return out, vec, scales


def adam_moments(grad, m, v):
    new_m = ADAM_BETA1 * m + (1.0 - ADAM_BETA1) * grad
    new_v = ADAM_BETA2 * v + (1.0 - ADAM_BETA2) * grad * grad
    return new_m, new_v


def adam_param(p, m, v, rate, decay):
    direction = (m / BIAS_ONE) / (jnp.sqrt(v / BIAS_TWO) + ADAM_EPS)
    return p - rate * (direction + decay * p)


def gather_kernel(axis_name, grad, p, m, v, scales_in, out, m_out, v_out, g_buf, p_buf, scales,
                  scales_sem, g_sem, p_sem, m_sem, v_sem, s_sem, r_sem, ds_sem, dr_sem):
    own = COLORS * PARTS
    rows = p.shape[1]
    step = min(rows, ROWS)
    me = lax.axis_index(axis_name)
    deltas = [s * (1 - 2 * lax.rem(me // s, 2)) for s in STRIDES]
    partner = me + 1 - 2 * lax.rem(me, 2)
    peers = [me + d for d in deltas]

    barrier = pltpu.get_barrier_semaphore()
    for dev in (partner, *peers):
        pl.semaphore_signal(barrier, inc=1, device_id=(dev,), device_id_type=MESH_ID)

    def loads(color, q):
        i = color * PARTS + q
        return (pltpu.make_async_copy(grad.at[i], g_buf.at[color], g_sem.at[color]),
                pltpu.make_async_copy(m.at[i], m_out.at[i], m_sem.at[i]),
                pltpu.make_async_copy(v.at[i], v_out.at[i], v_sem.at[i]),
                pltpu.make_async_copy(p.at[i], p_buf.at[color], p_sem.at[color]))

    def across(index):
        return pltpu.make_async_remote_copy(
            src_ref=out.at[index], dst_ref=out.at[index], send_sem=ds_sem, recv_sem=dr_sem,
            device_id=(partner,), device_id_type=MESH_ID)

    def route(stage, axis):
        b1, b2 = (axis - 2) % 3, (axis - 1) % 3
        color = (axis, b2, b2, b1, b1, b1, b1)[stage]
        flips = ((), (), (b2,), (), (b1,), (b2,), (b1, b2))[stage]
        return color, sum((deltas[f] for f in flips), me)

    def push(stage, axis, q):
        color, owner = route(stage, axis)
        index = owner * own + color * PARTS + q
        k = (stage * 3 + axis) * PARTS + q
        return pltpu.make_async_remote_copy(
            src_ref=out.at[index], dst_ref=out.at[index], send_sem=s_sem.at[k], recv_sem=r_sem.at[k],
            device_id=(peers[axis],), device_id_type=MESH_ID)

    def land(stage, axis, q):
        color, owner = route(stage, axis)
        push(stage, axis, q).wait_recv()
        across((owner + deltas[axis]) * own + color * PARTS + q).start()

    def update(color, q):
        i = color * PARTS + q

        @pl.loop(0, rows // step)
        def _(r):
            s = pl.ds(pl.multiple_of(r * step, step), step)
            new_m, new_v = adam_moments(g_buf[color, s, :] * scales[0:1, :], m_out[i, s, :], v_out[i, s, :])
            m_out[i, s, :] = new_m
            v_out[i, s, :] = new_v
            new_p = adam_param(p_buf[color, s, :], new_m, new_v, scales[1:2, :], WEIGHT_DECAY)
            out[me * own + i, s, :] = new_p.astype(jnp.bfloat16)

    def each(count, body):
        lax.fori_loop(0, count, lambda i, c: (body(i), c)[1], 0)

    scales_load = pltpu.make_async_copy(scales_in, scales, scales_sem)
    scales_load.start()
    for color in range(COLORS):
        for copy in loads(color, 0):
            copy.start()
    scales_load.wait()
    for q in range(PARTS):
        for color in range(COLORS):
            for copy in loads(color, q):
                copy.wait()
            update(color, q)
            if q == 0 and color == 0:
                pl.semaphore_wait(barrier, 4)
            push(0, color, q).start()
            push(1, (color + 1) % 3, q).start()
            across(me * own + color * PARTS + q).start()
            if q + 1 < PARTS:
                for copy in loads(color, q + 1):
                    copy.start()
        if q >= 2:
            for axis in range(3):
                land(0, axis, q - 2)
                land(1, axis, q - 2)
    for q in range(PARTS):
        for axis in range(3):
            push(2, axis, q).start()
            land(q % 2, axis, 2 + q // 2)
    for stage in range(3, 8):
        def body(q, stage=stage):
            for axis in range(3):
                if stage < 7:
                    push(stage, axis, q).start()
                land(stage - 1, axis, q)
        each(PARTS, body)

    for stage in range(7):
        def body(q, stage=stage):
            for axis in range(3):
                push(stage, axis, q).wait_send()
        each(PARTS, body)
    half = pltpu.make_async_remote_copy(
        src_ref=out.at[pl.ds(0, 8 * own)], dst_ref=out.at[pl.ds(0, 8 * own)], send_sem=ds_sem, recv_sem=dr_sem,
        device_id=(partner,), device_id_type=MESH_ID)
    half.wait_recv()
    half.wait_send()


def write_kernel(held, m_held, v_held, p, scales_in, g_vec, p_vec, m_vec, v_vec,
                 out, p_out, m_out, v_out, pv_out, mv_out, vv_out,
                 p_buf, vec_buf, scales, in_sem, out_sem, sem, vec_sem, vec_out_sem, scales_sem):
    own, rows, _ = p.shape
    step = min(rows, ROWS)
    span = held.shape[0] // own

    def load(i):
        return pltpu.make_async_copy(p.at[i], p_buf.at[i % RING], in_sem.at[i % RING])

    def store(i):
        return pltpu.make_async_copy(p_buf.at[i % RING], p_out.at[i], out_sem.at[i % RING])

    def copies(i):
        part = pl.ds(i * span, span)
        return (pltpu.make_async_copy(held.at[part], out.at[part], sem.at[0, i]),
                pltpu.make_async_copy(m_held.at[i], m_out.at[i], sem.at[1, i]),
                pltpu.make_async_copy(v_held.at[i], v_out.at[i], sem.at[2, i]))

    scales_load = pltpu.make_async_copy(scales_in, scales, scales_sem)
    scales_load.start()
    vec_loads = [pltpu.make_async_copy(a, vec_buf.at[k], vec_sem.at[k])
                 for k, a in enumerate((p_vec, m_vec, v_vec, g_vec))]
    vec_stores = [pltpu.make_async_copy(vec_buf.at[k], a, vec_out_sem.at[k])
                  for k, a in enumerate((pv_out, mv_out, vv_out))]
    for i in range(RING - 1):
        load(i).start()
    for copy in vec_loads:
        copy.start()
    for i in range(own):
        for copy in copies(i):
            copy.start()
    scales_load.wait()
    for i in range(own):
        load(i).wait()

        @pl.loop(0, rows // step)
        def _(r):
            s = pl.ds(pl.multiple_of(r * step, step), step)
            p_buf[i % RING, s, :] = adam_param(
                p_buf[i % RING, s, :], m_held[i, s, :], v_held[i, s, :], scales[1:2, :], WEIGHT_DECAY)

        store(i).start()
        if i + RING - 1 < own:
            if i:
                store(i - 1).wait()
            load(i + RING - 1).start()
    for copy in vec_loads:
        copy.wait()

    @pl.loop(0, g_vec.shape[1] // 1024)
    def _(i):
        s = pl.ds(pl.multiple_of(i * 1024, 1024), 1024)
        new_m, new_v = adam_moments(vec_buf[3, :, s] * scales[0:1, 0:1], vec_buf[1, :, s], vec_buf[2, :, s])
        vec_buf[1, :, s] = new_m
        vec_buf[2, :, s] = new_v
        vec_buf[0, :, s] = adam_param(vec_buf[0, :, s], new_m, new_v, scales[1:2, 0:1], 0.0)

    for copy in vec_stores:
        copy.start()
    for i in range(own - RING, own):
        store(i).wait()
    for i in range(own):
        for copy in copies(i):
            copy.wait()
    for copy in vec_stores:
        copy.wait()


def gather_update(grad, p, m, v, scales, grad_vec, p_vec, m_vec, v_vec, axis_name, group_size):
    own = COLORS * PARTS
    piece = p.shape[0]
    n_vec = p_vec.shape[0]
    rows = piece // (own * 128)
    dma = pltpu.SemaphoreType.DMA
    any_spec = pl.BlockSpec(memory_space=pl.ANY)
    vmem_spec = pl.BlockSpec(memory_space=pltpu.VMEM)
    grad, p, m, v = (a.reshape(own, rows, 128) for a in (grad, p, m, v))
    p_vec, m_vec, v_vec = (a.reshape(1, n_vec) for a in (p_vec, m_vec, v_vec))
    full, new_m, new_v = pl.pallas_call(
        functools.partial(gather_kernel, axis_name),
        out_shape=(pltpu.VMEM((group_size * own, rows, 128), jnp.bfloat16),
                   pltpu.VMEM((own, rows, 128), jnp.float32),
                   pltpu.VMEM((own, rows, 128), jnp.float32)),
        in_specs=[any_spec] * 5,
        out_specs=[vmem_spec] * 3,
        scratch_shapes=[
            pltpu.VMEM((COLORS, rows, 128), jnp.float32), pltpu.VMEM((COLORS, rows, 128), jnp.float32),
            pltpu.VMEM((2, 128), jnp.float32), dma, dma((COLORS,)), dma((COLORS,)), dma((own,)), dma((own,)),
            dma((7 * 3 * PARTS,)), dma((7 * 3 * PARTS,)), dma, dma],
        compiler_params=pltpu.CompilerParams(
            collective_id=1, has_side_effects=True, vmem_limit_bytes=SMALL_VMEM),
        name="gather_update",
    )(grad, p, m, v, scales)
    flat = jax.ShapeDtypeStruct((own, rows, 128), jnp.float32)
    line = jax.ShapeDtypeStruct((1, n_vec), jnp.float32)
    full, new_p, new_m, new_v, *vecs = pl.pallas_call(
        write_kernel,
        out_shape=(jax.ShapeDtypeStruct(full.shape, full.dtype), flat, flat, flat, line, line, line),
        in_specs=[vmem_spec] * 3 + [any_spec] * 6,
        out_specs=[any_spec] * 7,
        scratch_shapes=[
            pltpu.VMEM((RING, rows, 128), jnp.float32), pltpu.VMEM((4, 1, n_vec), jnp.float32),
            pltpu.VMEM((2, 128), jnp.float32),
            dma((RING,)), dma((RING,)), dma((3, own)), dma((4,)), dma((3,)), dma],
        compiler_params=pltpu.CompilerParams(vmem_limit_bytes=SMALL_VMEM),
        name="write_out",
    )(*(pltpu.with_memory_space_constraint(a, pltpu.VMEM) for a in (full, new_m, new_v)),
      p, scales, grad_vec, p_vec, m_vec, v_vec)
    return (*(a.reshape(piece) for a in (new_p, new_m, new_v)), *(a.reshape(n_vec) for a in vecs),
            full.reshape(group_size * piece))


def solution(mesh):
    axis_name = mesh.axis_names[0]
    group_size = mesh.shape[axis_name]

    def local_step(g_mat, g_vec, p_mat, m_mat, v_mat, p_vec, m_vec, v_vec, learn_rate):
        grad_mat, grad_vec, scales = scatter_sum(g_mat, g_vec, learn_rate, axis_name, group_size)
        return gather_update(grad_mat, p_mat, m_mat, v_mat, scales, grad_vec, p_vec, m_vec, v_vec, axis_name, group_size)

    return jax.shard_map(
        local_step,
        mesh=mesh,
        in_specs=(P(axis_name, None), P(axis_name, None), P(axis_name), P(axis_name), P(axis_name), P(), P(), P(), P()),
        out_specs=(P(axis_name), P(axis_name), P(axis_name), P(), P(), P(), P()),
        check_vma=False,
    )
```

```python
import functools

import jax
import jax.numpy as jnp
from jax import lax
from jax.experimental import pallas as pl
from jax.experimental.pallas import tpu as pltpu
from jax.sharding import PartitionSpec as P

STEP = 10
ADAM_BETA1 = 0.9
ADAM_BETA2 = 0.98
ADAM_EPS = 1e-8
WEIGHT_DECAY = 0.01
MAX_NORM = 1.0
NORM_EPS = 1e-6
BIAS_ONE = 1.0 - ADAM_BETA1 ** STEP
BIAS_TWO = 1.0 - ADAM_BETA2 ** STEP

MESH_ID = pl.DeviceIdType.MESH
COLORS = 3
PARTS = 4
STRIDES = (2, 4, 8)
STEPS = 8 * PARTS
DEVICES = 16
WIDTH = 4096
ROWS = 64
SMALL_VMEM = 3400 * 1024
RING = 5
AHEAD = 2
CUTS = 4
MEAN_SCALE = 1.0 / 16.0


def scatter_kernel(axis_name, piece, g, gv, lr, out, pg, vec_out, scale_out,
                   a_buf, b_buf, stage, r1, r2, r3, v_in, v_full, v_acc, v_get, v_mean, n_put, n_get, squares, lr_smem, scale_buf,
                   a_sem, b_sem, ds_sem, dr_sem, dc_sem, s1_sem, r1_sem, s2_sem, r2_sem, s3_sem, r3_sem, o_sem,
                   vi_sem, vs_sem, vr_sem, ns_sem, nr_sem, vo_sem, lr_sem, so_sem):
    chunk = piece // (COLORS * PARTS)
    width = min(chunk // CUTS, WIDTH)
    part = chunk // CUTS
    n_vec = gv.shape[1]
    n_half = n_vec // 2
    me = lax.axis_index(axis_name)
    core = lax.rem(me, 2)
    core_step = 1 - 2 * core
    deltas = [s * (1 - 2 * lax.rem(me // s, 2)) for s in STRIDES]
    partner = me + core_step
    peers = [me + d for d in deltas]

    barrier = pltpu.get_barrier_semaphore()
    for dev in (partner, *peers):
        pl.semaphore_signal(barrier, inc=1, device_id=(dev,), device_id_type=MESH_ID)

    def offset(color, t):
        unit = t // PARTS
        f1 = 1 - unit // 4
        f2 = 1 - lax.rem(unit // 2, 2)
        f3 = 1 - lax.rem(unit, 2)
        d1, d2, d3 = (deltas[(color + k) % 3] for k in range(3))
        owner = me + f1 * d1 + f2 * d2 + f3 * d3
        return owner * piece + (color * PARTS + lax.rem(t, PARTS)) * chunk

    def cut(ref, start):
        return ref.at[:, pl.ds(pl.multiple_of(start, 1024), chunk)]

    def swap(color, t):
        return pltpu.make_async_remote_copy(
            src_ref=cut(g, offset(color, t) + core_step * piece),
            dst_ref=cut(pg, (color * STEPS + t) * chunk),
            send_sem=ds_sem.at[color * 4 + lax.rem(t, 4)],
            recv_sem=dr_sem.at[color * STEPS + t],
            device_id=(partner,), device_id_type=MESH_ID)

    def swap_early(color, t):
        k = color * 2 + t
        return pltpu.make_async_remote_copy(
            src_ref=cut(g, offset(color, t) + core_step * piece), dst_ref=b_buf.at[k],
            send_sem=ds_sem.at[color * 4 + t], recv_sem=dr_sem.at[color * STEPS + t],
            device_id=(partner,), device_id_type=MESH_ID)

    def swap_cut(color, i):
        start = pl.multiple_of(offset(color, 0) + core_step * piece + i * part, 1024)
        return pltpu.make_async_remote_copy(
            src_ref=g.at[:, pl.ds(start, part)], dst_ref=b_buf.at[color * 2, :, pl.ds(i * part, part)],
            send_sem=ds_sem.at[color * 4], recv_sem=dc_sem.at[color * CUTS + i],
            device_id=(partner,), device_id_type=MESH_ID)

    def push_cut(color, i):
        k, j = color * 3, color * 4 * PARTS
        s = pl.ds(i * part, part)
        return push(stage.at[k, :, s], r1.at[j, :, s], s1_sem.at[k], r1_sem.at[j], color)

    def load_a(color, t):
        k = color * 2 + lax.rem(t, 2)
        return pltpu.make_async_copy(cut(g, offset(color, t)), a_buf.at[k], a_sem.at[k])

    def load_b(color, t):
        k = color * 2 + lax.rem(t, 2)
        return pltpu.make_async_copy(cut(pg, (color * STEPS + t) * chunk), b_buf.at[k], b_sem.at[k])

    def push(src, dst, send_sem, recv_sem, axis):
        return pltpu.make_async_remote_copy(
            src_ref=src, dst_ref=dst, send_sem=send_sem, recv_sem=recv_sem,
            device_id=(peers[axis],), device_id_type=MESH_ID)

    def push1(color, t):
        k = color * 3 + lax.rem(t, 3)
        j = color * 4 * PARTS + t
        return push(stage.at[k], r1.at[j], s1_sem.at[k], r1_sem.at[j], color)

    def push2(color, t):
        j = color * 2 * PARTS + t - 4 * PARTS
        return push(r1.at[color * 4 * PARTS + t - 4 * PARTS], r2.at[j], s2_sem.at[j], r2_sem.at[j], (color + 1) % 3)

    def push3(color, t):
        j = color * PARTS + t - 6 * PARTS
        return push(r1.at[color * 4 * PARTS + t - 4 * PARTS], r3.at[j], s3_sem.at[j], r3_sem.at[j], (color + 2) % 3)

    def store(color, t):
        j = color * PARTS + t - 7 * PARTS
        return pltpu.make_async_copy(r3.at[j], cut(out, j * chunk), o_sem.at[j])

    def add_up(color, t, dst, extra, last=False, span=None):
        k = color * 2 + lax.rem(t, 2)
        first, count = span or (0, chunk)

        @pl.loop(first // width, (first + count) // width)
        def _(i):
            s = pl.ds(pl.multiple_of(i * width, width), width)
            acc = a_buf[k, :, s].astype(jnp.float32) + b_buf[k, :, s].astype(jnp.float32)
            for ref, j in extra:
                acc = acc + ref[j, :, s]
            if last:
                acc = acc * MEAN_SCALE
                squares[...] += acc * acc
            dst[0][dst[1], :, s] = acc

    def half(ref, which):
        return ref.at[:, pl.ds(pl.multiple_of(which * n_half, 1024), n_half)]

    def vec_push(k):
        src = half(v_full, 1 - core) if k == 0 else half(v_mean, core) if k == 4 else v_acc.at[k]
        return pltpu.make_async_remote_copy(
            src_ref=src, dst_ref=half(v_mean, core) if k == 4 else v_get.at[k],
            send_sem=vs_sem.at[k], recv_sem=vr_sem.at[k],
            device_id=((partner, *peers, partner)[k],), device_id_type=MESH_ID)

    def norm_push(k):
        return pltpu.make_async_remote_copy(
            src_ref=n_put, dst_ref=n_get.at[me], send_sem=ns_sem, recv_sem=nr_sem,
            device_id=(lax.rem(me + k, DEVICES),), device_id_type=MESH_ID)

    def vec_loop(count, body):
        @pl.loop(0, count // 1024)
        def _(i):
            body(pl.multiple_of(i * 1024, 1024))

    def vec_turn(k):
        def body(i):
            s = pl.ds(i, 1024)
            here = pl.ds(pl.multiple_of(core * n_half + i, 1024), 1024)
            total = (v_acc[k, :, s] if k else v_full[:, here]) + v_get[k, :, s]
            if k < 3:
                v_acc[k + 1, :, s] = total
            else:
                v_mean[:, here] = total * MEAN_SCALE
        vec_push(k).wait_recv()
        vec_loop(n_half, body)
        vec_push(k + 1).start()

    def ready(color, t):
        load_a(color, t).wait()
        load_b(color, t).wait()

    def refill(color, t):
        load_a(color, t).start()
        swap(color, t).wait_recv()
        load_b(color, t).start()

    def more_swap(color, t):
        swap(color, t - 4).wait_send()
        swap(color, t).start()

    for t in range(2):
        for color in range(COLORS):
            load_a(color, t).start()
    vec_load = pltpu.make_async_copy(gv, v_in, vi_sem)
    vec_load.start()
    lr_load = pltpu.make_async_copy(lr, lr_smem, lr_sem)
    lr_load.start()
    squares[...] = jnp.zeros_like(squares)
    pl.semaphore_wait(barrier, 4)
    for i in range(CUTS):
        for color in range(COLORS):
            swap_cut(color, i).start()
    for color in range(COLORS):
        swap_early(color, 1).start()
    for t in range(2, 4):
        for color in range(COLORS):
            swap(color, t).start()
    for i in range(CUTS):
        for color in range(COLORS):
            if i == 0:
                load_a(color, 0).wait()
            swap_cut(color, i).wait_recv()
            add_up(color, 0, (stage, color * 3), (), span=(i * part, part))
            push_cut(color, i).start()
    for color in range(COLORS):
        more_swap(color, 4)
        refill(color, 2)

    def phase_one(t, first, early=False):
        for color in range(COLORS):
            if early:
                load_a(color, t).wait()
                swap_early(color, t).wait_recv()
            else:
                ready(color, t)
            if not first:
                push1(color, t - 3).wait_send()
            add_up(color, t, (stage, color * 3 + lax.rem(t, 3)), ())
            push1(color, t).start()
            more_swap(color, t + 4)
            refill(color, t + 2)

    def run(lo, hi, body):
        lax.fori_loop(lo, hi, lambda t, c: (body(t), c)[1], 0)

    phase_one(1, True, True)
    phase_one(2, True)
    vec_load.wait()

    def widen(i):
        s = pl.ds(i, 1024)
        v_full[:, s] = v_in[:, s].astype(jnp.float32)

    vec_loop(n_vec, widen)
    vec_push(0).start()
    for k in range(4):
        run(3 * k + 3, 3 * k + 6, lambda t: phase_one(t, False))
        vec_turn(k)
    run(15, 4 * PARTS, lambda t: phase_one(t, False))
    vec_push(4).wait_recv()
    vec_store = pltpu.make_async_copy(v_mean, vec_out, vo_sem)
    vec_store.start()

    def phase_two(t):
        for color in range(COLORS):
            ready(color, t)
            j = color * 4 * PARTS + t - 4 * PARTS
            push1(color, t - 4 * PARTS).wait_recv()
            add_up(color, t, (r1, j), ((r1, j),))
            push2(color, t).start()
            more_swap(color, t + 4)
            refill(color, t + 2)

    run(4 * PARTS, 6 * PARTS, phase_two)

    def phase_three(t):
        for color in range(COLORS):
            ready(color, t)
            j = color * 4 * PARTS + t - 4 * PARTS
            push1(color, t - 4 * PARTS).wait_recv()
            push2(color, t - 2 * PARTS).wait_recv()
            add_up(color, t, (r1, j), ((r1, j), (r2, color * 2 * PARTS + t - 6 * PARTS)))
            push3(color, t).start()
            more_swap(color, t + 4)
            refill(color, t + 2)

    run(6 * PARTS, 7 * PARTS, phase_three)

    def phase_four(t, fill):
        for color in range(COLORS):
            ready(color, t)
            push1(color, t - 4 * PARTS).wait_recv()
            push2(color, t - 2 * PARTS).wait_recv()
            push3(color, t - PARTS).wait_recv()
            add_up(color, t, (r3, color * PARTS + t - 7 * PARTS), (
                (r1, color * 4 * PARTS + t - 4 * PARTS),
                (r2, color * 2 * PARTS + t - 6 * PARTS),
                (r3, color * PARTS + t - 7 * PARTS)), last=True)
            store(color, t).start()
            if fill:
                refill(color, t + 2)

    run(7 * PARTS, 7 * PARTS + 2, lambda t: phase_four(t, True))
    run(7 * PARTS + 2, STEPS, lambda t: phase_four(t, False))

    vec_sq = jnp.sum(v_mean[...] * v_mean[...], axis=1, keepdims=True)
    mine = jnp.broadcast_to(jnp.sum(squares[...], axis=1, keepdims=True), (1, 128))
    n_put[...] = mine
    n_get[me] = mine
    for k in range(1, DEVICES):
        norm_push(k).start()
    rest = pltpu.make_async_remote_copy(
        src_ref=n_get.at[pl.ds(0, DEVICES - 1)], dst_ref=n_get.at[pl.ds(0, DEVICES - 1)],
        send_sem=ns_sem, recv_sem=nr_sem, device_id=(partner,), device_id_type=MESH_ID)
    rest.wait_recv()
    norm_sq = n_get[0]
    for k in range(1, DEVICES):
        norm_sq = norm_sq + n_get[k]
    norm_sq = norm_sq + vec_sq
    scale_buf[0:1, :] = jnp.minimum(1.0, MAX_NORM / (jnp.sqrt(norm_sq) + NORM_EPS))
    lr_load.wait()
    scale_buf[1:2, :] = jnp.full((1, 128), lr_smem[0, 0])
    scale_store = pltpu.make_async_copy(scale_buf, scale_out, so_sem)
    scale_store.start()

    def drain(lo, hi, wait):
        def body(t):
            for color in range(COLORS):
                wait(color, t)
        run(lo, hi, body)

    drain(4 * PARTS - 3, 4 * PARTS, lambda c, t: push1(c, t).wait_send())
    drain(4 * PARTS, 6 * PARTS, lambda c, t: push2(c, t).wait_send())
    drain(6 * PARTS, 7 * PARTS, lambda c, t: push3(c, t).wait_send())
    drain(STEPS - 4, STEPS, lambda c, t: swap(c, t).wait_send())
    drain(7 * PARTS, STEPS, lambda c, t: store(c, t).wait())
    for k in range(5):
        vec_push(k).wait_send()
    rest.wait_send()
    vec_store.wait()
    scale_store.wait()


def scatter_sum(g_mat, g_vec, learn_rate, axis_name, group_size):
    total = g_mat.shape[1]
    n_vec = g_vec.shape[1]
    piece = total // group_size
    chunk = piece // (COLORS * PARTS)
    dma = pltpu.SemaphoreType.DMA
    any_spec = pl.BlockSpec(memory_space=pl.ANY)
    out, _, vec, scales = pl.pallas_call(
        functools.partial(scatter_kernel, axis_name, piece),
        out_shape=(jax.ShapeDtypeStruct((1, piece), jnp.float32),
                   jax.ShapeDtypeStruct((1, total // 2), jnp.bfloat16),
                   jax.ShapeDtypeStruct((1, n_vec), jnp.float32),
                   jax.ShapeDtypeStruct((2, 128), jnp.float32)),
        in_specs=[any_spec] * 3,
        out_specs=[any_spec] * 4,
        scratch_shapes=[
            pltpu.VMEM((2 * COLORS, 1, chunk), jnp.bfloat16),
            pltpu.VMEM((2 * COLORS, 1, chunk), jnp.bfloat16),
            pltpu.VMEM((3 * COLORS, 1, chunk), jnp.float32),
            pltpu.VMEM((4 * PARTS * COLORS, 1, chunk), jnp.float32),
            pltpu.VMEM((2 * PARTS * COLORS, 1, chunk), jnp.float32),
            pltpu.VMEM((PARTS * COLORS, 1, chunk), jnp.float32),
            pltpu.VMEM((1, n_vec), jnp.bfloat16),
            pltpu.VMEM((1, n_vec), jnp.float32),
            pltpu.VMEM((4, 1, n_vec // 2), jnp.float32),
            pltpu.VMEM((4, 1, n_vec // 2), jnp.float32),
            pltpu.VMEM((1, n_vec), jnp.float32),
            pltpu.VMEM((1, 128), jnp.float32),
            pltpu.VMEM((DEVICES, 1, 128), jnp.float32),
            pltpu.VMEM((1, min(chunk // CUTS, WIDTH)), jnp.float32),
            pltpu.SMEM((1, 1), jnp.float32),
            pltpu.VMEM((2, 128), jnp.float32),
            dma((2 * COLORS,)), dma((2 * COLORS,)),
            dma((4 * COLORS,)), dma((STEPS * COLORS,)), dma((CUTS * COLORS,)),
            dma((3 * COLORS,)), dma((4 * PARTS * COLORS,)),
            dma((2 * PARTS * COLORS,)), dma((2 * PARTS * COLORS,)),
            dma((PARTS * COLORS,)), dma((PARTS * COLORS,)),
            dma((PARTS * COLORS,)),
            dma, dma((5,)), dma((5,)), dma, dma, dma, dma, dma,
        ],
        compiler_params=pltpu.CompilerParams(
            collective_id=0, has_side_effects=True, vmem_limit_bytes=63 * 1024 * 1024),
        name="scatter_sum",
    )(g_mat, g_vec, learn_rate.reshape(1, 1))
    return out, vec, scales


def adam_moments(grad, m, v):
    new_m = ADAM_BETA1 * m + (1.0 - ADAM_BETA1) * grad
    new_v = ADAM_BETA2 * v + (1.0 - ADAM_BETA2) * grad * grad
    return new_m, new_v


def adam_param(p, m, v, rate, decay):
    direction = (m / BIAS_ONE) / (jnp.sqrt(v / BIAS_TWO) + ADAM_EPS)
    return p - rate * (direction + decay * p)


def gather_kernel(axis_name, grad, p, m, v, scales_in, out, m_out, v_out, g_buf, p_buf, scales,
                  scales_sem, g_sem, p_sem, m_sem, v_sem, s_sem, r_sem, ds_sem, dr_sem):
    own = COLORS * PARTS
    rows = p.shape[1]
    step = min(rows, ROWS)
    me = lax.axis_index(axis_name)
    deltas = [s * (1 - 2 * lax.rem(me // s, 2)) for s in STRIDES]
    partner = me + 1 - 2 * lax.rem(me, 2)
    peers = [me + d for d in deltas]

    barrier = pltpu.get_barrier_semaphore()
    for dev in (partner, *peers):
        pl.semaphore_signal(barrier, inc=1, device_id=(dev,), device_id_type=MESH_ID)

    def loads(color, q):
        i = color * PARTS + q
        return (pltpu.make_async_copy(grad.at[i], g_buf.at[color], g_sem.at[color]),
                pltpu.make_async_copy(m.at[i], m_out.at[i], m_sem.at[i]),
                pltpu.make_async_copy(v.at[i], v_out.at[i], v_sem.at[i]),
                pltpu.make_async_copy(p.at[i], p_buf.at[color], p_sem.at[color]))

    def across(index):
        return pltpu.make_async_remote_copy(
            src_ref=out.at[index], dst_ref=out.at[index], send_sem=ds_sem, recv_sem=dr_sem,
            device_id=(partner,), device_id_type=MESH_ID)

    def route(stage, axis):
        b1, b2 = (axis - 2) % 3, (axis - 1) % 3
        color = (axis, b2, b2, b1, b1, b1, b1)[stage]
        flips = ((), (), (b2,), (), (b1,), (b2,), (b1, b2))[stage]
        return color, sum((deltas[f] for f in flips), me)

    def push(stage, axis, q):
        color, owner = route(stage, axis)
        index = owner * own + color * PARTS + q
        k = (stage * 3 + axis) * PARTS + q
        return pltpu.make_async_remote_copy(
            src_ref=out.at[index], dst_ref=out.at[index], send_sem=s_sem.at[k], recv_sem=r_sem.at[k],
            device_id=(peers[axis],), device_id_type=MESH_ID)

    def land(stage, axis, q):
        color, owner = route(stage, axis)
        push(stage, axis, q).wait_recv()
        across((owner + deltas[axis]) * own + color * PARTS + q).start()

    def update(color, q):
        i = color * PARTS + q

        @pl.loop(0, rows // step)
        def _(r):
            s = pl.ds(pl.multiple_of(r * step, step), step)
            new_m, new_v = adam_moments(g_buf[color, s, :] * scales[0:1, :], m_out[i, s, :], v_out[i, s, :])
            m_out[i, s, :] = new_m
            v_out[i, s, :] = new_v
            new_p = adam_param(p_buf[color, s, :], new_m, new_v, scales[1:2, :], WEIGHT_DECAY)
            out[me * own + i, s, :] = new_p.astype(jnp.bfloat16)

    def each(count, body):
        lax.fori_loop(0, count, lambda i, c: (body(i), c)[1], 0)

    scales_load = pltpu.make_async_copy(scales_in, scales, scales_sem)
    scales_load.start()
    for color in range(COLORS):
        for copy in loads(color, 0):
            copy.start()
    scales_load.wait()
    for q in range(PARTS):
        for color in range(COLORS):
            for copy in loads(color, q):
                copy.wait()
            update(color, q)
            if q == 0 and color == 0:
                pl.semaphore_wait(barrier, 4)
            push(0, color, q).start()
            push(1, (color + 1) % 3, q).start()
            across(me * own + color * PARTS + q).start()
            if q + 1 < PARTS:
                for copy in loads(color, q + 1):
                    copy.start()
        if q >= 2:
            for axis in range(3):
                land(0, axis, q - 2)
                land(1, axis, q - 2)
    for q in range(PARTS):
        for axis in range(3):
            push(2, axis, q).start()
            land(q % 2, axis, 2 + q // 2)
    for stage in range(3, 8):
        def body(q, stage=stage):
            for axis in range(3):
                if stage < 7:
                    push(stage, axis, q).start()
                land(stage - 1, axis, q)
        each(PARTS, body)

    for stage in range(7):
        def body(q, stage=stage):
            for axis in range(3):
                push(stage, axis, q).wait_send()
        each(PARTS, body)
    half = pltpu.make_async_remote_copy(
        src_ref=out.at[pl.ds(0, 8 * own)], dst_ref=out.at[pl.ds(0, 8 * own)], send_sem=ds_sem, recv_sem=dr_sem,
        device_id=(partner,), device_id_type=MESH_ID)
    half.wait_recv()
    half.wait_send()


def write_kernel(held, m_held, v_held, p, scales_in, g_vec, p_vec, m_vec, v_vec,
                 out, p_out, m_out, v_out, pv_out, mv_out, vv_out,
                 p_buf, vec_buf, scales, in_sem, out_sem, sem, vec_sem, vec_out_sem, scales_sem):
    own, rows, _ = p.shape
    step = min(rows, ROWS)
    span = held.shape[0] // own

    def load(i):
        return pltpu.make_async_copy(p.at[i], p_buf.at[i % RING], in_sem.at[i % RING])

    def store(i):
        return pltpu.make_async_copy(p_buf.at[i % RING], p_out.at[i], out_sem.at[i % RING])

    def copies(i):
        part = pl.ds(i * span, span)
        return (pltpu.make_async_copy(held.at[part], out.at[part], sem.at[0, i]),
                pltpu.make_async_copy(m_held.at[i], m_out.at[i], sem.at[1, i]),
                pltpu.make_async_copy(v_held.at[i], v_out.at[i], sem.at[2, i]))

    scales_load = pltpu.make_async_copy(scales_in, scales, scales_sem)
    scales_load.start()
    vec_loads = [pltpu.make_async_copy(a, vec_buf.at[k], vec_sem.at[k])
                 for k, a in enumerate((p_vec, m_vec, v_vec, g_vec))]
    vec_stores = [pltpu.make_async_copy(vec_buf.at[k], a, vec_out_sem.at[k])
                  for k, a in enumerate((pv_out, mv_out, vv_out))]
    def vec_update():
        for copy in vec_loads:
            copy.wait()

        @pl.loop(0, g_vec.shape[1] // 1024)
        def _(i):
            s = pl.ds(pl.multiple_of(i * 1024, 1024), 1024)
            new_m, new_v = adam_moments(vec_buf[3, :, s] * scales[0:1, 0:1], vec_buf[1, :, s], vec_buf[2, :, s])
            vec_buf[1, :, s] = new_m
            vec_buf[2, :, s] = new_v
            vec_buf[0, :, s] = adam_param(vec_buf[0, :, s], new_m, new_v, scales[1:2, 0:1], 0.0)

        for copy in vec_stores:
            copy.start()

    for i in range(RING - 1):
        load(i).start()
    for copy in vec_loads:
        copy.start()
    for i in range(AHEAD):
        for copy in copies(i):
            copy.start()
    scales_load.wait()
    for i in range(own):
        load(i).wait()

        @pl.loop(0, rows // step)
        def _(r):
            s = pl.ds(pl.multiple_of(r * step, step), step)
            p_buf[i % RING, s, :] = adam_param(
                p_buf[i % RING, s, :], m_held[i, s, :], v_held[i, s, :], scales[1:2, :], WEIGHT_DECAY)

        store(i).start()
        if i + RING - 1 < own:
            if i:
                store(i - 1).wait()
            load(i + RING - 1).start()
        if i + AHEAD < own:
            for copy in copies(i):
                copy.wait()
            for copy in copies(i + AHEAD):
                copy.start()
        if i == 0:
            vec_update()

    for i in range(own - RING, own):
        store(i).wait()
    for i in range(own - AHEAD, own):
        for copy in copies(i):
            copy.wait()
    for copy in vec_stores:
        copy.wait()


def gather_update(grad, p, m, v, scales, grad_vec, p_vec, m_vec, v_vec, axis_name, group_size):
    own = COLORS * PARTS
    piece = p.shape[0]
    n_vec = p_vec.shape[0]
    rows = piece // (own * 128)
    dma = pltpu.SemaphoreType.DMA
    any_spec = pl.BlockSpec(memory_space=pl.ANY)
    vmem_spec = pl.BlockSpec(memory_space=pltpu.VMEM)
    grad, p, m, v = (a.reshape(own, rows, 128) for a in (grad, p, m, v))
    p_vec, m_vec, v_vec = (a.reshape(1, n_vec) for a in (p_vec, m_vec, v_vec))
    full, new_m, new_v = pl.pallas_call(
        functools.partial(gather_kernel, axis_name),
        out_shape=(pltpu.VMEM((group_size * own, rows, 128), jnp.bfloat16),
                   pltpu.VMEM((own, rows, 128), jnp.float32),
                   pltpu.VMEM((own, rows, 128), jnp.float32)),
        in_specs=[any_spec] * 5,
        out_specs=[vmem_spec] * 3,
        scratch_shapes=[
            pltpu.VMEM((COLORS, rows, 128), jnp.float32), pltpu.VMEM((COLORS, rows, 128), jnp.float32),
            pltpu.VMEM((2, 128), jnp.float32), dma, dma((COLORS,)), dma((COLORS,)), dma((own,)), dma((own,)),
            dma((7 * 3 * PARTS,)), dma((7 * 3 * PARTS,)), dma, dma],
        compiler_params=pltpu.CompilerParams(
            collective_id=1, has_side_effects=True, vmem_limit_bytes=SMALL_VMEM),
        name="gather_update",
    )(grad, p, m, v, scales)
    flat = jax.ShapeDtypeStruct((own, rows, 128), jnp.float32)
    line = jax.ShapeDtypeStruct((1, n_vec), jnp.float32)
    full, new_p, new_m, new_v, *vecs = pl.pallas_call(
        write_kernel,
        out_shape=(jax.ShapeDtypeStruct(full.shape, full.dtype), flat, flat, flat, line, line, line),
        in_specs=[vmem_spec] * 3 + [any_spec] * 6,
        out_specs=[any_spec] * 7,
        scratch_shapes=[
            pltpu.VMEM((RING, rows, 128), jnp.float32), pltpu.VMEM((4, 1, n_vec), jnp.float32),
            pltpu.VMEM((2, 128), jnp.float32),
            dma((RING,)), dma((RING,)), dma((3, own)), dma((4,)), dma((3,)), dma],
        compiler_params=pltpu.CompilerParams(vmem_limit_bytes=SMALL_VMEM),
        name="write_out",
    )(*(pltpu.with_memory_space_constraint(a, pltpu.VMEM) for a in (full, new_m, new_v)),
      p, scales, grad_vec, p_vec, m_vec, v_vec)
    return (*(a.reshape(piece) for a in (new_p, new_m, new_v)), *(a.reshape(n_vec) for a in vecs),
            full.reshape(group_size * piece))


def solution(mesh):
    axis_name = mesh.axis_names[0]
    group_size = mesh.shape[axis_name]

    def local_step(g_mat, g_vec, p_mat, m_mat, v_mat, p_vec, m_vec, v_vec, learn_rate):
        grad_mat, grad_vec, scales = scatter_sum(g_mat, g_vec, learn_rate, axis_name, group_size)
        return gather_update(grad_mat, p_mat, m_mat, v_mat, scales, grad_vec, p_vec, m_vec, v_vec, axis_name, group_size)

    return jax.shard_map(
        local_step,
        mesh=mesh,
        in_specs=(P(axis_name, None), P(axis_name, None), P(axis_name), P(axis_name), P(axis_name), P(), P(), P(), P()),
        out_specs=(P(axis_name), P(axis_name), P(axis_name), P(), P(), P(), P()),
        check_vma=False,
    )
```

```python
import functools

import jax
import jax.numpy as jnp
from jax import lax
from jax.experimental import pallas as pl
from jax.experimental.pallas import tpu as pltpu
from jax.sharding import PartitionSpec as P

STEP = 10
ADAM_BETA1 = 0.9
ADAM_BETA2 = 0.98
ADAM_EPS = 1e-8
WEIGHT_DECAY = 0.01
MAX_NORM = 1.0
NORM_EPS = 1e-6
BIAS_ONE = 1.0 - ADAM_BETA1 ** STEP
BIAS_TWO = 1.0 - ADAM_BETA2 ** STEP

MESH_ID = pl.DeviceIdType.MESH
COLORS = 3
PARTS = 4
STRIDES = (2, 4, 8)
STEPS = 8 * PARTS
DEVICES = 16
WIDTH = 4096
ROWS = 64
SMALL_VMEM = 3400 * 1024
RING = 5
AHEAD = 2
CUTS = 4
MEAN_SCALE = 1.0 / 16.0


def scatter_kernel(axis_name, piece, g, gv, lr, out, pg, vec_out, scale_out,
                   a_buf, b_buf, e_buf, stage, r1, r2, r3, v_in, v_full, v_acc, v_get, v_mean, n_put, n_get, squares, lr_smem, scale_buf,
                   a_sem, b_sem, e_sem, ds_sem, dr_sem, dc_sem, s1_sem, r1_sem, s2_sem, r2_sem, s3_sem, r3_sem, rc_sem, o_sem,
                   vi_sem, vs_sem, vr_sem, ns_sem, nr_sem, vo_sem, lr_sem, so_sem):
    chunk = piece // (COLORS * PARTS)
    width = min(chunk // CUTS, WIDTH)
    part = chunk // CUTS
    n_vec = gv.shape[1]
    n_half = n_vec // 2
    me = lax.axis_index(axis_name)
    core = lax.rem(me, 2)
    core_step = 1 - 2 * core
    deltas = [s * (1 - 2 * lax.rem(me // s, 2)) for s in STRIDES]
    partner = me + core_step
    peers = [me + d for d in deltas]

    barrier = pltpu.get_barrier_semaphore()
    for dev in (partner, *peers):
        pl.semaphore_signal(barrier, inc=1, device_id=(dev,), device_id_type=MESH_ID)

    def offset(color, t):
        unit = t // PARTS
        f1 = 1 - unit // 4
        f2 = 1 - lax.rem(unit // 2, 2)
        f3 = 1 - lax.rem(unit, 2)
        d1, d2, d3 = (deltas[(color + k) % 3] for k in range(3))
        owner = me + f1 * d1 + f2 * d2 + f3 * d3
        return owner * piece + (color * PARTS + lax.rem(t, PARTS)) * chunk

    def cut(ref, start):
        return ref.at[:, pl.ds(pl.multiple_of(start, 1024), chunk)]

    def swap(color, t):
        return pltpu.make_async_remote_copy(
            src_ref=cut(g, offset(color, t) + core_step * piece),
            dst_ref=cut(pg, (color * STEPS + t) * chunk),
            send_sem=ds_sem.at[color * 4 + lax.rem(t, 4)],
            recv_sem=dr_sem.at[color * 8 + lax.rem(t, 8)],
            device_id=(partner,), device_id_type=MESH_ID)

    def swap_early(color, t):
        k = color * 2 + t
        return pltpu.make_async_remote_copy(
            src_ref=cut(g, offset(color, t) + core_step * piece), dst_ref=b_buf.at[k],
            send_sem=ds_sem.at[color * 4 + t], recv_sem=dr_sem.at[color * 8 + t],
            device_id=(partner,), device_id_type=MESH_ID)

    def swap_cut(color, i):
        s = pl.ds(i * part, part)
        return pltpu.make_async_remote_copy(
            src_ref=e_buf.at[color, :, s], dst_ref=b_buf.at[color * 2, :, s],
            send_sem=ds_sem.at[color * 4], recv_sem=dc_sem.at[color * CUTS + i],
            device_id=(partner,), device_id_type=MESH_ID)

    def load_e(color):
        return pltpu.make_async_copy(
            cut(g, offset(color, 0) + core_step * piece), e_buf.at[color], e_sem.at[color])

    def push_cut(color, i):
        k, j = color * 3, color * 4 * PARTS
        s = pl.ds(i * part, part)
        return push(stage.at[k, :, s], r1.at[j, :, s], s1_sem.at[k], r1_sem.at[color * 4], color)

    def load_a(color, t):
        k = color * 2 + lax.rem(t, 2)
        return pltpu.make_async_copy(cut(g, offset(color, t)), a_buf.at[k], a_sem.at[k])

    def load_b(color, t):
        k = color * 2 + lax.rem(t, 2)
        return pltpu.make_async_copy(cut(pg, (color * STEPS + t) * chunk), b_buf.at[k], b_sem.at[k])

    def push(src, dst, send_sem, recv_sem, axis):
        return pltpu.make_async_remote_copy(
            src_ref=src, dst_ref=dst, send_sem=send_sem, recv_sem=recv_sem,
            device_id=(peers[axis],), device_id_type=MESH_ID)

    def push1(color, t):
        k = color * 3 + lax.rem(t, 3)
        j = color * 4 * PARTS + t
        return push(stage.at[k], r1.at[j], s1_sem.at[k], r1_sem.at[color * 4 + t // PARTS], color)

    def push2(color, t):
        j = color * 2 * PARTS + t - 4 * PARTS
        return push(r1.at[color * 4 * PARTS + t - 4 * PARTS], r2.at[j], s2_sem,
                    r2_sem.at[color * 2 + t // PARTS - 4], (color + 1) % 3)

    def push3(color, t):
        j = color * PARTS + t - 6 * PARTS
        return push(r1.at[color * 4 * PARTS + t - 4 * PARTS], r3.at[j], s3_sem, r3_sem.at[j], (color + 2) % 3)

    def push3_cut(color, i):
        s = pl.ds(i * part, part)
        return push(r1.at[color * 4 * PARTS + 3 * PARTS - 1, :, s], r3.at[color * PARTS + PARTS - 1, :, s],
                    s3_sem, rc_sem.at[color * CUTS + i], (color + 2) % 3)

    def unit1(color, u):
        span = r1.at[pl.ds((color * 4 + u) * PARTS, PARTS)]
        return push(span, span, s2_sem, r1_sem.at[color * 4 + u], color)

    def unit2(color, w):
        span = r2.at[pl.ds((color * 2 + w) * PARTS, PARTS)]
        return push(span, span, s2_sem, r2_sem.at[color * 2 + w], (color + 1) % 3)

    def store(color, t):
        j = color * PARTS + t - 7 * PARTS
        return pltpu.make_async_copy(r3.at[j], cut(out, j * chunk), o_sem)

    def add_up(color, t, dst, extra, last=False, span=None):
        k = color * 2 + lax.rem(t, 2)
        first, count = span or (0, chunk)

        @pl.loop(first // width, (first + count) // width)
        def _(i):
            s = pl.ds(pl.multiple_of(i * width, width), width)
            acc = a_buf[k, :, s].astype(jnp.float32) + b_buf[k, :, s].astype(jnp.float32)
            for ref, j in extra:
                acc = acc + ref[j, :, s]
            if last:
                acc = acc * MEAN_SCALE
                squares[...] += acc * acc
            dst[0][dst[1], :, s] = acc

    def half(ref, which):
        return ref.at[:, pl.ds(pl.multiple_of(which * n_half, 1024), n_half)]

    def vec_push(k):
        src = half(v_full, 1 - core) if k == 0 else half(v_mean, core) if k == 4 else v_acc.at[k]
        return pltpu.make_async_remote_copy(
            src_ref=src, dst_ref=half(v_mean, core) if k == 4 else v_get.at[k],
            send_sem=vs_sem.at[k], recv_sem=vr_sem.at[k],
            device_id=((partner, *peers, partner)[k],), device_id_type=MESH_ID)

    def norm_push(k):
        return pltpu.make_async_remote_copy(
            src_ref=n_put, dst_ref=n_get.at[me], send_sem=ns_sem, recv_sem=nr_sem,
            device_id=(lax.rem(me + k, DEVICES),), device_id_type=MESH_ID)

    def vec_loop(count, body):
        @pl.loop(0, count // 1024)
        def _(i):
            body(pl.multiple_of(i * 1024, 1024))

    def vec_turn(k):
        def body(i):
            s = pl.ds(i, 1024)
            here = pl.ds(pl.multiple_of(core * n_half + i, 1024), 1024)
            total = (v_acc[k, :, s] if k else v_full[:, here]) + v_get[k, :, s]
            if k < 3:
                v_acc[k + 1, :, s] = total
            else:
                v_mean[:, here] = total * MEAN_SCALE
        vec_push(k).wait_recv()
        vec_loop(n_half, body)
        vec_push(k + 1).start()

    def ready(color, t):
        load_a(color, t).wait()
        load_b(color, t).wait()

    def refill(color, t):
        load_a(color, t).start()
        swap(color, t).wait_recv()
        load_b(color, t).start()

    def more_swap(color, t):
        swap(color, t - 4).wait_send()
        swap(color, t).start()

    for color in range(COLORS):
        load_e(color).start()
    for t in range(2):
        for color in range(COLORS):
            load_a(color, t).start()
    vec_load = pltpu.make_async_copy(gv, v_in, vi_sem)
    vec_load.start()
    lr_load = pltpu.make_async_copy(lr, lr_smem, lr_sem)
    lr_load.start()
    squares[...] = jnp.zeros_like(squares)
    for color in range(COLORS):
        load_e(color).wait()
    pl.semaphore_wait(barrier, 4)
    for i in range(CUTS):
        for color in range(COLORS):
            swap_cut(color, i).start()
    for color in range(COLORS):
        swap_early(color, 1).start()
    for t in range(2, 4):
        for color in range(COLORS):
            swap(color, t).start()
    for i in range(CUTS):
        for color in range(COLORS):
            if i == 0:
                load_a(color, 0).wait()
            swap_cut(color, i).wait_recv()
            add_up(color, 0, (stage, color * 3), (), span=(i * part, part))
            push_cut(color, i).start()
    for color in range(COLORS):
        more_swap(color, 4)
        refill(color, 2)

    def phase_one(t, first, early=False):
        for color in range(COLORS):
            if early:
                load_a(color, t).wait()
                swap_early(color, t).wait_recv()
            else:
                ready(color, t)
            if not first:
                push1(color, t - 3).wait_send()
            add_up(color, t, (stage, color * 3 + lax.rem(t, 3)), ())
            push1(color, t).start()
            more_swap(color, t + 4)
            refill(color, t + 2)

    def run(lo, hi, body):
        lax.fori_loop(lo, hi, lambda t, c: (body(t), c)[1], 0)

    phase_one(1, True, True)
    phase_one(2, True)
    vec_load.wait()

    def widen(i):
        s = pl.ds(i, 1024)
        v_full[:, s] = v_in[:, s].astype(jnp.float32)

    vec_loop(n_vec, widen)
    vec_push(0).start()
    for k in range(4):
        run(3 * k + 3, 3 * k + 6, lambda t: phase_one(t, False))
        vec_turn(k)
    run(15, 4 * PARTS, lambda t: phase_one(t, False))
    vec_push(4).wait_recv()
    vec_store = pltpu.make_async_copy(v_mean, vec_out, vo_sem)
    vec_store.start()

    def phase_two(t):
        for color in range(COLORS):
            ready(color, t)
            j = color * 4 * PARTS + t - 4 * PARTS
            add_up(color, t, (r1, j), ((r1, j),))
            push2(color, t).start()
            more_swap(color, t + 4)
            refill(color, t + 2)

    def phase_three(t, cuts):
        for color in range(COLORS):
            ready(color, t)
            j = color * 4 * PARTS + t - 4 * PARTS
            add_up(color, t, (r1, j), ((r1, j), (r2, color * 2 * PARTS + t - 6 * PARTS)))
            if cuts:
                for i in range(CUTS):
                    push3_cut(color, i).start()
            else:
                push3(color, t).start()
            more_swap(color, t + 4)
            refill(color, t + 2)

    def finish(color, t, span=None):
        j = color * PARTS + t - 7 * PARTS
        add_up(color, t, (r3, j), (
            (r1, color * 4 * PARTS + t - 4 * PARTS),
            (r2, color * 2 * PARTS + t - 6 * PARTS),
            (r3, j)), last=True, span=span)

    def phase_four(t, fill):
        for color in range(COLORS):
            ready(color, t)
            push3(color, t - PARTS).wait_recv()
            finish(color, t)
            store(color, t).start()
            if fill:
                refill(color, t + 2)

    for unit in range(4, 8):
        for color in range(COLORS):
            unit1(color, unit - 4).wait_recv()
            if unit >= 6:
                unit2(color, unit - 6).wait_recv()
        lo = unit * PARTS
        if unit < 6:
            run(lo, lo + PARTS, phase_two)
        elif unit == 6:
            run(lo, lo + PARTS - 1, lambda t: phase_three(t, False))
            phase_three(lo + PARTS - 1, True)
        else:
            run(lo, lo + PARTS - 2, lambda t: phase_four(t, True))
            phase_four(lo + PARTS - 2, False)
    for color in range(COLORS):
        ready(color, STEPS - 1)
    for i in range(CUTS):
        for color in range(COLORS):
            push3_cut(color, i).wait_recv()
            finish(color, STEPS - 1, span=(i * part, part))
    for color in range(COLORS):
        store(color, STEPS - 1).start()

    vec_sq = jnp.sum(v_mean[...] * v_mean[...], axis=1, keepdims=True)
    mine = jnp.broadcast_to(jnp.sum(squares[...], axis=1, keepdims=True), (1, 128))
    n_put[...] = mine
    n_get[me] = mine
    for k in range(1, DEVICES):
        norm_push(k).start()
    rest = pltpu.make_async_remote_copy(
        src_ref=n_get.at[pl.ds(0, DEVICES - 1)], dst_ref=n_get.at[pl.ds(0, DEVICES - 1)],
        send_sem=ns_sem, recv_sem=nr_sem, device_id=(partner,), device_id_type=MESH_ID)
    rest.wait_recv()
    norm_sq = n_get[0]
    for k in range(1, DEVICES):
        norm_sq = norm_sq + n_get[k]
    norm_sq = norm_sq + vec_sq
    scale_buf[0:1, :] = jnp.minimum(1.0, MAX_NORM / (jnp.sqrt(norm_sq) + NORM_EPS))
    lr_load.wait()
    scale_buf[1:2, :] = jnp.full((1, 128), lr_smem[0])
    scale_store = pltpu.make_async_copy(scale_buf, scale_out, so_sem)
    scale_store.start()

    def drain(lo, hi, wait):
        def body(t):
            for color in range(COLORS):
                wait(color, t)
        run(lo, hi, body)

    drain(4 * PARTS - 3, 4 * PARTS, lambda c, t: push1(c, t).wait_send())
    push(r2, r2, s2_sem, r2_sem.at[0], 0).wait_send()
    push(r3, r3, s3_sem, r3_sem.at[0], 0).wait_send()
    drain(STEPS - 4, STEPS, lambda c, t: swap(c, t).wait_send())
    pltpu.make_async_copy(out, out, o_sem).wait()
    for k in range(5):
        vec_push(k).wait_send()
    rest.wait_send()
    vec_store.wait()
    scale_store.wait()


def scatter_sum(g_mat, g_vec, learn_rate, axis_name, group_size):
    total = g_mat.shape[1]
    n_vec = g_vec.shape[1]
    piece = total // group_size
    chunk = piece // (COLORS * PARTS)
    dma = pltpu.SemaphoreType.DMA
    any_spec = pl.BlockSpec(memory_space=pl.ANY)
    out, _, vec, scales = pl.pallas_call(
        functools.partial(scatter_kernel, axis_name, piece),
        out_shape=(jax.ShapeDtypeStruct((1, piece), jnp.float32),
                   jax.ShapeDtypeStruct((1, total // 2), jnp.bfloat16),
                   jax.ShapeDtypeStruct((1, n_vec), jnp.float32),
                   jax.ShapeDtypeStruct((2, 128), jnp.float32)),
        in_specs=[any_spec] * 3,
        out_specs=[any_spec] * 4,
        scratch_shapes=[
            pltpu.VMEM((2 * COLORS, 1, chunk), jnp.bfloat16),
            pltpu.VMEM((2 * COLORS, 1, chunk), jnp.bfloat16),
            pltpu.VMEM((COLORS, 1, chunk), jnp.bfloat16),
            pltpu.VMEM((3 * COLORS, 1, chunk), jnp.float32),
            pltpu.VMEM((4 * PARTS * COLORS, 1, chunk), jnp.float32),
            pltpu.VMEM((2 * PARTS * COLORS, 1, chunk), jnp.float32),
            pltpu.VMEM((PARTS * COLORS, 1, chunk), jnp.float32),
            pltpu.VMEM((1, n_vec), jnp.bfloat16),
            pltpu.VMEM((1, n_vec), jnp.float32),
            pltpu.VMEM((4, 1, n_vec // 2), jnp.float32),
            pltpu.VMEM((4, 1, n_vec // 2), jnp.float32),
            pltpu.VMEM((1, n_vec), jnp.float32),
            pltpu.VMEM((1, 128), jnp.float32),
            pltpu.VMEM((DEVICES, 1, 128), jnp.float32),
            pltpu.VMEM((1, min(chunk // CUTS, WIDTH)), jnp.float32),
            pltpu.SMEM((1,), jnp.float32),
            pltpu.VMEM((2, 128), jnp.float32),
            dma((2 * COLORS,)), dma((2 * COLORS,)), dma((COLORS,)),
            dma((4 * COLORS,)), dma((8 * COLORS,)), dma((CUTS * COLORS,)),
            dma((3 * COLORS,)), dma((4 * COLORS,)), dma, dma((2 * COLORS,)),
            dma, dma((PARTS * COLORS,)), dma((CUTS * COLORS,)), dma,
            dma, dma((5,)), dma((5,)), dma, dma, dma, dma, dma,
        ],
        compiler_params=pltpu.CompilerParams(
            collective_id=0, has_side_effects=True, vmem_limit_bytes=63 * 1024 * 1024),
        name="scatter_sum",
    )(g_mat, g_vec, learn_rate.reshape(1))
    return out, vec, scales


def adam_moments(grad, m, v):
    new_m = ADAM_BETA1 * m + (1.0 - ADAM_BETA1) * grad
    new_v = ADAM_BETA2 * v + (1.0 - ADAM_BETA2) * grad * grad
    return new_m, new_v


def adam_param(p, m, v, rate, decay):
    direction = (m / BIAS_ONE) / (jnp.sqrt(v / BIAS_TWO) + ADAM_EPS)
    return p - rate * (direction + decay * p)


def gather_kernel(axis_name, grad, p, m, v, scales_in, out, m_out, v_out, g_buf, p_buf, scales,
                  scales_sem, g_sem, p_sem, m_sem, v_sem, s_sem, r_sem, ds_sem, dr_sem):
    own = COLORS * PARTS
    rows = p.shape[1]
    part = rows // CUTS
    step = min(part, ROWS)
    me = lax.axis_index(axis_name)
    deltas = [s * (1 - 2 * lax.rem(me // s, 2)) for s in STRIDES]
    partner = me + 1 - 2 * lax.rem(me, 2)
    peers = [me + d for d in deltas]

    barrier = pltpu.get_barrier_semaphore()
    for dev in (partner, *peers):
        pl.semaphore_signal(barrier, inc=1, device_id=(dev,), device_id_type=MESH_ID)

    def loads(color, q):
        i = color * PARTS + q
        return (pltpu.make_async_copy(grad.at[i], g_buf.at[color], g_sem.at[color]),
                pltpu.make_async_copy(m.at[i], m_out.at[i], m_sem.at[color]),
                pltpu.make_async_copy(v.at[i], v_out.at[i], v_sem.at[color]),
                pltpu.make_async_copy(p.at[i], p_buf.at[color], p_sem.at[color]))

    def across(index):
        return pltpu.make_async_remote_copy(
            src_ref=out.at[index], dst_ref=out.at[index], send_sem=ds_sem, recv_sem=dr_sem,
            device_id=(partner,), device_id_type=MESH_ID)

    def route(stage, axis):
        b1, b2 = (axis - 2) % 3, (axis - 1) % 3
        color = (axis, b2, b2, b1, b1, b1, b1)[stage]
        flips = ((), (), (b2,), (), (b1,), (b2,), (b1, b2))[stage]
        return color, sum((deltas[f] for f in flips), me)

    def push(stage, axis, q, span=None):
        color, owner = route(stage, axis)
        index = owner * own + color * PARTS + q
        place = 2 * q + stage if stage < 2 else stage * PARTS + q
        ref = out.at[index] if span is None else out.at[index, span]
        return pltpu.make_async_remote_copy(
            src_ref=ref, dst_ref=ref, send_sem=s_sem, recv_sem=r_sem.at[axis * 14 + lax.rem(place, 14)],
            device_id=(peers[axis],), device_id_type=MESH_ID)

    def land(stage, axis, q):
        color, owner = route(stage, axis)
        push(stage, axis, q).wait_recv()
        across((owner + deltas[axis]) * own + color * PARTS + q).start()

    def update(color, q, first=0, count=None):
        i = color * PARTS + q

        @pl.loop(first // step, (first + (count or rows)) // step)
        def _(r):
            s = pl.ds(pl.multiple_of(r * step, step), step)
            new_m, new_v = adam_moments(g_buf[color, s, :] * scales[0:1, :], m_out[i, s, :], v_out[i, s, :])
            m_out[i, s, :] = new_m
            v_out[i, s, :] = new_v
            new_p = adam_param(p_buf[color, s, :], new_m, new_v, scales[1:2, :], WEIGHT_DECAY)
            out[me * own + i, s, :] = new_p.astype(jnp.bfloat16)

    def each(count, body):
        lax.fori_loop(0, count, lambda i, c: (body(i), c)[1], 0)

    scales_load = pltpu.make_async_copy(scales_in, scales, scales_sem)
    scales_load.start()
    for color in range(COLORS):
        for copy in loads(color, 0):
            copy.start()
    scales_load.wait()
    for q in range(PARTS):
        for color in range(COLORS):
            for copy in loads(color, q):
                copy.wait()
            if q == 0:
                for i in range(CUTS):
                    update(color, q, i * part, part)
                    if color == 0 and i == 0:
                        pl.semaphore_wait(barrier, 4)
                    push(0, color, q, pl.ds(i * part, part)).start()
            else:
                update(color, q)
                push(0, color, q).start()
            push(1, (color + 1) % 3, q).start()
            across(me * own + color * PARTS + q).start()
            if q + 1 < PARTS:
                for copy in loads(color, q + 1):
                    copy.start()
        if q >= 2:
            for axis in range(3):
                land(0, axis, q - 2)
                land(1, axis, q - 2)
    for q in range(PARTS):
        for axis in range(3):
            push(2, axis, q).start()
            land(q % 2, axis, 2 + q // 2)
    for stage in range(3, 8):
        def body(q, stage=stage):
            for axis in range(3):
                if stage < 7:
                    push(stage, axis, q).start()
                land(stage - 1, axis, q)
        each(PARTS, body)

    sent = out.at[pl.ds(0, 7 * own)]
    pltpu.make_async_remote_copy(
        src_ref=sent, dst_ref=sent, send_sem=s_sem, recv_sem=r_sem.at[0],
        device_id=(partner,), device_id_type=MESH_ID).wait_send()
    half = pltpu.make_async_remote_copy(
        src_ref=out.at[pl.ds(0, 8 * own)], dst_ref=out.at[pl.ds(0, 8 * own)], send_sem=ds_sem, recv_sem=dr_sem,
        device_id=(partner,), device_id_type=MESH_ID)
    half.wait_recv()
    half.wait_send()


def write_kernel(held, m_held, v_held, p, scales_in, g_vec, p_vec, m_vec, v_vec,
                 out, p_out, m_out, v_out, pv_out, mv_out, vv_out,
                 p_buf, vec_buf, scales, in_sem, out_sem, sem, vec_sem, vec_out_sem, scales_sem):
    own, rows, _ = p.shape
    step = min(rows, ROWS)
    span = held.shape[0] // own

    def load(i):
        return pltpu.make_async_copy(p.at[i], p_buf.at[i % RING], in_sem.at[i % RING])

    def store(i):
        return pltpu.make_async_copy(p_buf.at[i % RING], p_out.at[i], out_sem.at[i % RING])

    def copies(i):
        part = pl.ds(i * span, span)
        return (pltpu.make_async_copy(held.at[part], out.at[part], sem.at[0, i % AHEAD]),
                pltpu.make_async_copy(m_held.at[i], m_out.at[i], sem.at[1, i % AHEAD]),
                pltpu.make_async_copy(v_held.at[i], v_out.at[i], sem.at[2, i % AHEAD]))

    scales_load = pltpu.make_async_copy(scales_in, scales, scales_sem)
    scales_load.start()
    vec_loads = [pltpu.make_async_copy(a, vec_buf.at[k], vec_sem.at[k])
                 for k, a in enumerate((p_vec, m_vec, v_vec, g_vec))]
    vec_stores = [pltpu.make_async_copy(vec_buf.at[k], a, vec_out_sem.at[k])
                  for k, a in enumerate((pv_out, mv_out, vv_out))]
    def vec_update():
        for copy in vec_loads:
            copy.wait()

        @pl.loop(0, g_vec.shape[1] // 1024)
        def _(i):
            s = pl.ds(pl.multiple_of(i * 1024, 1024), 1024)
            new_m, new_v = adam_moments(vec_buf[3, :, s] * scales[0:1, 0:1], vec_buf[1, :, s], vec_buf[2, :, s])
            vec_buf[1, :, s] = new_m
            vec_buf[2, :, s] = new_v
            vec_buf[0, :, s] = adam_param(vec_buf[0, :, s], new_m, new_v, scales[1:2, 0:1], 0.0)

        for copy in vec_stores:
            copy.start()

    for i in range(RING - 1):
        load(i).start()
    for copy in vec_loads:
        copy.start()
    for i in range(AHEAD):
        for copy in copies(i):
            copy.start()
    scales_load.wait()
    for i in range(own):
        load(i).wait()

        @pl.loop(0, rows // step)
        def _(r):
            s = pl.ds(pl.multiple_of(r * step, step), step)
            p_buf[i % RING, s, :] = adam_param(
                p_buf[i % RING, s, :], m_held[i, s, :], v_held[i, s, :], scales[1:2, :], WEIGHT_DECAY)

        store(i).start()
        if i + RING - 1 < own:
            if i:
                store(i - 1).wait()
            load(i + RING - 1).start()
        if i + AHEAD < own:
            for copy in copies(i):
                copy.wait()
            for copy in copies(i + AHEAD):
                copy.start()
        if i == 0:
            vec_update()

    for i in range(own - RING, own):
        store(i).wait()
    for i in range(own - AHEAD, own):
        for copy in copies(i):
            copy.wait()
    for copy in vec_stores:
        copy.wait()


def gather_update(grad, p, m, v, scales, grad_vec, p_vec, m_vec, v_vec, axis_name, group_size):
    own = COLORS * PARTS
    piece = p.shape[0]
    n_vec = p_vec.shape[0]
    rows = piece // (own * 128)
    dma = pltpu.SemaphoreType.DMA
    any_spec = pl.BlockSpec(memory_space=pl.ANY)
    vmem_spec = pl.BlockSpec(memory_space=pltpu.VMEM)
    grad, p, m, v = (a.reshape(own, rows, 128) for a in (grad, p, m, v))
    p_vec, m_vec, v_vec = (a.reshape(1, n_vec) for a in (p_vec, m_vec, v_vec))
    full, new_m, new_v = pl.pallas_call(
        functools.partial(gather_kernel, axis_name),
        out_shape=(pltpu.VMEM((group_size * own, rows, 128), jnp.bfloat16),
                   pltpu.VMEM((own, rows, 128), jnp.float32),
                   pltpu.VMEM((own, rows, 128), jnp.float32)),
        in_specs=[any_spec] * 5,
        out_specs=[vmem_spec] * 3,
        scratch_shapes=[
            pltpu.VMEM((COLORS, rows, 128), jnp.float32), pltpu.VMEM((COLORS, rows, 128), jnp.float32),
            pltpu.VMEM((2, 128), jnp.float32), dma, dma((COLORS,)), dma((COLORS,)), dma((COLORS,)), dma((COLORS,)),
            dma, dma((3 * 14,)), dma, dma],
        compiler_params=pltpu.CompilerParams(
            collective_id=1, has_side_effects=True, vmem_limit_bytes=SMALL_VMEM),
        name="gather_update",
    )(grad, p, m, v, scales)
    flat = jax.ShapeDtypeStruct((own, rows, 128), jnp.float32)
    line = jax.ShapeDtypeStruct((1, n_vec), jnp.float32)
    full, new_p, new_m, new_v, *vecs = pl.pallas_call(
        write_kernel,
        out_shape=(jax.ShapeDtypeStruct(full.shape, full.dtype), flat, flat, flat, line, line, line),
        in_specs=[vmem_spec] * 3 + [any_spec] * 6,
        out_specs=[any_spec] * 7,
        scratch_shapes=[
            pltpu.VMEM((RING, rows, 128), jnp.float32), pltpu.VMEM((4, 1, n_vec), jnp.float32),
            pltpu.VMEM((2, 128), jnp.float32),
            dma((RING,)), dma((RING,)), dma((3, AHEAD)), dma((4,)), dma((3,)), dma],
        compiler_params=pltpu.CompilerParams(vmem_limit_bytes=SMALL_VMEM),
        name="write_out",
    )(*(pltpu.with_memory_space_constraint(a, pltpu.VMEM) for a in (full, new_m, new_v)),
      p, scales, grad_vec, p_vec, m_vec, v_vec)
    return (*(a.reshape(piece) for a in (new_p, new_m, new_v)), *(a.reshape(n_vec) for a in vecs),
            full.reshape(group_size * piece))


def solution(mesh):
    axis_name = mesh.axis_names[0]
    group_size = mesh.shape[axis_name]

    def local_step(g_mat, g_vec, p_mat, m_mat, v_mat, p_vec, m_vec, v_vec, learn_rate):
        grad_mat, grad_vec, scales = scatter_sum(g_mat, g_vec, learn_rate, axis_name, group_size)
        return gather_update(grad_mat, p_mat, m_mat, v_mat, scales, grad_vec, p_vec, m_vec, v_vec, axis_name, group_size)

    return jax.shard_map(
        local_step,
        mesh=mesh,
        in_specs=(P(axis_name, None), P(axis_name, None), P(axis_name), P(axis_name), P(axis_name), P(), P(), P(), P()),
        out_specs=(P(axis_name), P(axis_name), P(axis_name), P(), P(), P(), P()),
        check_vma=False,
    )
```

```python
import functools

import jax
import jax.numpy as jnp
from jax import lax
from jax.experimental import pallas as pl
from jax.experimental.pallas import tpu as pltpu
from jax.sharding import PartitionSpec as P

STEP = 10
ADAM_BETA1 = 0.9
ADAM_BETA2 = 0.98
ADAM_EPS = 1e-8
WEIGHT_DECAY = 0.01
MAX_NORM = 1.0
NORM_EPS = 1e-6
BIAS_ONE = 1.0 - ADAM_BETA1 ** STEP
BIAS_TWO = 1.0 - ADAM_BETA2 ** STEP

MESH_ID = pl.DeviceIdType.MESH
COLORS = 3
PARTS = 4
STRIDES = (2, 4, 8)
STEPS = 8 * PARTS
DEVICES = 16
WIDTH = 4096
ROWS = 64
SMALL_VMEM = 3400 * 1024
RING = 5
AHEAD = 2
SWAPS = 8
PLACES = 20
CUTS = 4
MEAN_SCALE = 1.0 / 16.0


def scatter_kernel(axis_name, piece, g, gv, lr, out, pg, vec_out, scale_out,
                   a_buf, b_buf, e_buf, stage, r1, r2, r3, v_in, v_full, v_acc, v_get, v_mean, n_put, n_get, squares, lr_smem, scale_buf,
                   a_sem, b_sem, e_sem, ds_sem, dr_sem, dc_sem, s1_sem, r1_sem, s2_sem, r2_sem, s3_sem, r3_sem, rc_sem, o_sem,
                   vi_sem, vs_sem, vr_sem, ns_sem, nr_sem, vo_sem, lr_sem, so_sem):
    chunk = piece // (COLORS * PARTS)
    width = min(chunk // CUTS, WIDTH)
    part = chunk // CUTS
    n_vec = gv.shape[1]
    n_half = n_vec // 2
    me = lax.axis_index(axis_name)
    core = lax.rem(me, 2)
    core_step = 1 - 2 * core
    deltas = [s * (1 - 2 * lax.rem(me // s, 2)) for s in STRIDES]
    partner = me + core_step
    peers = [me + d for d in deltas]

    barrier = pltpu.get_barrier_semaphore()
    for dev in (partner, *peers):
        pl.semaphore_signal(barrier, inc=1, device_id=(dev,), device_id_type=MESH_ID)

    def offset(color, t):
        unit = t // PARTS
        f1 = 1 - unit // 4
        f2 = 1 - lax.rem(unit // 2, 2)
        f3 = 1 - lax.rem(unit, 2)
        d1, d2, d3 = (deltas[(color + k) % 3] for k in range(3))
        owner = me + f1 * d1 + f2 * d2 + f3 * d3
        return owner * piece + (color * PARTS + lax.rem(t, PARTS)) * chunk

    def cut(ref, start):
        return ref.at[:, pl.ds(pl.multiple_of(start, 1024), chunk)]

    def swap(color, t):
        return pltpu.make_async_remote_copy(
            src_ref=cut(g, offset(color, t) + core_step * piece),
            dst_ref=cut(pg, (color * STEPS + t) * chunk),
            send_sem=ds_sem, recv_sem=dr_sem.at[color * SWAPS + lax.rem(t, SWAPS)],
            device_id=(partner,), device_id_type=MESH_ID)

    def swap_early(color, t):
        k = color * 2 + t
        return pltpu.make_async_remote_copy(
            src_ref=cut(g, offset(color, t) + core_step * piece), dst_ref=b_buf.at[k],
            send_sem=ds_sem, recv_sem=dr_sem.at[color * SWAPS + t],
            device_id=(partner,), device_id_type=MESH_ID)

    def swap_cut(color, i):
        s = pl.ds(i * part, part)
        return pltpu.make_async_remote_copy(
            src_ref=e_buf.at[color, :, s], dst_ref=b_buf.at[color * 2, :, s],
            send_sem=ds_sem, recv_sem=dc_sem.at[color * CUTS + i],
            device_id=(partner,), device_id_type=MESH_ID)

    def load_e(color):
        return pltpu.make_async_copy(
            cut(g, offset(color, 0) + core_step * piece), e_buf.at[color], e_sem.at[color])

    def push_cut(color, i):
        k, j = color * 3, color * 4 * PARTS
        s = pl.ds(i * part, part)
        return push(stage.at[k, :, s], r1.at[j, :, s], s1_sem.at[k], r1_sem.at[color * 4], color)

    def load_a(color, t):
        k = color * 2 + lax.rem(t, 2)
        return pltpu.make_async_copy(cut(g, offset(color, t)), a_buf.at[k], a_sem.at[k])

    def load_b(color, t):
        k = color * 2 + lax.rem(t, 2)
        return pltpu.make_async_copy(cut(pg, (color * STEPS + t) * chunk), b_buf.at[k], b_sem.at[k])

    def push(src, dst, send_sem, recv_sem, axis):
        return pltpu.make_async_remote_copy(
            src_ref=src, dst_ref=dst, send_sem=send_sem, recv_sem=recv_sem,
            device_id=(peers[axis],), device_id_type=MESH_ID)

    def push1(color, t):
        k = color * 3 + lax.rem(t, 3)
        j = color * 4 * PARTS + t
        return push(stage.at[k], r1.at[j], s1_sem.at[k], r1_sem.at[color * 4 + t // PARTS], color)

    def push2(color, t):
        j = color * 2 * PARTS + t - 4 * PARTS
        return push(r1.at[color * 4 * PARTS + t - 4 * PARTS], r2.at[j], s2_sem,
                    r2_sem.at[color * 2 + t // PARTS - 4], (color + 1) % 3)

    def push3(color, t):
        j = color * PARTS + t - 6 * PARTS
        return push(r1.at[color * 4 * PARTS + t - 4 * PARTS], r3.at[j], s3_sem, r3_sem.at[j], (color + 2) % 3)

    def push3_cut(color, i):
        s = pl.ds(i * part, part)
        return push(r1.at[color * 4 * PARTS + 3 * PARTS - 1, :, s], r3.at[color * PARTS + PARTS - 1, :, s],
                    s3_sem, rc_sem.at[color * CUTS + i], (color + 2) % 3)

    def unit1(color, u):
        span = r1.at[pl.ds((color * 4 + u) * PARTS, PARTS)]
        return push(span, span, s2_sem, r1_sem.at[color * 4 + u], color)

    def unit2(color, w):
        span = r2.at[pl.ds((color * 2 + w) * PARTS, PARTS)]
        return push(span, span, s2_sem, r2_sem.at[color * 2 + w], (color + 1) % 3)

    def store(color, t):
        j = color * PARTS + t - 7 * PARTS
        return pltpu.make_async_copy(r3.at[j], cut(out, j * chunk), o_sem)

    def add_up(color, t, dst, extra, last=False, span=None):
        k = color * 2 + lax.rem(t, 2)
        first, count = span or (0, chunk)

        @pl.loop(first // width, (first + count) // width)
        def _(i):
            s = pl.ds(pl.multiple_of(i * width, width), width)
            acc = a_buf[k, :, s].astype(jnp.float32) + b_buf[k, :, s].astype(jnp.float32)
            for ref, j in extra:
                acc = acc + ref[j, :, s]
            if last:
                acc = acc * MEAN_SCALE
                squares[...] += acc * acc
            dst[0][dst[1], :, s] = acc

    def half(ref, which):
        return ref.at[:, pl.ds(pl.multiple_of(which * n_half, 1024), n_half)]

    def vec_push(k):
        src = half(v_full, 1 - core) if k == 0 else half(v_mean, core) if k == 4 else v_acc.at[k]
        return pltpu.make_async_remote_copy(
            src_ref=src, dst_ref=half(v_mean, core) if k == 4 else v_get.at[k],
            send_sem=vs_sem, recv_sem=vr_sem.at[k],
            device_id=((partner, *peers, partner)[k],), device_id_type=MESH_ID)

    def norm_push(k):
        return pltpu.make_async_remote_copy(
            src_ref=n_put, dst_ref=n_get.at[me], send_sem=ns_sem, recv_sem=nr_sem,
            device_id=(lax.rem(me + k, DEVICES),), device_id_type=MESH_ID)

    def vec_loop(count, body):
        @pl.loop(0, count // 1024)
        def _(i):
            body(pl.multiple_of(i * 1024, 1024))

    def vec_turn(k):
        def body(i):
            s = pl.ds(i, 1024)
            here = pl.ds(pl.multiple_of(core * n_half + i, 1024), 1024)
            total = (v_acc[k, :, s] if k else v_full[:, here]) + v_get[k, :, s]
            if k < 3:
                v_acc[k + 1, :, s] = total
            else:
                v_mean[:, here] = total * MEAN_SCALE
        vec_push(k).wait_recv()
        vec_loop(n_half, body)
        vec_push(k + 1).start()

    def ready(color, t):
        load_a(color, t).wait()
        load_b(color, t).wait()

    def refill(color, t):
        load_a(color, t).start()
        swap(color, t).wait_recv()
        load_b(color, t).start()

    def more_swap(color, t):
        swap(color, t).start()

    for color in range(COLORS):
        load_e(color).start()
    for t in range(2):
        for color in range(COLORS):
            load_a(color, t).start()
    vec_load = pltpu.make_async_copy(gv, v_in, vi_sem)
    vec_load.start()
    lr_load = pltpu.make_async_copy(lr, lr_smem, lr_sem)
    lr_load.start()
    squares[...] = jnp.zeros_like(squares)
    for color in range(COLORS):
        load_e(color).wait()
    pl.semaphore_wait(barrier, 4)
    for i in range(CUTS):
        for color in range(COLORS):
            swap_cut(color, i).start()
    for color in range(COLORS):
        swap_early(color, 1).start()
    for t in range(2, 4):
        for color in range(COLORS):
            swap(color, t).start()
    for i in range(CUTS):
        for color in range(COLORS):
            if i == 0:
                load_a(color, 0).wait()
            swap_cut(color, i).wait_recv()
            add_up(color, 0, (stage, color * 3), (), span=(i * part, part))
            push_cut(color, i).start()
    for color in range(COLORS):
        more_swap(color, 4)
        refill(color, 2)

    def phase_one(t, first, early=False):
        for color in range(COLORS):
            if early:
                load_a(color, t).wait()
                swap_early(color, t).wait_recv()
            else:
                ready(color, t)
            if not first:
                push1(color, t - 3).wait_send()
            add_up(color, t, (stage, color * 3 + lax.rem(t, 3)), ())
            push1(color, t).start()
            more_swap(color, t + 4)
            refill(color, t + 2)

    def run(lo, hi, body):
        lax.fori_loop(lo, hi, lambda t, c: (body(t), c)[1], 0)

    phase_one(1, True, True)
    phase_one(2, True)
    vec_load.wait()

    def widen(i):
        s = pl.ds(i, 1024)
        v_full[:, s] = v_in[:, s].astype(jnp.float32)

    vec_loop(n_vec, widen)
    vec_push(0).start()
    for k in range(4):
        run(3 * k + 3, 3 * k + 6, lambda t: phase_one(t, False))
        vec_turn(k)
    run(15, 4 * PARTS, lambda t: phase_one(t, False))
    vec_push(4).wait_recv()
    vec_store = pltpu.make_async_copy(v_mean, vec_out, vo_sem)
    vec_store.start()

    def phase_two(t):
        for color in range(COLORS):
            ready(color, t)
            j = color * 4 * PARTS + t - 4 * PARTS
            add_up(color, t, (r1, j), ((r1, j),))
            push2(color, t).start()
            more_swap(color, t + 4)
            refill(color, t + 2)

    def phase_three(t, cuts):
        for color in range(COLORS):
            ready(color, t)
            j = color * 4 * PARTS + t - 4 * PARTS
            add_up(color, t, (r1, j), ((r1, j), (r2, color * 2 * PARTS + t - 6 * PARTS)))
            if cuts:
                for i in range(CUTS):
                    push3_cut(color, i).start()
            else:
                push3(color, t).start()
            more_swap(color, t + 4)
            refill(color, t + 2)

    def finish(color, t, span=None):
        j = color * PARTS + t - 7 * PARTS
        add_up(color, t, (r3, j), (
            (r1, color * 4 * PARTS + t - 4 * PARTS),
            (r2, color * 2 * PARTS + t - 6 * PARTS),
            (r3, j)), last=True, span=span)

    def phase_four(t, fill):
        for color in range(COLORS):
            ready(color, t)
            push3(color, t - PARTS).wait_recv()
            finish(color, t)
            store(color, t).start()
            if fill:
                refill(color, t + 2)

    for unit in range(4, 8):
        for color in range(COLORS):
            unit1(color, unit - 4).wait_recv()
            if unit >= 6:
                unit2(color, unit - 6).wait_recv()
        lo = unit * PARTS
        if unit < 6:
            run(lo, lo + PARTS, phase_two)
        elif unit == 6:
            run(lo, lo + PARTS - 1, lambda t: phase_three(t, False))
            phase_three(lo + PARTS - 1, True)
        else:
            run(lo, lo + PARTS - 2, lambda t: phase_four(t, True))
            phase_four(lo + PARTS - 2, False)
    for color in range(COLORS):
        ready(color, STEPS - 1)
    for i in range(CUTS):
        for color in range(COLORS):
            push3_cut(color, i).wait_recv()
            finish(color, STEPS - 1, span=(i * part, part))
    for color in range(COLORS):
        store(color, STEPS - 1).start()

    vec_sq = jnp.sum(v_mean[...] * v_mean[...], axis=1, keepdims=True)
    mine = jnp.broadcast_to(jnp.sum(squares[...], axis=1, keepdims=True), (1, 128))
    n_put[...] = mine
    n_get[me] = mine
    for k in range(1, DEVICES):
        norm_push(k).start()
    rest = pltpu.make_async_remote_copy(
        src_ref=n_get.at[pl.ds(0, DEVICES - 1)], dst_ref=n_get.at[pl.ds(0, DEVICES - 1)],
        send_sem=ns_sem, recv_sem=nr_sem, device_id=(partner,), device_id_type=MESH_ID)
    rest.wait_recv()
    norm_sq = n_get[0]
    for k in range(1, DEVICES):
        norm_sq = norm_sq + n_get[k]
    norm_sq = norm_sq + vec_sq
    scale_buf[0:1, :] = jnp.minimum(1.0, MAX_NORM / (jnp.sqrt(norm_sq) + NORM_EPS))
    lr_load.wait()
    scale_buf[1:2, :] = jnp.full((1, 128), lr_smem[0])
    scale_store = pltpu.make_async_copy(scale_buf, scale_out, so_sem)
    scale_store.start()

    def drain(lo, hi, wait):
        def body(t):
            for color in range(COLORS):
                wait(color, t)
        run(lo, hi, body)

    drain(4 * PARTS - 3, 4 * PARTS, lambda c, t: push1(c, t).wait_send())
    push(r2, r2, s2_sem, r2_sem.at[0], 0).wait_send()
    push(r3, r3, s3_sem, r3_sem.at[0], 0).wait_send()
    pltpu.make_async_remote_copy(
        src_ref=pg, dst_ref=pg, send_sem=ds_sem, recv_sem=dr_sem.at[0],
        device_id=(partner,), device_id_type=MESH_ID).wait_send()
    pltpu.make_async_copy(out, out, o_sem).wait()
    push(v_get, v_get, vs_sem, vr_sem.at[0], 0).wait_send()
    rest.wait_send()
    vec_store.wait()
    scale_store.wait()


def scatter_sum(g_mat, g_vec, learn_rate, axis_name, group_size):
    total = g_mat.shape[1]
    n_vec = g_vec.shape[1]
    piece = total // group_size
    chunk = piece // (COLORS * PARTS)
    dma = pltpu.SemaphoreType.DMA
    any_spec = pl.BlockSpec(memory_space=pl.ANY)
    out, _, vec, scales = pl.pallas_call(
        functools.partial(scatter_kernel, axis_name, piece),
        out_shape=(jax.ShapeDtypeStruct((1, piece), jnp.float32),
                   jax.ShapeDtypeStruct((1, total // 2), jnp.bfloat16),
                   jax.ShapeDtypeStruct((1, n_vec), jnp.float32),
                   jax.ShapeDtypeStruct((2, 128), jnp.float32)),
        in_specs=[any_spec] * 3,
        out_specs=[any_spec] * 4,
        scratch_shapes=[
            pltpu.VMEM((2 * COLORS, 1, chunk), jnp.bfloat16),
            pltpu.VMEM((2 * COLORS, 1, chunk), jnp.bfloat16),
            pltpu.VMEM((COLORS, 1, chunk), jnp.bfloat16),
            pltpu.VMEM((3 * COLORS, 1, chunk), jnp.float32),
            pltpu.VMEM((4 * PARTS * COLORS, 1, chunk), jnp.float32),
            pltpu.VMEM((2 * PARTS * COLORS, 1, chunk), jnp.float32),
            pltpu.VMEM((PARTS * COLORS, 1, chunk), jnp.float32),
            pltpu.VMEM((1, n_vec), jnp.bfloat16),
            pltpu.VMEM((1, n_vec), jnp.float32),
            pltpu.VMEM((4, 1, n_vec // 2), jnp.float32),
            pltpu.VMEM((5, 1, n_vec // 2), jnp.float32),
            pltpu.VMEM((1, n_vec), jnp.float32),
            pltpu.VMEM((1, 128), jnp.float32),
            pltpu.VMEM((DEVICES, 1, 128), jnp.float32),
            pltpu.VMEM((1, min(chunk // CUTS, WIDTH)), jnp.float32),
            pltpu.SMEM((1,), jnp.float32),
            pltpu.VMEM((2, 128), jnp.float32),
            dma((2 * COLORS,)), dma((2 * COLORS,)), dma((COLORS,)),
            dma, dma((SWAPS * COLORS,)), dma((CUTS * COLORS,)),
            dma((3 * COLORS,)), dma((4 * COLORS,)), dma, dma((2 * COLORS,)),
            dma, dma((PARTS * COLORS,)), dma((CUTS * COLORS,)), dma,
            dma, dma, dma((5,)), dma, dma, dma, dma, dma,
        ],
        compiler_params=pltpu.CompilerParams(
            collective_id=0, has_side_effects=True, vmem_limit_bytes=63 * 1024 * 1024),
        name="scatter_sum",
    )(g_mat, g_vec, learn_rate.reshape(1))
    return out, vec, scales


def adam_moments(grad, m, v):
    new_m = ADAM_BETA1 * m + (1.0 - ADAM_BETA1) * grad
    new_v = ADAM_BETA2 * v + (1.0 - ADAM_BETA2) * grad * grad
    return new_m, new_v


def adam_param(p, m, v, rate, decay):
    direction = (m / BIAS_ONE) / (jnp.sqrt(v / BIAS_TWO) + ADAM_EPS)
    return p - rate * (direction + decay * p)


def gather_kernel(axis_name, grad, p, m, v, scales_in, out, m_out, v_out, g_buf, p_buf, scales,
                  scales_sem, g_sem, p_sem, m_sem, v_sem, s_sem, r_sem, ds_sem, dr_sem):
    own = COLORS * PARTS
    rows = p.shape[1]
    part = rows // CUTS
    step = min(part, ROWS)
    me = lax.axis_index(axis_name)
    deltas = [s * (1 - 2 * lax.rem(me // s, 2)) for s in STRIDES]
    partner = me + 1 - 2 * lax.rem(me, 2)
    peers = [me + d for d in deltas]

    barrier = pltpu.get_barrier_semaphore()
    for dev in (partner, *peers):
        pl.semaphore_signal(barrier, inc=1, device_id=(dev,), device_id_type=MESH_ID)

    def loads(color, q):
        i = color * PARTS + q
        return (pltpu.make_async_copy(grad.at[i], g_buf.at[color], g_sem.at[color]),
                pltpu.make_async_copy(m.at[i], m_out.at[i], m_sem.at[color]),
                pltpu.make_async_copy(v.at[i], v_out.at[i], v_sem.at[color]),
                pltpu.make_async_copy(p.at[i], p_buf.at[color], p_sem.at[color]))

    def across(index):
        return pltpu.make_async_remote_copy(
            src_ref=out.at[index], dst_ref=out.at[index], send_sem=ds_sem, recv_sem=dr_sem,
            device_id=(partner,), device_id_type=MESH_ID)

    def route(stage, axis):
        b1, b2 = (axis - 2) % 3, (axis - 1) % 3
        color = (axis, b2, b2, b1, b1, b1, b1)[stage]
        flips = ((), (), (b2,), (), (b1,), (b2,), (b1, b2))[stage]
        return color, sum((deltas[f] for f in flips), me)

    def push(stage, axis, q, span=None):
        color, owner = route(stage, axis)
        index = owner * own + color * PARTS + q
        place = (3 * q, 3 * q + 1, 3 * PARTS + q, 3 * q + 2)[stage] if stage < 4 else stage * PARTS + q
        ref = out.at[index] if span is None else out.at[index, span]
        return pltpu.make_async_remote_copy(
            src_ref=ref, dst_ref=ref, send_sem=s_sem, recv_sem=r_sem.at[axis * PLACES + lax.rem(place, PLACES)],
            device_id=(peers[axis],), device_id_type=MESH_ID)

    def land(stage, axis, q):
        color, owner = route(stage, axis)
        push(stage, axis, q).wait_recv()
        across((owner + deltas[axis]) * own + color * PARTS + q).start()

    def update(color, q, first=0, count=None):
        i = color * PARTS + q

        @pl.loop(first // step, (first + (count or rows)) // step)
        def _(r):
            s = pl.ds(pl.multiple_of(r * step, step), step)
            new_m, new_v = adam_moments(g_buf[color, s, :] * scales[0:1, :], m_out[i, s, :], v_out[i, s, :])
            m_out[i, s, :] = new_m
            v_out[i, s, :] = new_v
            new_p = adam_param(p_buf[color, s, :], new_m, new_v, scales[1:2, :], WEIGHT_DECAY)
            out[me * own + i, s, :] = new_p.astype(jnp.bfloat16)

    def each(count, body):
        lax.fori_loop(0, count, lambda i, c: (body(i), c)[1], 0)

    scales_load = pltpu.make_async_copy(scales_in, scales, scales_sem)
    scales_load.start()

    def fetch(color, q):
        for copy in loads(color, q):
            copy.start()

    fetch(0, 0)
    scales_load.wait()
    fetch(1, 0)
    for q in range(PARTS):
        for color in range(COLORS):
            for copy in loads(color, q):
                copy.wait()
            if q == 0 and color == 0:
                fetch(2, 0)
            for i in range(CUTS if q == 0 else 1):
                count = rows // CUTS if q == 0 else rows
                update(color, q, i * count, count)
                if q == 0 and color == 0 and i == 0:
                    pl.semaphore_wait(barrier, 4)
                for k, stage in enumerate((0, 1, 3)):
                    push(stage, (color + k) % 3, q, pl.ds(i * count, count)).start()
            across(me * own + color * PARTS + q).start()
            if q + 1 < PARTS:
                fetch(color, q + 1)

    def own_stage(q):
        for axis in range(3):
            for stage in (0, 1, 3):
                land(stage, axis, q)
            push(2, (axis + 1) % 3, q).start()

    each(PARTS, own_stage)
    for stage, last in ((4, 2), (5, 4), (6, 5), (None, 6)):
        def body(q, stage=stage, last=last):
            for axis in range(3):
                if stage:
                    push(stage, axis, q).start()
                land(last, axis, q)
        each(PARTS, body)

    sent = out.at[pl.ds(0, 7 * own)]
    pltpu.make_async_remote_copy(
        src_ref=sent, dst_ref=sent, send_sem=s_sem, recv_sem=r_sem.at[0],
        device_id=(partner,), device_id_type=MESH_ID).wait_send()
    half = pltpu.make_async_remote_copy(
        src_ref=out.at[pl.ds(0, 8 * own)], dst_ref=out.at[pl.ds(0, 8 * own)], send_sem=ds_sem, recv_sem=dr_sem,
        device_id=(partner,), device_id_type=MESH_ID)
    half.wait_recv()
    half.wait_send()


def write_kernel(held, m_held, v_held, p, scales_in, g_vec, p_vec, m_vec, v_vec,
                 out, p_out, m_out, v_out, pv_out, mv_out, vv_out,
                 p_buf, vec_buf, scales, in_sem, out_sem, sem, vec_sem, vec_out_sem, scales_sem):
    own, rows, _ = p.shape
    step = min(rows, ROWS)
    span = held.shape[0] // own

    def load(i):
        return pltpu.make_async_copy(p.at[i], p_buf.at[i % RING], in_sem.at[i % RING])

    def store(i):
        return pltpu.make_async_copy(p_buf.at[i % RING], p_out.at[i], out_sem.at[i % RING])

    def copies(i):
        part = pl.ds(i * span, span)
        return (pltpu.make_async_copy(held.at[part], out.at[part], sem.at[0, i % AHEAD]),
                pltpu.make_async_copy(m_held.at[i], m_out.at[i], sem.at[1, i % AHEAD]),
                pltpu.make_async_copy(v_held.at[i], v_out.at[i], sem.at[2, i % AHEAD]))

    scales_load = pltpu.make_async_copy(scales_in, scales, scales_sem)
    scales_load.start()
    vec_loads = [pltpu.make_async_copy(a, vec_buf.at[k], vec_sem.at[k])
                 for k, a in enumerate((p_vec, m_vec, v_vec, g_vec))]
    vec_stores = [pltpu.make_async_copy(vec_buf.at[k], a, vec_out_sem.at[k])
                  for k, a in enumerate((pv_out, mv_out, vv_out))]
    def vec_update():
        for copy in vec_loads:
            copy.wait()

        @pl.loop(0, g_vec.shape[1] // 1024)
        def _(i):
            s = pl.ds(pl.multiple_of(i * 1024, 1024), 1024)
            new_m, new_v = adam_moments(vec_buf[3, :, s] * scales[0:1, 0:1], vec_buf[1, :, s], vec_buf[2, :, s])
            vec_buf[1, :, s] = new_m
            vec_buf[2, :, s] = new_v
            vec_buf[0, :, s] = adam_param(vec_buf[0, :, s], new_m, new_v, scales[1:2, 0:1], 0.0)

        for copy in vec_stores:
            copy.start()

    for i in range(RING - 1):
        load(i).start()
    for copy in vec_loads:
        copy.start()
    for i in range(AHEAD):
        for copy in copies(i):
            copy.start()
    scales_load.wait()
    for i in range(own):
        load(i).wait()

        @pl.loop(0, rows // step)
        def _(r):
            s = pl.ds(pl.multiple_of(r * step, step), step)
            p_buf[i % RING, s, :] = adam_param(
                p_buf[i % RING, s, :], m_held[i, s, :], v_held[i, s, :], scales[1:2, :], WEIGHT_DECAY)

        store(i).start()
        if i + RING - 1 < own:
            if i:
                store(i - 1).wait()
            load(i + RING - 1).start()
        if i + AHEAD < own:
            for copy in copies(i):
                copy.wait()
            for copy in copies(i + AHEAD):
                copy.start()
        if i == 0:
            vec_update()

    for i in range(own - RING, own):
        store(i).wait()
    for i in range(own - AHEAD, own):
        for copy in copies(i):
            copy.wait()
    for copy in vec_stores:
        copy.wait()


def gather_update(grad, p, m, v, scales, grad_vec, p_vec, m_vec, v_vec, axis_name, group_size):
    own = COLORS * PARTS
    piece = p.shape[0]
    n_vec = p_vec.shape[0]
    rows = piece // (own * 128)
    dma = pltpu.SemaphoreType.DMA
    any_spec = pl.BlockSpec(memory_space=pl.ANY)
    vmem_spec = pl.BlockSpec(memory_space=pltpu.VMEM)
    grad, p, m, v = (a.reshape(own, rows, 128) for a in (grad, p, m, v))
    p_vec, m_vec, v_vec = (a.reshape(1, n_vec) for a in (p_vec, m_vec, v_vec))
    full, new_m, new_v = pl.pallas_call(
        functools.partial(gather_kernel, axis_name),
        out_shape=(pltpu.VMEM((group_size * own, rows, 128), jnp.bfloat16),
                   pltpu.VMEM((own, rows, 128), jnp.float32),
                   pltpu.VMEM((own, rows, 128), jnp.float32)),
        in_specs=[any_spec] * 5,
        out_specs=[vmem_spec] * 3,
        scratch_shapes=[
            pltpu.VMEM((COLORS, rows, 128), jnp.float32), pltpu.VMEM((COLORS, rows, 128), jnp.float32),
            pltpu.VMEM((2, 128), jnp.float32), dma, dma((COLORS,)), dma((COLORS,)), dma((COLORS,)), dma((COLORS,)),
            dma, dma((3 * PLACES,)), dma, dma],
        compiler_params=pltpu.CompilerParams(
            collective_id=1, has_side_effects=True, vmem_limit_bytes=SMALL_VMEM),
        name="gather_update",
    )(grad, p, m, v, scales)
    flat = jax.ShapeDtypeStruct((own, rows, 128), jnp.float32)
    line = jax.ShapeDtypeStruct((1, n_vec), jnp.float32)
    full, new_p, new_m, new_v, *vecs = pl.pallas_call(
        write_kernel,
        out_shape=(jax.ShapeDtypeStruct(full.shape, full.dtype), flat, flat, flat, line, line, line),
        in_specs=[vmem_spec] * 3 + [any_spec] * 6,
        out_specs=[any_spec] * 7,
        scratch_shapes=[
            pltpu.VMEM((RING, rows, 128), jnp.float32), pltpu.VMEM((4, 1, n_vec), jnp.float32),
            pltpu.VMEM((2, 128), jnp.float32),
            dma((RING,)), dma((RING,)), dma((3, AHEAD)), dma((4,)), dma((3,)), dma],
        compiler_params=pltpu.CompilerParams(vmem_limit_bytes=SMALL_VMEM),
        name="write_out",
    )(*(pltpu.with_memory_space_constraint(a, pltpu.VMEM) for a in (full, new_m, new_v)),
      p, scales, grad_vec, p_vec, m_vec, v_vec)
    return (*(a.reshape(piece) for a in (new_p, new_m, new_v)), *(a.reshape(n_vec) for a in vecs),
            full.reshape(group_size * piece))


def solution(mesh):
    axis_name = mesh.axis_names[0]
    group_size = mesh.shape[axis_name]

    def local_step(g_mat, g_vec, p_mat, m_mat, v_mat, p_vec, m_vec, v_vec, learn_rate):
        grad_mat, grad_vec, scales = scatter_sum(g_mat, g_vec, learn_rate, axis_name, group_size)
        return gather_update(grad_mat, p_mat, m_mat, v_mat, scales, grad_vec, p_vec, m_vec, v_vec, axis_name, group_size)

    return jax.shard_map(
        local_step,
        mesh=mesh,
        in_specs=(P(axis_name, None), P(axis_name, None), P(axis_name), P(axis_name), P(axis_name), P(), P(), P(), P()),
        out_specs=(P(axis_name), P(axis_name), P(axis_name), P(), P(), P(), P()),
        check_vma=False,
    )
```

```python
import functools

import jax
import jax.numpy as jnp
from jax import lax
from jax.experimental import pallas as pl
from jax.experimental.pallas import tpu as pltpu
from jax.sharding import PartitionSpec as P

STEP = 10
ADAM_BETA1 = 0.9
ADAM_BETA2 = 0.98
ADAM_EPS = 1e-8
WEIGHT_DECAY = 0.01
MAX_NORM = 1.0
NORM_EPS = 1e-6
BIAS_ONE = 1.0 - ADAM_BETA1 ** STEP
BIAS_TWO = 1.0 - ADAM_BETA2 ** STEP

MESH_ID = pl.DeviceIdType.MESH
COLORS = 3
PARTS = 4
STRIDES = (2, 4, 8)
STEPS = 8 * PARTS
DEVICES = 16
WIDTH = 4096
ROWS = 64
SMALL_VMEM = 1344 * 1024
RING = 3
KEEP = 4
AHEAD = 2
SWAPS = 8
PLACES = 20
CUTS = 4
MEAN_SCALE = 1.0 / 16.0


def scatter_kernel(axis_name, piece, g, gv, lr, out, pg, vec_out, scale_out,
                   a_buf, b_buf, e_buf, stage, r1, r2, r3, v_in, v_full, v_acc, v_get, v_mean, n_put, n_get, squares, lr_smem, scale_buf,
                   a_sem, b_sem, e_sem, ds_sem, dr_sem, dc_sem, s1_sem, r1_sem, s2_sem, r2_sem, s3_sem, r3_sem, rc_sem, o_sem,
                   vi_sem, vs_sem, vr_sem, ns_sem, nr_sem, vo_sem, lr_sem, so_sem):
    chunk = piece // (COLORS * PARTS)
    width = min(chunk // CUTS, WIDTH)
    part = chunk // CUTS
    n_vec = gv.shape[1]
    n_half = n_vec // 2
    me = lax.axis_index(axis_name)
    core = lax.rem(me, 2)
    core_step = 1 - 2 * core
    deltas = [s * (1 - 2 * lax.rem(me // s, 2)) for s in STRIDES]
    partner = me + core_step
    peers = [me + d for d in deltas]

    barrier = pltpu.get_barrier_semaphore()
    for dev in (partner, *peers):
        pl.semaphore_signal(barrier, inc=1, device_id=(dev,), device_id_type=MESH_ID)

    def offset(color, t):
        unit = t // PARTS
        f1 = 1 - unit // 4
        f2 = 1 - lax.rem(unit // 2, 2)
        f3 = 1 - lax.rem(unit, 2)
        d1, d2, d3 = (deltas[(color + k) % 3] for k in range(3))
        owner = me + f1 * d1 + f2 * d2 + f3 * d3
        return owner * piece + (color * PARTS + lax.rem(t, PARTS)) * chunk

    def cut(ref, start):
        return ref.at[:, pl.ds(pl.multiple_of(start, 1024), chunk)]

    def swap(color, t):
        return pltpu.make_async_remote_copy(
            src_ref=cut(g, offset(color, t) + core_step * piece),
            dst_ref=cut(pg, (color * STEPS + t) * chunk),
            send_sem=ds_sem, recv_sem=dr_sem.at[color * SWAPS + lax.rem(t, SWAPS)],
            device_id=(partner,), device_id_type=MESH_ID)

    def swap_early(color, t):
        k = color * 2 + t
        return pltpu.make_async_remote_copy(
            src_ref=cut(g, offset(color, t) + core_step * piece), dst_ref=b_buf.at[k],
            send_sem=ds_sem, recv_sem=dr_sem.at[color * SWAPS + t],
            device_id=(partner,), device_id_type=MESH_ID)

    def swap_cut(color, i):
        s = pl.ds(i * part, part)
        return pltpu.make_async_remote_copy(
            src_ref=e_buf.at[color, :, s], dst_ref=b_buf.at[color * 2, :, s],
            send_sem=ds_sem, recv_sem=dc_sem.at[color * CUTS + i],
            device_id=(partner,), device_id_type=MESH_ID)

    def load_e(color):
        return pltpu.make_async_copy(
            cut(g, offset(color, 0) + core_step * piece), e_buf.at[color], e_sem.at[color])

    def push_cut(color, i):
        k, j = color * 3, color * 4 * PARTS
        s = pl.ds(i * part, part)
        return push(stage.at[k, :, s], r1.at[j, :, s], s1_sem.at[k], r1_sem.at[color * 4], color)

    def load_a(color, t):
        k = color * 2 + lax.rem(t, 2)
        return pltpu.make_async_copy(cut(g, offset(color, t)), a_buf.at[k], a_sem.at[k])

    def load_b(color, t):
        k = color * 2 + lax.rem(t, 2)
        return pltpu.make_async_copy(cut(pg, (color * STEPS + t) * chunk), b_buf.at[k], b_sem.at[k])

    def push(src, dst, send_sem, recv_sem, axis):
        return pltpu.make_async_remote_copy(
            src_ref=src, dst_ref=dst, send_sem=send_sem, recv_sem=recv_sem,
            device_id=(peers[axis],), device_id_type=MESH_ID)

    def push1(color, t):
        k = color * 3 + lax.rem(t, 3)
        j = color * 4 * PARTS + t
        return push(stage.at[k], r1.at[j], s1_sem.at[k], r1_sem.at[color * 4 + t // PARTS], color)

    def push2(color, t):
        j = color * 2 * PARTS + t - 4 * PARTS
        return push(r1.at[color * 4 * PARTS + t - 4 * PARTS], r2.at[j], s2_sem,
                    r2_sem.at[color * 2 + t // PARTS - 4], (color + 1) % 3)

    def push3(color, t):
        j = color * PARTS + t - 6 * PARTS
        return push(r1.at[color * 4 * PARTS + t - 4 * PARTS], r3.at[j], s3_sem, r3_sem.at[j], (color + 2) % 3)

    def push3_cut(color, i):
        s = pl.ds(i * part, part)
        return push(r1.at[color * 4 * PARTS + 3 * PARTS - 1, :, s], r3.at[color * PARTS + PARTS - 1, :, s],
                    s3_sem, rc_sem.at[color * CUTS + i], (color + 2) % 3)

    def unit1(color, u):
        span = r1.at[pl.ds((color * 4 + u) * PARTS, PARTS)]
        return push(span, span, s2_sem, r1_sem.at[color * 4 + u], color)

    def unit2(color, w):
        span = r2.at[pl.ds((color * 2 + w) * PARTS, PARTS)]
        return push(span, span, s2_sem, r2_sem.at[color * 2 + w], (color + 1) % 3)

    def store(color, t):
        j = color * PARTS + t - 7 * PARTS
        return pltpu.make_async_copy(r3.at[j], cut(out, j * chunk), o_sem)

    def add_up(color, t, dst, extra, last=False, span=None):
        k = color * 2 + lax.rem(t, 2)
        first, count = span or (0, chunk)

        @pl.loop(first // width, (first + count) // width)
        def _(i):
            s = pl.ds(pl.multiple_of(i * width, width), width)
            acc = a_buf[k, :, s].astype(jnp.float32) + b_buf[k, :, s].astype(jnp.float32)
            for ref, j in extra:
                acc = acc + ref[j, :, s]
            if last:
                acc = acc * MEAN_SCALE
                squares[...] += acc * acc
            dst[0][dst[1], :, s] = acc

    def half(ref, which):
        return ref.at[:, pl.ds(pl.multiple_of(which * n_half, 1024), n_half)]

    def vec_push(k):
        src = half(v_full, 1 - core) if k == 0 else half(v_mean, core) if k == 4 else v_acc.at[k]
        return pltpu.make_async_remote_copy(
            src_ref=src, dst_ref=half(v_mean, core) if k == 4 else v_get.at[k],
            send_sem=vs_sem, recv_sem=vr_sem.at[k],
            device_id=((partner, *peers, partner)[k],), device_id_type=MESH_ID)

    def norm_push(k):
        return pltpu.make_async_remote_copy(
            src_ref=n_put, dst_ref=n_get.at[me], send_sem=ns_sem, recv_sem=nr_sem,
            device_id=(lax.rem(me + k, DEVICES),), device_id_type=MESH_ID)

    def vec_loop(count, body):
        @pl.loop(0, count // 1024)
        def _(i):
            body(pl.multiple_of(i * 1024, 1024))

    def vec_turn(k):
        def body(i):
            s = pl.ds(i, 1024)
            here = pl.ds(pl.multiple_of(core * n_half + i, 1024), 1024)
            total = (v_acc[k, :, s] if k else v_full[:, here]) + v_get[k, :, s]
            if k < 3:
                v_acc[k + 1, :, s] = total
            else:
                v_mean[:, here] = total * MEAN_SCALE
        vec_push(k).wait_recv()
        vec_loop(n_half, body)
        vec_push(k + 1).start()

    def ready(color, t):
        load_a(color, t).wait()
        load_b(color, t).wait()

    def refill(color, t):
        load_a(color, t).start()
        swap(color, t).wait_recv()
        load_b(color, t).start()

    def more_swap(color, t):
        swap(color, t).start()

    for color in range(COLORS):
        load_e(color).start()
    for t in range(2):
        for color in range(COLORS):
            load_a(color, t).start()
    vec_load = pltpu.make_async_copy(gv, v_in, vi_sem)
    vec_load.start()
    lr_load = pltpu.make_async_copy(lr, lr_smem, lr_sem)
    lr_load.start()
    squares[...] = jnp.zeros_like(squares)
    for color in range(COLORS):
        load_e(color).wait()
    pl.semaphore_wait(barrier, 4)
    for i in range(CUTS):
        for color in range(COLORS):
            swap_cut(color, i).start()
    for color in range(COLORS):
        swap_early(color, 1).start()
    for t in range(2, 4):
        for color in range(COLORS):
            swap(color, t).start()
    for i in range(CUTS):
        for color in range(COLORS):
            if i == 0:
                load_a(color, 0).wait()
            swap_cut(color, i).wait_recv()
            add_up(color, 0, (stage, color * 3), (), span=(i * part, part))
            push_cut(color, i).start()
    for color in range(COLORS):
        more_swap(color, 4)
        refill(color, 2)

    def phase_one(t, first, early=False):
        for color in range(COLORS):
            if early:
                load_a(color, t).wait()
                swap_early(color, t).wait_recv()
            else:
                ready(color, t)
            if not first:
                push1(color, t - 3).wait_send()
            add_up(color, t, (stage, color * 3 + lax.rem(t, 3)), ())
            push1(color, t).start()
            more_swap(color, t + 4)
            refill(color, t + 2)

    def run(lo, hi, body):
        lax.fori_loop(lo, hi, lambda t, c: (body(t), c)[1], 0)

    phase_one(1, True, True)
    phase_one(2, True)
    vec_load.wait()

    def widen(i):
        s = pl.ds(i, 1024)
        v_full[:, s] = v_in[:, s].astype(jnp.float32)

    vec_loop(n_vec, widen)
    vec_push(0).start()
    for k in range(4):
        run(3 * k + 3, 3 * k + 6, lambda t: phase_one(t, False))
        vec_turn(k)
    run(15, 4 * PARTS, lambda t: phase_one(t, False))
    vec_push(4).wait_recv()
    vec_store = pltpu.make_async_copy(v_mean, vec_out, vo_sem)
    vec_store.start()

    def phase_two(t):
        for color in range(COLORS):
            ready(color, t)
            j = color * 4 * PARTS + t - 4 * PARTS
            add_up(color, t, (r1, j), ((r1, j),))
            push2(color, t).start()
            more_swap(color, t + 4)
            refill(color, t + 2)

    def phase_three(t, cuts):
        for color in range(COLORS):
            ready(color, t)
            j = color * 4 * PARTS + t - 4 * PARTS
            add_up(color, t, (r1, j), ((r1, j), (r2, color * 2 * PARTS + t - 6 * PARTS)))
            if cuts:
                for i in range(CUTS):
                    push3_cut(color, i).start()
            else:
                push3(color, t).start()
            more_swap(color, t + 4)
            refill(color, t + 2)

    def finish(color, t, span=None):
        j = color * PARTS + t - 7 * PARTS
        add_up(color, t, (r3, j), (
            (r1, color * 4 * PARTS + t - 4 * PARTS),
            (r2, color * 2 * PARTS + t - 6 * PARTS),
            (r3, j)), last=True, span=span)

    def phase_four(t, fill):
        for color in range(COLORS):
            ready(color, t)
            push3(color, t - PARTS).wait_recv()
            finish(color, t)
            store(color, t).start()
            if fill:
                refill(color, t + 2)

    for unit in range(4, 8):
        for color in range(COLORS):
            unit1(color, unit - 4).wait_recv()
            if unit >= 6:
                unit2(color, unit - 6).wait_recv()
        lo = unit * PARTS
        if unit < 6:
            run(lo, lo + PARTS, phase_two)
        elif unit == 6:
            run(lo, lo + PARTS - 1, lambda t: phase_three(t, False))
            phase_three(lo + PARTS - 1, True)
        else:
            run(lo, lo + PARTS - 2, lambda t: phase_four(t, True))
            phase_four(lo + PARTS - 2, False)
    for color in range(COLORS):
        ready(color, STEPS - 1)
    for i in range(CUTS):
        for color in range(COLORS):
            push3_cut(color, i).wait_recv()
            finish(color, STEPS - 1, span=(i * part, part))
    for color in range(COLORS):
        store(color, STEPS - 1).start()

    vec_sq = jnp.sum(v_mean[...] * v_mean[...], axis=1, keepdims=True)
    mine = jnp.broadcast_to(jnp.sum(squares[...], axis=1, keepdims=True), (1, 128))
    n_put[...] = mine
    n_get[me] = mine
    for k in range(1, DEVICES):
        norm_push(k).start()
    rest = pltpu.make_async_remote_copy(
        src_ref=n_get.at[pl.ds(0, DEVICES - 1)], dst_ref=n_get.at[pl.ds(0, DEVICES - 1)],
        send_sem=ns_sem, recv_sem=nr_sem, device_id=(partner,), device_id_type=MESH_ID)
    rest.wait_recv()
    norm_sq = n_get[0]
    for k in range(1, DEVICES):
        norm_sq = norm_sq + n_get[k]
    norm_sq = norm_sq + vec_sq
    scale_buf[0:1, :] = jnp.minimum(1.0, MAX_NORM / (jnp.sqrt(norm_sq) + NORM_EPS))
    lr_load.wait()
    scale_buf[1:2, :] = jnp.full((1, 128), lr_smem[0])
    scale_store = pltpu.make_async_copy(scale_buf, scale_out, so_sem)
    scale_store.start()

    def drain(lo, hi, wait):
        def body(t):
            for color in range(COLORS):
                wait(color, t)
        run(lo, hi, body)

    drain(4 * PARTS - 3, 4 * PARTS, lambda c, t: push1(c, t).wait_send())
    push(r2, r2, s2_sem, r2_sem.at[0], 0).wait_send()
    push(r3, r3, s3_sem, r3_sem.at[0], 0).wait_send()
    pltpu.make_async_remote_copy(
        src_ref=pg, dst_ref=pg, send_sem=ds_sem, recv_sem=dr_sem.at[0],
        device_id=(partner,), device_id_type=MESH_ID).wait_send()
    pltpu.make_async_copy(out, out, o_sem).wait()
    push(v_get, v_get, vs_sem, vr_sem.at[0], 0).wait_send()
    rest.wait_send()
    vec_store.wait()
    scale_store.wait()


def scatter_sum(g_mat, g_vec, learn_rate, axis_name, group_size):
    total = g_mat.shape[1]
    n_vec = g_vec.shape[1]
    piece = total // group_size
    chunk = piece // (COLORS * PARTS)
    dma = pltpu.SemaphoreType.DMA
    any_spec = pl.BlockSpec(memory_space=pl.ANY)
    out, _, vec, scales = pl.pallas_call(
        functools.partial(scatter_kernel, axis_name, piece),
        out_shape=(jax.ShapeDtypeStruct((1, piece), jnp.float32),
                   jax.ShapeDtypeStruct((1, total // 2), jnp.bfloat16),
                   jax.ShapeDtypeStruct((1, n_vec), jnp.float32),
                   jax.ShapeDtypeStruct((2, 128), jnp.float32)),
        in_specs=[any_spec] * 3,
        out_specs=[any_spec] * 4,
        scratch_shapes=[
            pltpu.VMEM((2 * COLORS, 1, chunk), jnp.bfloat16),
            pltpu.VMEM((2 * COLORS, 1, chunk), jnp.bfloat16),
            pltpu.VMEM((COLORS, 1, chunk), jnp.bfloat16),
            pltpu.VMEM((3 * COLORS, 1, chunk), jnp.float32),
            pltpu.VMEM((4 * PARTS * COLORS, 1, chunk), jnp.float32),
            pltpu.VMEM((2 * PARTS * COLORS, 1, chunk), jnp.float32),
            pltpu.VMEM((PARTS * COLORS, 1, chunk), jnp.float32),
            pltpu.VMEM((1, n_vec), jnp.bfloat16),
            pltpu.VMEM((1, n_vec), jnp.float32),
            pltpu.VMEM((4, 1, n_vec // 2), jnp.float32),
            pltpu.VMEM((5, 1, n_vec // 2), jnp.float32),
            pltpu.VMEM((1, n_vec), jnp.float32),
            pltpu.VMEM((1, 128), jnp.float32),
            pltpu.VMEM((DEVICES, 1, 128), jnp.float32),
            pltpu.VMEM((1, min(chunk // CUTS, WIDTH)), jnp.float32),
            pltpu.SMEM((1,), jnp.float32),
            pltpu.VMEM((2, 128), jnp.float32),
            dma((2 * COLORS,)), dma((2 * COLORS,)), dma((COLORS,)),
            dma, dma((SWAPS * COLORS,)), dma((CUTS * COLORS,)),
            dma((3 * COLORS,)), dma((4 * COLORS,)), dma, dma((2 * COLORS,)),
            dma, dma((PARTS * COLORS,)), dma((CUTS * COLORS,)), dma,
            dma, dma, dma((5,)), dma, dma, dma, dma, dma,
        ],
        compiler_params=pltpu.CompilerParams(
            collective_id=0, has_side_effects=True, vmem_limit_bytes=63 * 1024 * 1024),
        name="scatter_sum",
    )(g_mat, g_vec, learn_rate.reshape(1))
    return out, vec, scales


def adam_moments(grad, m, v):
    new_m = ADAM_BETA1 * m + (1.0 - ADAM_BETA1) * grad
    new_v = ADAM_BETA2 * v + (1.0 - ADAM_BETA2) * grad * grad
    return new_m, new_v


def adam_param(p, m, v, rate, decay):
    direction = (m / BIAS_ONE) / (jnp.sqrt(v / BIAS_TWO) + ADAM_EPS)
    return p - rate * (direction + decay * p)


def gather_kernel(axis_name, grad, p, m, v, scales_in, out, m_out, v_out, p_out, g_buf, p_buf, scales,
                  scales_sem, load_sem, s_sem, r_sem, ds_sem, dr_sem):
    own = COLORS * PARTS
    rows = p.shape[1]
    tile = rows // 2
    step = min(tile // 2, ROWS)
    me = lax.axis_index(axis_name)
    deltas = [s * (1 - 2 * lax.rem(me // s, 2)) for s in STRIDES]
    partner = me + 1 - 2 * lax.rem(me, 2)
    peers = [me + d for d in deltas]

    barrier = pltpu.get_barrier_semaphore()
    for dev in (partner, *peers):
        pl.semaphore_signal(barrier, inc=1, device_id=(dev,), device_id_type=MESH_ID)

    def fetch(n):
        q, color, h = n // (2 * COLORS), n // 2 % COLORS, n % 2
        i = color * PARTS + q
        s = pl.ds(h * tile, tile)
        p_dst = p_out.at[i, s] if i < KEEP else p_buf.at[h]
        for src, dst in ((grad, g_buf.at[h]), (m, m_out.at[i, s]), (v, v_out.at[i, s]), (p, p_dst)):
            pltpu.make_async_copy(src.at[i, s], dst, load_sem.at[h]).start()

    def arrived(n):
        pltpu.make_async_copy(m.at[pl.ds(0, 2)], m_out.at[pl.ds(0, 2)], load_sem.at[n % 2]).wait()

    def across(index):
        return pltpu.make_async_remote_copy(
            src_ref=out.at[index], dst_ref=out.at[index], send_sem=ds_sem, recv_sem=dr_sem,
            device_id=(partner,), device_id_type=MESH_ID)

    def route(stage, axis):
        b1, b2 = (axis - 2) % 3, (axis - 1) % 3
        color = (axis, b2, b2, b1, b1, b1, b1)[stage]
        flips = ((), (), (b2,), (), (b1,), (b2,), (b1, b2))[stage]
        return color, sum((deltas[f] for f in flips), me)

    def push(stage, axis, q, span=None):
        color, owner = route(stage, axis)
        index = owner * own + color * PARTS + q
        place = (3 * q, 3 * q + 1, 3 * PARTS + q, 3 * q + 2)[stage] if stage < 4 else stage * PARTS + q
        ref = out.at[index] if span is None else out.at[index, span]
        return pltpu.make_async_remote_copy(
            src_ref=ref, dst_ref=ref, send_sem=s_sem, recv_sem=r_sem.at[axis * PLACES + lax.rem(place, PLACES)],
            device_id=(peers[axis],), device_id_type=MESH_ID)

    def land(stage, axis, q):
        color, owner = route(stage, axis)
        push(stage, axis, q).wait_recv()
        across((owner + deltas[axis]) * own + color * PARTS + q).start()

    def update(color, q, h, first, count):
        i = color * PARTS + q

        @pl.loop(first // step, (first + count) // step)
        def _(r):
            t = pl.ds(pl.multiple_of(r * step, step), step)
            s = pl.ds(pl.multiple_of(h * tile + r * step, step), step)
            new_m, new_v = adam_moments(g_buf[h, t, :] * scales[0:1, :], m_out[i, s, :], v_out[i, s, :])
            m_out[i, s, :] = new_m
            v_out[i, s, :] = new_v
            old_p = p_out[i, s, :] if i < KEEP else p_buf[h, t, :]
            new_p = adam_param(old_p, new_m, new_v, scales[1:2, :], WEIGHT_DECAY)
            if i < KEEP:
                p_out[i, s, :] = new_p
            out[me * own + i, s, :] = new_p.astype(jnp.bfloat16)

    def each(count, body):
        lax.fori_loop(0, count, lambda i, c: (body(i), c)[1], 0)

    scales_load = pltpu.make_async_copy(scales_in, scales, scales_sem)
    scales_load.start()
    fetch(0)
    scales_load.wait()
    fetch(1)
    for n in range(2 * own):
        q, color, h = n // (2 * COLORS), n // 2 % COLORS, n % 2
        cuts = 2 if n < 2 else 1
        arrived(n)
        for c in range(cuts):
            count = tile // cuts
            update(color, q, h, c * count, count)
            if n == 0 and c == 0:
                pl.semaphore_wait(barrier, 4)
            for k, stage in enumerate((0, 1, 3)):
                push(stage, (color + k) % 3, q, pl.ds(h * tile + c * count, count)).start()
        if h:
            across(me * own + color * PARTS + q).start()
        if n + 2 < 2 * own:
            fetch(n + 2)

    def own_stage(q):
        for axis in range(3):
            for stage in (0, 1, 3):
                land(stage, axis, q)
            push(2, (axis + 1) % 3, q).start()

    each(PARTS, own_stage)
    for stage, last in ((4, 2), (5, 4), (6, 5), (None, 6)):
        def body(q, stage=stage, last=last):
            for axis in range(3):
                if stage:
                    push(stage, axis, q).start()
                land(last, axis, q)
        each(PARTS, body)

    sent = out.at[pl.ds(0, 7 * own)]
    pltpu.make_async_remote_copy(
        src_ref=sent, dst_ref=sent, send_sem=s_sem, recv_sem=r_sem.at[0],
        device_id=(partner,), device_id_type=MESH_ID).wait_send()
    half = pltpu.make_async_remote_copy(
        src_ref=out.at[pl.ds(0, 8 * own)], dst_ref=out.at[pl.ds(0, 8 * own)], send_sem=ds_sem, recv_sem=dr_sem,
        device_id=(partner,), device_id_type=MESH_ID)
    half.wait_recv()
    half.wait_send()


def write_kernel(held, m_held, v_held, p_held, p, scales_in, g_vec, p_vec, m_vec, v_vec,
                 out, p_out, m_out, v_out, pv_out, mv_out, vv_out,
                 p_buf, vec_buf, scales, in_sem, out_sem, sem, vec_sem, vec_out_sem, scales_sem):
    own, rows, _ = p.shape
    step = min(rows, ROWS)
    span = held.shape[0] // own

    tile = rows // 2
    tiles = 2 * (own - KEEP)

    def place(n):
        return KEEP + n // 2, pl.ds(n % 2 * tile, tile)

    def load(n):
        return pltpu.make_async_copy(p.at[place(n)], p_buf.at[n % RING], in_sem.at[n % RING])

    def store(n):
        return pltpu.make_async_copy(p_buf.at[n % RING], p_out.at[place(n)], out_sem.at[n % RING])

    def copies(i):
        part = pl.ds(i * span, span)
        pairs = [(held.at[part], out.at[part]), (m_held.at[i], m_out.at[i]), (v_held.at[i], v_out.at[i])]
        if i < KEEP:
            pairs.append((p_held.at[i], p_out.at[i]))
        return [pltpu.make_async_copy(src, dst, sem.at[k, i % AHEAD]) for k, (src, dst) in enumerate(pairs)]

    scales_load = pltpu.make_async_copy(scales_in, scales, scales_sem)
    scales_load.start()
    vec_loads = [pltpu.make_async_copy(a, vec_buf.at[k], vec_sem.at[k])
                 for k, a in enumerate((p_vec, m_vec, v_vec, g_vec))]
    vec_stores = [pltpu.make_async_copy(vec_buf.at[k], a, vec_out_sem.at[k])
                  for k, a in enumerate((pv_out, mv_out, vv_out))]
    def vec_update():
        for copy in vec_loads:
            copy.wait()

        @pl.loop(0, g_vec.shape[1] // 1024)
        def _(i):
            s = pl.ds(pl.multiple_of(i * 1024, 1024), 1024)
            new_m, new_v = adam_moments(vec_buf[3, :, s] * scales[0:1, 0:1], vec_buf[1, :, s], vec_buf[2, :, s])
            vec_buf[1, :, s] = new_m
            vec_buf[2, :, s] = new_v
            vec_buf[0, :, s] = adam_param(vec_buf[0, :, s], new_m, new_v, scales[1:2, 0:1], 0.0)

        for copy in vec_stores:
            copy.start()

    for n in range(RING - 1):
        load(n).start()
    for copy in vec_loads:
        copy.start()
    for i in range(AHEAD):
        for copy in copies(i):
            copy.start()
    scales_load.wait()
    for n in range(tiles):
        load(n).wait()
        i = KEEP + n // 2

        @pl.loop(0, tile // step)
        def _(r):
            t = pl.ds(pl.multiple_of(r * step, step), step)
            s = pl.ds(pl.multiple_of(n % 2 * tile + r * step, step), step)
            p_buf[n % RING, t, :] = adam_param(
                p_buf[n % RING, t, :], m_held[i, s, :], v_held[i, s, :], scales[1:2, :], WEIGHT_DECAY)

        store(n).start()
        if n + RING - 1 < tiles:
            if n:
                store(n - 1).wait()
            load(n + RING - 1).start()
        for j in range(n * (own - AHEAD) // tiles, (n + 1) * (own - AHEAD) // tiles):
            for copy in copies(j):
                copy.wait()
            for copy in copies(j + AHEAD):
                copy.start()
        if n == 0:
            vec_update()
    for n in range(tiles - RING, tiles):
        store(n).wait()
    for i in range(own - AHEAD, own):
        for copy in copies(i):
            copy.wait()
    for copy in vec_stores:
        copy.wait()


def gather_update(grad, p, m, v, scales, grad_vec, p_vec, m_vec, v_vec, axis_name, group_size):
    own = COLORS * PARTS
    piece = p.shape[0]
    n_vec = p_vec.shape[0]
    rows = piece // (own * 128)
    dma = pltpu.SemaphoreType.DMA
    any_spec = pl.BlockSpec(memory_space=pl.ANY)
    vmem_spec = pl.BlockSpec(memory_space=pltpu.VMEM)
    grad, p, m, v = (a.reshape(own, rows, 128) for a in (grad, p, m, v))
    p_vec, m_vec, v_vec = (a.reshape(1, n_vec) for a in (p_vec, m_vec, v_vec))
    full, new_m, new_v, new_p = pl.pallas_call(
        functools.partial(gather_kernel, axis_name),
        out_shape=(pltpu.VMEM((group_size * own, rows, 128), jnp.bfloat16),
                   pltpu.VMEM((own, rows, 128), jnp.float32),
                   pltpu.VMEM((own, rows, 128), jnp.float32),
                   pltpu.VMEM((KEEP, rows, 128), jnp.float32)),
        in_specs=[any_spec] * 5,
        out_specs=[vmem_spec] * 4,
        scratch_shapes=[
            pltpu.VMEM((2, rows // 2, 128), jnp.float32), pltpu.VMEM((2, rows // 2, 128), jnp.float32),
            pltpu.VMEM((2, 128), jnp.float32), dma, dma((2,)),
            dma, dma((3 * PLACES,)), dma, dma],
        compiler_params=pltpu.CompilerParams(
            collective_id=1, has_side_effects=True, vmem_limit_bytes=SMALL_VMEM),
        name="gather_update",
    )(grad, p, m, v, scales)
    flat = jax.ShapeDtypeStruct((own, rows, 128), jnp.float32)
    line = jax.ShapeDtypeStruct((1, n_vec), jnp.float32)
    full, new_p, new_m, new_v, *vecs = pl.pallas_call(
        write_kernel,
        out_shape=(jax.ShapeDtypeStruct(full.shape, full.dtype), flat, flat, flat, line, line, line),
        in_specs=[vmem_spec] * 4 + [any_spec] * 6,
        out_specs=[any_spec] * 7,
        scratch_shapes=[
            pltpu.VMEM((RING, rows // 2, 128), jnp.float32), pltpu.VMEM((4, 1, n_vec), jnp.float32),
            pltpu.VMEM((2, 128), jnp.float32),
            dma((RING,)), dma((RING,)), dma((4, AHEAD)), dma((4,)), dma((3,)), dma],
        compiler_params=pltpu.CompilerParams(vmem_limit_bytes=SMALL_VMEM),
        name="write_out",
    )(*(pltpu.with_memory_space_constraint(a, pltpu.VMEM) for a in (full, new_m, new_v, new_p)),
      p, scales, grad_vec, p_vec, m_vec, v_vec)
    return (*(a.reshape(piece) for a in (new_p, new_m, new_v)), *(a.reshape(n_vec) for a in vecs),
            full.reshape(group_size * piece))


def solution(mesh):
    axis_name = mesh.axis_names[0]
    group_size = mesh.shape[axis_name]

    def local_step(g_mat, g_vec, p_mat, m_mat, v_mat, p_vec, m_vec, v_vec, learn_rate):
        grad_mat, grad_vec, scales = scatter_sum(g_mat, g_vec, learn_rate, axis_name, group_size)
        return gather_update(grad_mat, p_mat, m_mat, v_mat, scales, grad_vec, p_vec, m_vec, v_vec, axis_name, group_size)

    return jax.shard_map(
        local_step,
        mesh=mesh,
        in_specs=(P(axis_name, None), P(axis_name, None), P(axis_name), P(axis_name), P(axis_name), P(), P(), P(), P()),
        out_specs=(P(axis_name), P(axis_name), P(axis_name), P(), P(), P(), P()),
        check_vma=False,
    )
```

```python
import functools

import jax
import jax.numpy as jnp
from jax import lax
from jax.experimental import pallas as pl
from jax.experimental.pallas import tpu as pltpu
from jax.sharding import PartitionSpec as P

STEP = 10
ADAM_BETA1 = 0.9
ADAM_BETA2 = 0.98
ADAM_EPS = 1e-8
WEIGHT_DECAY = 0.01
MAX_NORM = 1.0
NORM_EPS = 1e-6
BIAS_ONE = 1.0 - ADAM_BETA1 ** STEP
BIAS_TWO = 1.0 - ADAM_BETA2 ** STEP

MESH_ID = pl.DeviceIdType.MESH
COLORS = 3
PARTS = 4
STRIDES = (2, 4, 8)
STEPS = 8 * PARTS
DEVICES = 16
WIDTH = 4096
ROWS = 64
SMALL_VMEM = 1792 * 1024
RING = 5
KEEP = 4
AHEAD = 3
SWAPS = 8
PLACES = 20
CUTS = 4
MEAN_SCALE = 1.0 / 16.0


def scatter_kernel(axis_name, piece, g, gv, lr, out, pg, vec_out, scale_out,
                   a_buf, b_buf, e_buf, stage, r1, r2, r3, v_in, v_full, v_acc, v_get, v_mean, n_put, n_get, squares, lr_smem, scale_buf,
                   a_sem, b_sem, e_sem, ds_sem, dr_sem, dc_sem, s1_sem, r1_sem, s2_sem, r2_sem, s3_sem, r3_sem, rc_sem, o_sem,
                   vi_sem, vs_sem, vr_sem, ns_sem, nr_sem, vo_sem, lr_sem, so_sem):
    chunk = piece // (COLORS * PARTS)
    width = min(chunk // CUTS, WIDTH)
    part = chunk // CUTS
    n_vec = gv.shape[1]
    n_half = n_vec // 2
    me = lax.axis_index(axis_name)
    core = lax.rem(me, 2)
    core_step = 1 - 2 * core
    deltas = [s * (1 - 2 * lax.rem(me // s, 2)) for s in STRIDES]
    partner = me + core_step
    peers = [me + d for d in deltas]

    barrier = pltpu.get_barrier_semaphore()
    for dev in (partner, *peers):
        pl.semaphore_signal(barrier, inc=1, device_id=(dev,), device_id_type=MESH_ID)

    def offset(color, t):
        unit = t // PARTS
        f1 = 1 - unit // 4
        f2 = 1 - lax.rem(unit // 2, 2)
        f3 = 1 - lax.rem(unit, 2)
        d1, d2, d3 = (deltas[(color + k) % 3] for k in range(3))
        owner = me + f1 * d1 + f2 * d2 + f3 * d3
        return owner * piece + (color * PARTS + lax.rem(t, PARTS)) * chunk

    def cut(ref, start):
        return ref.at[:, pl.ds(pl.multiple_of(start, 1024), chunk)]

    def swap(color, t):
        return pltpu.make_async_remote_copy(
            src_ref=cut(g, offset(color, t) + core_step * piece),
            dst_ref=cut(pg, (color * STEPS + t) * chunk),
            send_sem=ds_sem, recv_sem=dr_sem.at[color * SWAPS + lax.rem(t, SWAPS)],
            device_id=(partner,), device_id_type=MESH_ID)

    def swap_early(color, t):
        k = color * 2 + t
        return pltpu.make_async_remote_copy(
            src_ref=cut(g, offset(color, t) + core_step * piece), dst_ref=b_buf.at[k],
            send_sem=ds_sem, recv_sem=dr_sem.at[color * SWAPS + t],
            device_id=(partner,), device_id_type=MESH_ID)

    def swap_cut(color, i):
        s = pl.ds(i * part, part)
        return pltpu.make_async_remote_copy(
            src_ref=e_buf.at[color, :, s], dst_ref=b_buf.at[color * 2, :, s],
            send_sem=ds_sem, recv_sem=dc_sem.at[color * CUTS + i],
            device_id=(partner,), device_id_type=MESH_ID)

    def load_e(color):
        return pltpu.make_async_copy(
            cut(g, offset(color, 0) + core_step * piece), e_buf.at[color], e_sem.at[color])

    def push_cut(color, i):
        k, j = color * 3, color * 4 * PARTS
        s = pl.ds(i * part, part)
        return push(stage.at[k, :, s], r1.at[j, :, s], s1_sem.at[k], r1_sem.at[color * 4], color)

    def load_a(color, t):
        k = color * 2 + lax.rem(t, 2)
        return pltpu.make_async_copy(cut(g, offset(color, t)), a_buf.at[k], a_sem.at[k])

    def load_b(color, t):
        k = color * 2 + lax.rem(t, 2)
        return pltpu.make_async_copy(cut(pg, (color * STEPS + t) * chunk), b_buf.at[k], b_sem.at[k])

    def push(src, dst, send_sem, recv_sem, axis):
        return pltpu.make_async_remote_copy(
            src_ref=src, dst_ref=dst, send_sem=send_sem, recv_sem=recv_sem,
            device_id=(peers[axis],), device_id_type=MESH_ID)

    def push1(color, t):
        k = color * 3 + lax.rem(t, 3)
        j = color * 4 * PARTS + t
        return push(stage.at[k], r1.at[j], s1_sem.at[k], r1_sem.at[color * 4 + t // PARTS], color)

    def push2(color, t):
        j = color * 2 * PARTS + t - 4 * PARTS
        return push(r1.at[color * 4 * PARTS + t - 4 * PARTS], r2.at[j], s2_sem,
                    r2_sem.at[color * 2 + t // PARTS - 4], (color + 1) % 3)

    def push3(color, t):
        j = color * PARTS + t - 6 * PARTS
        return push(r1.at[color * 4 * PARTS + t - 4 * PARTS], r3.at[j], s3_sem, r3_sem.at[j], (color + 2) % 3)

    def push3_cut(color, i):
        s = pl.ds(i * part, part)
        return push(r1.at[color * 4 * PARTS + 3 * PARTS - 1, :, s], r3.at[color * PARTS + PARTS - 1, :, s],
                    s3_sem, rc_sem.at[color * CUTS + i], (color + 2) % 3)

    def unit1(color, u):
        span = r1.at[pl.ds((color * 4 + u) * PARTS, PARTS)]
        return push(span, span, s2_sem, r1_sem.at[color * 4 + u], color)

    def unit2(color, w):
        span = r2.at[pl.ds((color * 2 + w) * PARTS, PARTS)]
        return push(span, span, s2_sem, r2_sem.at[color * 2 + w], (color + 1) % 3)

    def store(color, t):
        j = color * PARTS + t - 7 * PARTS
        return pltpu.make_async_copy(r3.at[j], cut(out, j * chunk), o_sem)

    def add_up(color, t, dst, extra, last=False, span=None):
        k = color * 2 + lax.rem(t, 2)
        first, count = span or (0, chunk)

        @pl.loop(first // width, (first + count) // width)
        def _(i):
            s = pl.ds(pl.multiple_of(i * width, width), width)
            acc = a_buf[k, :, s].astype(jnp.float32) + b_buf[k, :, s].astype(jnp.float32)
            for ref, j in extra:
                acc = acc + ref[j, :, s]
            if last:
                acc = acc * MEAN_SCALE
                squares[...] += acc * acc
            dst[0][dst[1], :, s] = acc

    def half(ref, which):
        return ref.at[:, pl.ds(pl.multiple_of(which * n_half, 1024), n_half)]

    def vec_push(k):
        src = half(v_full, 1 - core) if k == 0 else half(v_mean, core) if k == 4 else v_acc.at[k]
        return pltpu.make_async_remote_copy(
            src_ref=src, dst_ref=half(v_mean, core) if k == 4 else v_get.at[k],
            send_sem=vs_sem, recv_sem=vr_sem.at[k],
            device_id=((partner, *peers, partner)[k],), device_id_type=MESH_ID)

    def norm_push(k):
        return pltpu.make_async_remote_copy(
            src_ref=n_put, dst_ref=n_get.at[me], send_sem=ns_sem, recv_sem=nr_sem,
            device_id=(lax.rem(me + k, DEVICES),), device_id_type=MESH_ID)

    def vec_loop(count, body):
        @pl.loop(0, count // 1024)
        def _(i):
            body(pl.multiple_of(i * 1024, 1024))

    def vec_turn(k):
        def body(i):
            s = pl.ds(i, 1024)
            here = pl.ds(pl.multiple_of(core * n_half + i, 1024), 1024)
            total = (v_acc[k, :, s] if k else v_full[:, here]) + v_get[k, :, s]
            if k < 3:
                v_acc[k + 1, :, s] = total
            else:
                v_mean[:, here] = total * MEAN_SCALE
        vec_push(k).wait_recv()
        vec_loop(n_half, body)
        vec_push(k + 1).start()

    def ready(color, t):
        load_a(color, t).wait()
        load_b(color, t).wait()

    def refill(color, t):
        load_a(color, t).start()
        swap(color, t).wait_recv()
        load_b(color, t).start()

    def more_swap(color, t):
        swap(color, t).start()

    for color in range(COLORS):
        load_e(color).start()
    for t in range(2):
        for color in range(COLORS):
            load_a(color, t).start()
    vec_load = pltpu.make_async_copy(gv, v_in, vi_sem)
    vec_load.start()
    lr_load = pltpu.make_async_copy(lr, lr_smem, lr_sem)
    lr_load.start()
    squares[...] = jnp.zeros_like(squares)
    for color in range(COLORS):
        load_e(color).wait()
    pl.semaphore_wait(barrier, 4)
    for i in range(CUTS):
        for color in range(COLORS):
            swap_cut(color, i).start()
    for color in range(COLORS):
        swap_early(color, 1).start()
    for t in range(2, 4):
        for color in range(COLORS):
            swap(color, t).start()
    for i in range(CUTS):
        for color in range(COLORS):
            if i == 0:
                load_a(color, 0).wait()
            swap_cut(color, i).wait_recv()
            add_up(color, 0, (stage, color * 3), (), span=(i * part, part))
            push_cut(color, i).start()
    for color in range(COLORS):
        more_swap(color, 4)
        refill(color, 2)

    def phase_one(t, first, early=False):
        for color in range(COLORS):
            if early:
                load_a(color, t).wait()
                swap_early(color, t).wait_recv()
            else:
                ready(color, t)
            if not first:
                push1(color, t - 3).wait_send()
            add_up(color, t, (stage, color * 3 + lax.rem(t, 3)), ())
            push1(color, t).start()
            more_swap(color, t + 4)
            refill(color, t + 2)

    def run(lo, hi, body):
        lax.fori_loop(lo, hi, lambda t, c: (body(t), c)[1], 0)

    phase_one(1, True, True)
    phase_one(2, True)
    vec_load.wait()

    def widen(i):
        s = pl.ds(i, 1024)
        v_full[:, s] = v_in[:, s].astype(jnp.float32)

    vec_loop(n_vec, widen)
    vec_push(0).start()
    for k in range(4):
        run(3 * k + 3, 3 * k + 6, lambda t: phase_one(t, False))
        vec_turn(k)
    run(15, 4 * PARTS, lambda t: phase_one(t, False))
    vec_push(4).wait_recv()
    vec_store = pltpu.make_async_copy(v_mean, vec_out, vo_sem)
    vec_store.start()

    def phase_two(t):
        for color in range(COLORS):
            ready(color, t)
            j = color * 4 * PARTS + t - 4 * PARTS
            add_up(color, t, (r1, j), ((r1, j),))
            push2(color, t).start()
            more_swap(color, t + 4)
            refill(color, t + 2)

    def phase_three(t, cuts):
        for color in range(COLORS):
            ready(color, t)
            j = color * 4 * PARTS + t - 4 * PARTS
            add_up(color, t, (r1, j), ((r1, j), (r2, color * 2 * PARTS + t - 6 * PARTS)))
            if cuts:
                for i in range(CUTS):
                    push3_cut(color, i).start()
            else:
                push3(color, t).start()
            more_swap(color, t + 4)
            refill(color, t + 2)

    def finish(color, t, span=None):
        j = color * PARTS + t - 7 * PARTS
        add_up(color, t, (r3, j), (
            (r1, color * 4 * PARTS + t - 4 * PARTS),
            (r2, color * 2 * PARTS + t - 6 * PARTS),
            (r3, j)), last=True, span=span)

    def phase_four(t, fill):
        for color in range(COLORS):
            ready(color, t)
            push3(color, t - PARTS).wait_recv()
            finish(color, t)
            store(color, t).start()
            if fill:
                refill(color, t + 2)

    for unit in range(4, 8):
        for color in range(COLORS):
            unit1(color, unit - 4).wait_recv()
            if unit >= 6:
                unit2(color, unit - 6).wait_recv()
        lo = unit * PARTS
        if unit < 6:
            run(lo, lo + PARTS, phase_two)
        elif unit == 6:
            run(lo, lo + PARTS - 1, lambda t: phase_three(t, False))
            phase_three(lo + PARTS - 1, True)
        else:
            run(lo, lo + PARTS - 2, lambda t: phase_four(t, True))
            phase_four(lo + PARTS - 2, False)
    for color in range(COLORS):
        ready(color, STEPS - 1)
    for i in range(CUTS):
        for color in range(COLORS):
            push3_cut(color, i).wait_recv()
            finish(color, STEPS - 1, span=(i * part, part))
    for color in range(COLORS):
        store(color, STEPS - 1).start()

    vec_sq = jnp.sum(v_mean[...] * v_mean[...], axis=1, keepdims=True)
    mine = jnp.broadcast_to(jnp.sum(squares[...], axis=1, keepdims=True), (1, 128))
    n_put[...] = mine
    n_get[me] = mine
    for k in range(1, DEVICES):
        norm_push(k).start()
    rest = pltpu.make_async_remote_copy(
        src_ref=n_get.at[pl.ds(0, DEVICES - 1)], dst_ref=n_get.at[pl.ds(0, DEVICES - 1)],
        send_sem=ns_sem, recv_sem=nr_sem, device_id=(partner,), device_id_type=MESH_ID)
    rest.wait_recv()
    norm_sq = n_get[0]
    for k in range(1, DEVICES):
        norm_sq = norm_sq + n_get[k]
    norm_sq = norm_sq + vec_sq
    scale_buf[0:1, :] = jnp.minimum(1.0, MAX_NORM / (jnp.sqrt(norm_sq) + NORM_EPS))
    lr_load.wait()
    scale_buf[1:2, :] = jnp.full((1, 128), lr_smem[0])
    scale_store = pltpu.make_async_copy(scale_buf, scale_out, so_sem)
    scale_store.start()

    def drain(lo, hi, wait):
        def body(t):
            for color in range(COLORS):
                wait(color, t)
        run(lo, hi, body)

    drain(4 * PARTS - 3, 4 * PARTS, lambda c, t: push1(c, t).wait_send())
    push(r2, r2, s2_sem, r2_sem.at[0], 0).wait_send()
    push(r3, r3, s3_sem, r3_sem.at[0], 0).wait_send()
    pltpu.make_async_remote_copy(
        src_ref=pg, dst_ref=pg, send_sem=ds_sem, recv_sem=dr_sem.at[0],
        device_id=(partner,), device_id_type=MESH_ID).wait_send()
    pltpu.make_async_copy(out, out, o_sem).wait()
    push(v_get, v_get, vs_sem, vr_sem.at[0], 0).wait_send()
    rest.wait_send()
    vec_store.wait()
    scale_store.wait()


def scatter_sum(g_mat, g_vec, learn_rate, axis_name, group_size):
    total = g_mat.shape[1]
    n_vec = g_vec.shape[1]
    piece = total // group_size
    chunk = piece // (COLORS * PARTS)
    dma = pltpu.SemaphoreType.DMA
    any_spec = pl.BlockSpec(memory_space=pl.ANY)
    out, _, vec, scales = pl.pallas_call(
        functools.partial(scatter_kernel, axis_name, piece),
        out_shape=(jax.ShapeDtypeStruct((1, piece), jnp.float32),
                   jax.ShapeDtypeStruct((1, total // 2), jnp.bfloat16),
                   jax.ShapeDtypeStruct((1, n_vec), jnp.float32),
                   jax.ShapeDtypeStruct((2, 128), jnp.float32)),
        in_specs=[any_spec] * 3,
        out_specs=[any_spec] * 4,
        scratch_shapes=[
            pltpu.VMEM((2 * COLORS, 1, chunk), jnp.bfloat16),
            pltpu.VMEM((2 * COLORS, 1, chunk), jnp.bfloat16),
            pltpu.VMEM((COLORS, 1, chunk), jnp.bfloat16),
            pltpu.VMEM((3 * COLORS, 1, chunk), jnp.float32),
            pltpu.VMEM((4 * PARTS * COLORS, 1, chunk), jnp.float32),
            pltpu.VMEM((2 * PARTS * COLORS, 1, chunk), jnp.float32),
            pltpu.VMEM((PARTS * COLORS, 1, chunk), jnp.float32),
            pltpu.VMEM((1, n_vec), jnp.bfloat16),
            pltpu.VMEM((1, n_vec), jnp.float32),
            pltpu.VMEM((4, 1, n_vec // 2), jnp.float32),
            pltpu.VMEM((5, 1, n_vec // 2), jnp.float32),
            pltpu.VMEM((1, n_vec), jnp.float32),
            pltpu.VMEM((1, 128), jnp.float32),
            pltpu.VMEM((DEVICES, 1, 128), jnp.float32),
            pltpu.VMEM((1, min(chunk // CUTS, WIDTH)), jnp.float32),
            pltpu.SMEM((1,), jnp.float32),
            pltpu.VMEM((2, 128), jnp.float32),
            dma((2 * COLORS,)), dma((2 * COLORS,)), dma((COLORS,)),
            dma, dma((SWAPS * COLORS,)), dma((CUTS * COLORS,)),
            dma((3 * COLORS,)), dma((4 * COLORS,)), dma, dma((2 * COLORS,)),
            dma, dma((PARTS * COLORS,)), dma((CUTS * COLORS,)), dma,
            dma, dma, dma((5,)), dma, dma, dma, dma, dma,
        ],
        compiler_params=pltpu.CompilerParams(
            collective_id=0, has_side_effects=True, vmem_limit_bytes=63 * 1024 * 1024),
        name="scatter_sum",
    )(g_mat, g_vec, learn_rate.reshape(1))
    return out, vec, scales


def adam_moments(grad, m, v):
    new_m = ADAM_BETA1 * m + (1.0 - ADAM_BETA1) * grad
    new_v = ADAM_BETA2 * v + (1.0 - ADAM_BETA2) * grad * grad
    return new_m, new_v


def adam_param(p, m, v, rate, decay):
    direction = (m / BIAS_ONE) / (jnp.sqrt(v / BIAS_TWO) + ADAM_EPS)
    return p - rate * (direction + decay * p)


def gather_kernel(axis_name, grad, p, m, v, scales_in, out, m_out, v_out, p_out, g_buf, p_buf, scales,
                  scales_sem, load_sem, s_sem, r_sem, ds_sem, dr_sem):
    own = COLORS * PARTS
    rows = p.shape[1]
    tile = rows // 2
    step = min(tile // 2, ROWS)
    me = lax.axis_index(axis_name)
    deltas = [s * (1 - 2 * lax.rem(me // s, 2)) for s in STRIDES]
    partner = me + 1 - 2 * lax.rem(me, 2)
    peers = [me + d for d in deltas]

    barrier = pltpu.get_barrier_semaphore()
    for dev in (partner, *peers):
        pl.semaphore_signal(barrier, inc=1, device_id=(dev,), device_id_type=MESH_ID)

    def fetch(n):
        q, color, h = n // (2 * COLORS), n // 2 % COLORS, n % 2
        i = color * PARTS + q
        s = pl.ds(h * tile, tile)
        p_dst = p_out.at[i, s] if i < KEEP else p_buf.at[h]
        for src, dst in ((grad, g_buf.at[h]), (m, m_out.at[i, s]), (v, v_out.at[i, s]), (p, p_dst)):
            pltpu.make_async_copy(src.at[i, s], dst, load_sem.at[h]).start()

    def arrived(n):
        pltpu.make_async_copy(m.at[pl.ds(0, 2)], m_out.at[pl.ds(0, 2)], load_sem.at[n % 2]).wait()

    def across(index):
        return pltpu.make_async_remote_copy(
            src_ref=out.at[index], dst_ref=out.at[index], send_sem=ds_sem, recv_sem=dr_sem,
            device_id=(partner,), device_id_type=MESH_ID)

    def route(stage, axis):
        b1, b2 = (axis - 2) % 3, (axis - 1) % 3
        color = (axis, b2, b2, b1, b1, b1, b1)[stage]
        flips = ((), (), (b2,), (), (b1,), (b2,), (b1, b2))[stage]
        return color, sum((deltas[f] for f in flips), me)

    def push(stage, axis, q, span=None):
        color, owner = route(stage, axis)
        index = owner * own + color * PARTS + q
        place = (3 * q, 3 * q + 1, 3 * PARTS + q, 3 * q + 2)[stage] if stage < 4 else stage * PARTS + q
        ref = out.at[index] if span is None else out.at[index, span]
        return pltpu.make_async_remote_copy(
            src_ref=ref, dst_ref=ref, send_sem=s_sem, recv_sem=r_sem.at[axis * PLACES + lax.rem(place, PLACES)],
            device_id=(peers[axis],), device_id_type=MESH_ID)

    def land(stage, axis, q):
        color, owner = route(stage, axis)
        push(stage, axis, q).wait_recv()
        across((owner + deltas[axis]) * own + color * PARTS + q).start()

    def update(color, q, h, first, count):
        i = color * PARTS + q

        @pl.loop(first // step, (first + count) // step)
        def _(r):
            t = pl.ds(pl.multiple_of(r * step, step), step)
            s = pl.ds(pl.multiple_of(h * tile + r * step, step), step)
            new_m, new_v = adam_moments(g_buf[h, t, :] * scales[0:1, :], m_out[i, s, :], v_out[i, s, :])
            m_out[i, s, :] = new_m
            v_out[i, s, :] = new_v
            old_p = p_out[i, s, :] if i < KEEP else p_buf[h, t, :]
            new_p = adam_param(old_p, new_m, new_v, scales[1:2, :], WEIGHT_DECAY)
            if i < KEEP:
                p_out[i, s, :] = new_p
            out[me * own + i, s, :] = new_p.astype(jnp.bfloat16)

    def each(count, body):
        lax.fori_loop(0, count, lambda i, c: (body(i), c)[1], 0)

    scales_load = pltpu.make_async_copy(scales_in, scales, scales_sem)
    scales_load.start()
    fetch(0)
    scales_load.wait()
    fetch(1)
    for n in range(2 * own):
        q, color, h = n // (2 * COLORS), n // 2 % COLORS, n % 2
        cuts = 2 if n < 2 else 1
        arrived(n)
        for c in range(cuts):
            count = tile // cuts
            update(color, q, h, c * count, count)
            if n == 0 and c == 0:
                pl.semaphore_wait(barrier, 4)
            for k, stage in enumerate((0, 1, 3)):
                push(stage, (color + k) % 3, q, pl.ds(h * tile + c * count, count)).start()
        if h:
            across(me * own + color * PARTS + q).start()
        if n + 2 < 2 * own:
            fetch(n + 2)

    def own_stage(q):
        for axis in range(3):
            for stage in (0, 1, 3):
                land(stage, axis, q)
            push(2, (axis + 1) % 3, q).start()

    each(PARTS, own_stage)
    for stage, last in ((4, 2), (5, 4), (6, 5), (None, 6)):
        def body(q, stage=stage, last=last):
            for axis in range(3):
                if stage:
                    push(stage, axis, q).start()
                land(last, axis, q)
        each(PARTS, body)

    sent = out.at[pl.ds(0, 7 * own)]
    pltpu.make_async_remote_copy(
        src_ref=sent, dst_ref=sent, send_sem=s_sem, recv_sem=r_sem.at[0],
        device_id=(partner,), device_id_type=MESH_ID).wait_send()
    half = pltpu.make_async_remote_copy(
        src_ref=out.at[pl.ds(0, 8 * own)], dst_ref=out.at[pl.ds(0, 8 * own)], send_sem=ds_sem, recv_sem=dr_sem,
        device_id=(partner,), device_id_type=MESH_ID)
    half.wait_recv()
    half.wait_send()


def write_kernel(held, m_held, v_held, p_held, p, scales_in, g_vec, p_vec, m_vec, v_vec,
                 out, p_out, m_out, v_out, pv_out, mv_out, vv_out,
                 p_buf, vec_buf, scales, in_sem, out_sem, sem, vec_sem, vec_out_sem, scales_sem):
    own, rows, _ = p.shape
    step = min(rows, ROWS)
    span = held.shape[0] // own

    tile = rows // 2
    tiles = 2 * (own - KEEP)

    def place(n):
        return KEEP + n // 2, pl.ds(n % 2 * tile, tile)

    def load(n):
        return pltpu.make_async_copy(p.at[place(n)], p_buf.at[n % RING], in_sem.at[n % RING])

    def store(n):
        return pltpu.make_async_copy(p_buf.at[n % RING], p_out.at[place(n)], out_sem.at[n % RING])

    def copies(i):
        part = pl.ds(i * span, span)
        pairs = [(held.at[part], out.at[part]), (m_held.at[i], m_out.at[i]), (v_held.at[i], v_out.at[i])]
        if i < KEEP:
            pairs.append((p_held.at[i], p_out.at[i]))
        return [pltpu.make_async_copy(src, dst, sem.at[k, i % AHEAD]) for k, (src, dst) in enumerate(pairs)]

    scales_load = pltpu.make_async_copy(scales_in, scales, scales_sem)
    scales_load.start()
    vec_loads = [pltpu.make_async_copy(a, vec_buf.at[k], vec_sem.at[k])
                 for k, a in enumerate((p_vec, m_vec, v_vec, g_vec))]
    vec_stores = [pltpu.make_async_copy(vec_buf.at[k], a, vec_out_sem.at[k])
                  for k, a in enumerate((pv_out, mv_out, vv_out))]
    def vec_update():
        for copy in vec_loads:
            copy.wait()

        @pl.loop(0, g_vec.shape[1] // 1024)
        def _(i):
            s = pl.ds(pl.multiple_of(i * 1024, 1024), 1024)
            new_m, new_v = adam_moments(vec_buf[3, :, s] * scales[0:1, 0:1], vec_buf[1, :, s], vec_buf[2, :, s])
            vec_buf[1, :, s] = new_m
            vec_buf[2, :, s] = new_v
            vec_buf[0, :, s] = adam_param(vec_buf[0, :, s], new_m, new_v, scales[1:2, 0:1], 0.0)

        for copy in vec_stores:
            copy.start()

    for n in range(RING - 1):
        load(n).start()
    for copy in vec_loads:
        copy.start()
    for i in range(AHEAD):
        for copy in copies(i):
            copy.start()
    scales_load.wait()
    for n in range(tiles):
        load(n).wait()
        i = KEEP + n // 2

        @pl.loop(0, tile // step)
        def _(r):
            t = pl.ds(pl.multiple_of(r * step, step), step)
            s = pl.ds(pl.multiple_of(n % 2 * tile + r * step, step), step)
            p_buf[n % RING, t, :] = adam_param(
                p_buf[n % RING, t, :], m_held[i, s, :], v_held[i, s, :], scales[1:2, :], WEIGHT_DECAY)

        store(n).start()
        if n + RING - 1 < tiles:
            if n:
                store(n - 1).wait()
            load(n + RING - 1).start()
        for j in range(n * (own - AHEAD) // tiles, (n + 1) * (own - AHEAD) // tiles):
            for copy in copies(j):
                copy.wait()
            for copy in copies(j + AHEAD):
                copy.start()
        if n == 0:
            vec_update()
    for n in range(tiles - RING, tiles):
        store(n).wait()
    for i in range(own - AHEAD, own):
        for copy in copies(i):
            copy.wait()
    for copy in vec_stores:
        copy.wait()


def gather_update(grad, p, m, v, scales, grad_vec, p_vec, m_vec, v_vec, axis_name, group_size):
    own = COLORS * PARTS
    piece = p.shape[0]
    n_vec = p_vec.shape[0]
    rows = piece // (own * 128)
    dma = pltpu.SemaphoreType.DMA
    any_spec = pl.BlockSpec(memory_space=pl.ANY)
    vmem_spec = pl.BlockSpec(memory_space=pltpu.VMEM)
    grad, p, m, v = (a.reshape(own, rows, 128) for a in (grad, p, m, v))
    p_vec, m_vec, v_vec = (a.reshape(1, n_vec) for a in (p_vec, m_vec, v_vec))
    full, new_m, new_v, new_p = pl.pallas_call(
        functools.partial(gather_kernel, axis_name),
        out_shape=(pltpu.VMEM((group_size * own, rows, 128), jnp.bfloat16),
                   pltpu.VMEM((own, rows, 128), jnp.float32),
                   pltpu.VMEM((own, rows, 128), jnp.float32),
                   pltpu.VMEM((KEEP, rows, 128), jnp.float32)),
        in_specs=[any_spec] * 5,
        out_specs=[vmem_spec] * 4,
        scratch_shapes=[
            pltpu.VMEM((2, rows // 2, 128), jnp.float32), pltpu.VMEM((2, rows // 2, 128), jnp.float32),
            pltpu.VMEM((2, 128), jnp.float32), dma, dma((2,)),
            dma, dma((3 * PLACES,)), dma, dma],
        compiler_params=pltpu.CompilerParams(
            collective_id=1, has_side_effects=True, vmem_limit_bytes=SMALL_VMEM),
        name="gather_update",
    )(grad, p, m, v, scales)
    flat = jax.ShapeDtypeStruct((own, rows, 128), jnp.float32)
    line = jax.ShapeDtypeStruct((1, n_vec), jnp.float32)
    full, new_p, new_m, new_v, *vecs = pl.pallas_call(
        write_kernel,
        out_shape=(jax.ShapeDtypeStruct(full.shape, full.dtype), flat, flat, flat, line, line, line),
        in_specs=[vmem_spec] * 4 + [any_spec] * 6,
        out_specs=[any_spec] * 7,
        scratch_shapes=[
            pltpu.VMEM((RING, rows // 2, 128), jnp.float32), pltpu.VMEM((4, 1, n_vec), jnp.float32),
            pltpu.VMEM((2, 128), jnp.float32),
            dma((RING,)), dma((RING,)), dma((4, AHEAD)), dma((4,)), dma((3,)), dma],
        compiler_params=pltpu.CompilerParams(vmem_limit_bytes=SMALL_VMEM),
        name="write_out",
    )(*(pltpu.with_memory_space_constraint(a, pltpu.VMEM) for a in (full, new_m, new_v, new_p)),
      p, scales, grad_vec, p_vec, m_vec, v_vec)
    return (*(a.reshape(piece) for a in (new_p, new_m, new_v)), *(a.reshape(n_vec) for a in vecs),
            full.reshape(group_size * piece))


def solution(mesh):
    axis_name = mesh.axis_names[0]
    group_size = mesh.shape[axis_name]

    def local_step(g_mat, g_vec, p_mat, m_mat, v_mat, p_vec, m_vec, v_vec, learn_rate):
        grad_mat, grad_vec, scales = scatter_sum(g_mat, g_vec, learn_rate, axis_name, group_size)
        return gather_update(grad_mat, p_mat, m_mat, v_mat, scales, grad_vec, p_vec, m_vec, v_vec, axis_name, group_size)

    return jax.shard_map(
        local_step,
        mesh=mesh,
        in_specs=(P(axis_name, None), P(axis_name, None), P(axis_name), P(axis_name), P(axis_name), P(), P(), P(), P()),
        out_specs=(P(axis_name), P(axis_name), P(axis_name), P(), P(), P(), P()),
        check_vma=False,
    )
```

```python
import functools

import jax
import jax.numpy as jnp
from jax import lax
from jax.experimental import pallas as pl
from jax.experimental.pallas import tpu as pltpu
from jax.sharding import PartitionSpec as P

STEP = 10
ADAM_BETA1 = 0.9
ADAM_BETA2 = 0.98
ADAM_EPS = 1e-8
WEIGHT_DECAY = 0.01
MAX_NORM = 1.0
NORM_EPS = 1e-6
BIAS_ONE = 1.0 - ADAM_BETA1 ** STEP
BIAS_TWO = 1.0 - ADAM_BETA2 ** STEP

MESH_ID = pl.DeviceIdType.MESH
COLORS = 3
PARTS = 4
STRIDES = (2, 4, 8)
STEPS = 8 * PARTS
DEVICES = 16
WIDTH = 4096
ROWS = 64
SMALL_VMEM = 2048 * 1024
RING = 3
KEEP = 3
AHEAD = 2
SWAPS = 8
PLACES = 20
CUTS = 4
MEAN_SCALE = 1.0 / 16.0


def scatter_kernel(axis_name, piece, g, gv, lr, out, pg, vec_out, scale_out,
                   a_buf, b_buf, e_buf, stage, r1, r2, r3, v_in, v_full, v_acc, v_get, v_mean, n_put, n_get, squares, lr_smem, scale_buf,
                   a_sem, b_sem, e_sem, ds_sem, dr_sem, dc_sem, s1_sem, r1_sem, s2_sem, r2_sem, s3_sem, r3_sem, rc_sem, o_sem,
                   vi_sem, vs_sem, vr_sem, ns_sem, nr_sem, vo_sem, lr_sem, so_sem):
    chunk = piece // (COLORS * PARTS)
    width = min(chunk // CUTS, WIDTH)
    part = chunk // CUTS
    n_vec = gv.shape[1]
    n_half = n_vec // 2
    me = lax.axis_index(axis_name)
    core = lax.rem(me, 2)
    core_step = 1 - 2 * core
    deltas = [s * (1 - 2 * lax.rem(me // s, 2)) for s in STRIDES]
    partner = me + core_step
    peers = [me + d for d in deltas]

    barrier = pltpu.get_barrier_semaphore()
    for dev in (partner, *peers):
        pl.semaphore_signal(barrier, inc=1, device_id=(dev,), device_id_type=MESH_ID)

    def offset(color, t):
        unit = t // PARTS
        f1 = 1 - unit // 4
        f2 = 1 - lax.rem(unit // 2, 2)
        f3 = 1 - lax.rem(unit, 2)
        d1, d2, d3 = (deltas[(color + k) % 3] for k in range(3))
        owner = me + f1 * d1 + f2 * d2 + f3 * d3
        return owner * piece + (color * PARTS + lax.rem(t, PARTS)) * chunk

    def cut(ref, start):
        return ref.at[:, pl.ds(pl.multiple_of(start, 1024), chunk)]

    def swap(color, t):
        return pltpu.make_async_remote_copy(
            src_ref=cut(g, offset(color, t) + core_step * piece),
            dst_ref=cut(pg, (color * STEPS + t) * chunk),
            send_sem=ds_sem, recv_sem=dr_sem.at[color * SWAPS + lax.rem(t, SWAPS)],
            device_id=(partner,), device_id_type=MESH_ID)

    def swap_early(color, t):
        k = color * 2 + t
        return pltpu.make_async_remote_copy(
            src_ref=cut(g, offset(color, t) + core_step * piece), dst_ref=b_buf.at[k],
            send_sem=ds_sem, recv_sem=dr_sem.at[color * SWAPS + t],
            device_id=(partner,), device_id_type=MESH_ID)

    def swap_cut(color, i):
        s = pl.ds(i * part, part)
        return pltpu.make_async_remote_copy(
            src_ref=e_buf.at[color, :, s], dst_ref=b_buf.at[color * 2, :, s],
            send_sem=ds_sem, recv_sem=dc_sem.at[color * CUTS + i],
            device_id=(partner,), device_id_type=MESH_ID)

    def load_e(color):
        return pltpu.make_async_copy(
            cut(g, offset(color, 0) + core_step * piece), e_buf.at[color], e_sem.at[color])

    def push_cut(color, i):
        k, j = color * 3, color * 4 * PARTS
        s = pl.ds(i * part, part)
        return push(stage.at[k, :, s], r1.at[j, :, s], s1_sem.at[k], r1_sem.at[color * 4], color)

    def load_a(color, t):
        k = color * 2 + lax.rem(t, 2)
        return pltpu.make_async_copy(cut(g, offset(color, t)), a_buf.at[k], a_sem.at[k])

    def load_b(color, t):
        k = color * 2 + lax.rem(t, 2)
        return pltpu.make_async_copy(cut(pg, (color * STEPS + t) * chunk), b_buf.at[k], b_sem.at[k])

    def push(src, dst, send_sem, recv_sem, axis):
        return pltpu.make_async_remote_copy(
            src_ref=src, dst_ref=dst, send_sem=send_sem, recv_sem=recv_sem,
            device_id=(peers[axis],), device_id_type=MESH_ID)

    def push1(color, t):
        k = color * 3 + lax.rem(t, 3)
        j = color * 4 * PARTS + t
        return push(stage.at[k], r1.at[j], s1_sem.at[k], r1_sem.at[color * 4 + t // PARTS], color)

    def push2(color, t):
        j = color * 2 * PARTS + t - 4 * PARTS
        return push(r1.at[color * 4 * PARTS + t - 4 * PARTS], r2.at[j], s2_sem,
                    r2_sem.at[color * 2 + t // PARTS - 4], (color + 1) % 3)

    def push3(color, t):
        j = color * PARTS + t - 6 * PARTS
        return push(r1.at[color * 4 * PARTS + t - 4 * PARTS], r3.at[j], s3_sem, r3_sem.at[j], (color + 2) % 3)

    def push3_cut(color, i):
        s = pl.ds(i * part, part)
        return push(r1.at[color * 4 * PARTS + 3 * PARTS - 1, :, s], r3.at[color * PARTS + PARTS - 1, :, s],
                    s3_sem, rc_sem.at[color * CUTS + i], (color + 2) % 3)

    def unit1(color, u):
        span = r1.at[pl.ds((color * 4 + u) * PARTS, PARTS)]
        return push(span, span, s2_sem, r1_sem.at[color * 4 + u], color)

    def unit2(color, w):
        span = r2.at[pl.ds((color * 2 + w) * PARTS, PARTS)]
        return push(span, span, s2_sem, r2_sem.at[color * 2 + w], (color + 1) % 3)

    def store(color, t):
        j = color * PARTS + t - 7 * PARTS
        return pltpu.make_async_copy(r3.at[j], cut(out, j * chunk), o_sem)

    def add_up(color, t, dst, extra, last=False, span=None):
        k = color * 2 + lax.rem(t, 2)
        first, count = span or (0, chunk)

        @pl.loop(first // width, (first + count) // width)
        def _(i):
            s = pl.ds(pl.multiple_of(i * width, width), width)
            acc = a_buf[k, :, s].astype(jnp.float32) + b_buf[k, :, s].astype(jnp.float32)
            for ref, j in extra:
                acc = acc + ref[j, :, s]
            if last:
                acc = acc * MEAN_SCALE
                squares[...] += acc * acc
            dst[0][dst[1], :, s] = acc

    def half(ref, which):
        return ref.at[:, pl.ds(pl.multiple_of(which * n_half, 1024), n_half)]

    def vec_push(k):
        src = half(v_full, 1 - core) if k == 0 else half(v_mean, core) if k == 4 else v_acc.at[k]
        return pltpu.make_async_remote_copy(
            src_ref=src, dst_ref=half(v_mean, core) if k == 4 else v_get.at[k],
            send_sem=vs_sem, recv_sem=vr_sem.at[k],
            device_id=((partner, *peers, partner)[k],), device_id_type=MESH_ID)

    def norm_push(k):
        return pltpu.make_async_remote_copy(
            src_ref=n_put, dst_ref=n_get.at[me], send_sem=ns_sem, recv_sem=nr_sem,
            device_id=(lax.rem(me + k, DEVICES),), device_id_type=MESH_ID)

    def vec_loop(count, body):
        @pl.loop(0, count // 1024)
        def _(i):
            body(pl.multiple_of(i * 1024, 1024))

    def vec_turn(k):
        def body(i):
            s = pl.ds(i, 1024)
            here = pl.ds(pl.multiple_of(core * n_half + i, 1024), 1024)
            total = (v_acc[k, :, s] if k else v_full[:, here]) + v_get[k, :, s]
            if k < 3:
                v_acc[k + 1, :, s] = total
            else:
                v_mean[:, here] = total * MEAN_SCALE
        vec_push(k).wait_recv()
        vec_loop(n_half, body)
        vec_push(k + 1).start()

    def ready(color, t):
        load_a(color, t).wait()
        load_b(color, t).wait()

    def refill(color, t):
        load_a(color, t).start()
        swap(color, t).wait_recv()
        load_b(color, t).start()

    def more_swap(color, t):
        swap(color, t).start()

    for color in range(COLORS):
        load_e(color).start()
    for t in range(2):
        for color in range(COLORS):
            load_a(color, t).start()
    vec_load = pltpu.make_async_copy(gv, v_in, vi_sem)
    vec_load.start()
    lr_load = pltpu.make_async_copy(lr, lr_smem, lr_sem)
    lr_load.start()
    squares[...] = jnp.zeros_like(squares)
    for color in range(COLORS):
        load_e(color).wait()
    pl.semaphore_wait(barrier, 4)
    for i in range(CUTS):
        for color in range(COLORS):
            swap_cut(color, i).start()
    for color in range(COLORS):
        swap_early(color, 1).start()
    for t in range(2, 4):
        for color in range(COLORS):
            swap(color, t).start()
    for i in range(CUTS):
        for color in range(COLORS):
            if i == 0:
                load_a(color, 0).wait()
            swap_cut(color, i).wait_recv()
            add_up(color, 0, (stage, color * 3), (), span=(i * part, part))
            push_cut(color, i).start()
    for color in range(COLORS):
        more_swap(color, 4)
        refill(color, 2)

    def phase_one(t, first, early=False):
        for color in range(COLORS):
            if early:
                load_a(color, t).wait()
                swap_early(color, t).wait_recv()
            else:
                ready(color, t)
            if not first:
                push1(color, t - 3).wait_send()
            add_up(color, t, (stage, color * 3 + lax.rem(t, 3)), ())
            push1(color, t).start()
            more_swap(color, t + 4)
            refill(color, t + 2)

    def run(lo, hi, body):
        lax.fori_loop(lo, hi, lambda t, c: (body(t), c)[1], 0)

    phase_one(1, True, True)
    phase_one(2, True)
    vec_load.wait()

    def widen(i):
        s = pl.ds(i, 1024)
        v_full[:, s] = v_in[:, s].astype(jnp.float32)

    vec_loop(n_vec, widen)
    vec_push(0).start()
    for k in range(4):
        run(3 * k + 3, 3 * k + 6, lambda t: phase_one(t, False))
        vec_turn(k)
    run(15, 4 * PARTS, lambda t: phase_one(t, False))
    vec_push(4).wait_recv()
    vec_store = pltpu.make_async_copy(v_mean, vec_out, vo_sem)
    vec_store.start()

    def phase_two(t):
        for color in range(COLORS):
            ready(color, t)
            j = color * 4 * PARTS + t - 4 * PARTS
            add_up(color, t, (r1, j), ((r1, j),))
            push2(color, t).start()
            more_swap(color, t + 4)
            refill(color, t + 2)

    def phase_three(t, cuts):
        for color in range(COLORS):
            ready(color, t)
            j = color * 4 * PARTS + t - 4 * PARTS
            add_up(color, t, (r1, j), ((r1, j), (r2, color * 2 * PARTS + t - 6 * PARTS)))
            if cuts:
                for i in range(CUTS):
                    push3_cut(color, i).start()
            else:
                push3(color, t).start()
            more_swap(color, t + 4)
            refill(color, t + 2)

    def finish(color, t, span=None):
        j = color * PARTS + t - 7 * PARTS
        add_up(color, t, (r3, j), (
            (r1, color * 4 * PARTS + t - 4 * PARTS),
            (r2, color * 2 * PARTS + t - 6 * PARTS),
            (r3, j)), last=True, span=span)

    def phase_four(t, fill):
        for color in range(COLORS):
            ready(color, t)
            push3(color, t - PARTS).wait_recv()
            finish(color, t)
            store(color, t).start()
            if fill:
                refill(color, t + 2)

    for unit in range(4, 8):
        for color in range(COLORS):
            unit1(color, unit - 4).wait_recv()
            if unit >= 6:
                unit2(color, unit - 6).wait_recv()
        lo = unit * PARTS
        if unit < 6:
            run(lo, lo + PARTS, phase_two)
        elif unit == 6:
            run(lo, lo + PARTS - 1, lambda t: phase_three(t, False))
            phase_three(lo + PARTS - 1, True)
        else:
            run(lo, lo + PARTS - 2, lambda t: phase_four(t, True))
            phase_four(lo + PARTS - 2, False)
    for color in range(COLORS):
        ready(color, STEPS - 1)
    for i in range(CUTS):
        for color in range(COLORS):
            push3_cut(color, i).wait_recv()
            finish(color, STEPS - 1, span=(i * part, part))
    for color in range(COLORS):
        store(color, STEPS - 1).start()

    vec_sq = jnp.sum(v_mean[...] * v_mean[...], axis=1, keepdims=True)
    mine = jnp.broadcast_to(jnp.sum(squares[...], axis=1, keepdims=True), (1, 128))
    n_put[...] = mine
    n_get[me] = mine
    for k in range(1, DEVICES):
        norm_push(k).start()
    rest = pltpu.make_async_remote_copy(
        src_ref=n_get.at[pl.ds(0, DEVICES - 1)], dst_ref=n_get.at[pl.ds(0, DEVICES - 1)],
        send_sem=ns_sem, recv_sem=nr_sem, device_id=(partner,), device_id_type=MESH_ID)
    rest.wait_recv()
    norm_sq = n_get[0]
    for k in range(1, DEVICES):
        norm_sq = norm_sq + n_get[k]
    norm_sq = norm_sq + vec_sq
    scale_buf[0:1, :] = jnp.minimum(1.0, MAX_NORM / (jnp.sqrt(norm_sq) + NORM_EPS))
    lr_load.wait()
    scale_buf[1:2, :] = jnp.full((1, 128), lr_smem[0])
    scale_store = pltpu.make_async_copy(scale_buf, scale_out, so_sem)
    scale_store.start()

    def drain(lo, hi, wait):
        def body(t):
            for color in range(COLORS):
                wait(color, t)
        run(lo, hi, body)

    drain(4 * PARTS - 3, 4 * PARTS, lambda c, t: push1(c, t).wait_send())
    push(r2, r2, s2_sem, r2_sem.at[0], 0).wait_send()
    push(r3, r3, s3_sem, r3_sem.at[0], 0).wait_send()
    pltpu.make_async_remote_copy(
        src_ref=pg, dst_ref=pg, send_sem=ds_sem, recv_sem=dr_sem.at[0],
        device_id=(partner,), device_id_type=MESH_ID).wait_send()
    pltpu.make_async_copy(out, out, o_sem).wait()
    push(v_get, v_get, vs_sem, vr_sem.at[0], 0).wait_send()
    rest.wait_send()
    vec_store.wait()
    scale_store.wait()


def scatter_sum(g_mat, g_vec, learn_rate, axis_name, group_size):
    total = g_mat.shape[1]
    n_vec = g_vec.shape[1]
    piece = total // group_size
    chunk = piece // (COLORS * PARTS)
    dma = pltpu.SemaphoreType.DMA
    any_spec = pl.BlockSpec(memory_space=pl.ANY)
    out, _, vec, scales = pl.pallas_call(
        functools.partial(scatter_kernel, axis_name, piece),
        out_shape=(jax.ShapeDtypeStruct((1, piece), jnp.float32),
                   jax.ShapeDtypeStruct((1, total // 2), jnp.bfloat16),
                   jax.ShapeDtypeStruct((1, n_vec), jnp.float32),
                   jax.ShapeDtypeStruct((2, 128), jnp.float32)),
        in_specs=[any_spec] * 3,
        out_specs=[any_spec] * 4,
        scratch_shapes=[
            pltpu.VMEM((2 * COLORS, 1, chunk), jnp.bfloat16),
            pltpu.VMEM((2 * COLORS, 1, chunk), jnp.bfloat16),
            pltpu.VMEM((COLORS, 1, chunk), jnp.bfloat16),
            pltpu.VMEM((3 * COLORS, 1, chunk), jnp.float32),
            pltpu.VMEM((4 * PARTS * COLORS, 1, chunk), jnp.float32),
            pltpu.VMEM((2 * PARTS * COLORS, 1, chunk), jnp.float32),
            pltpu.VMEM((PARTS * COLORS, 1, chunk), jnp.float32),
            pltpu.VMEM((1, n_vec), jnp.bfloat16),
            pltpu.VMEM((1, n_vec), jnp.float32),
            pltpu.VMEM((4, 1, n_vec // 2), jnp.float32),
            pltpu.VMEM((5, 1, n_vec // 2), jnp.float32),
            pltpu.VMEM((1, n_vec), jnp.float32),
            pltpu.VMEM((1, 128), jnp.float32),
            pltpu.VMEM((DEVICES, 1, 128), jnp.float32),
            pltpu.VMEM((1, min(chunk // CUTS, WIDTH)), jnp.float32),
            pltpu.SMEM((1,), jnp.float32),
            pltpu.VMEM((2, 128), jnp.float32),
            dma((2 * COLORS,)), dma((2 * COLORS,)), dma((COLORS,)),
            dma, dma((SWAPS * COLORS,)), dma((CUTS * COLORS,)),
            dma((3 * COLORS,)), dma((4 * COLORS,)), dma, dma((2 * COLORS,)),
            dma, dma((PARTS * COLORS,)), dma((CUTS * COLORS,)), dma,
            dma, dma, dma((5,)), dma, dma, dma, dma, dma,
        ],
        compiler_params=pltpu.CompilerParams(
            collective_id=0, has_side_effects=True, vmem_limit_bytes=63 * 1024 * 1024),
        name="scatter_sum",
    )(g_mat, g_vec, learn_rate.reshape(1))
    return out, vec, scales


def adam_moments(grad, m, v):
    new_m = ADAM_BETA1 * m + (1.0 - ADAM_BETA1) * grad
    new_v = ADAM_BETA2 * v + (1.0 - ADAM_BETA2) * grad * grad
    return new_m, new_v


def adam_param(p, m, v, rate, decay):
    direction = (m / BIAS_ONE) / (jnp.sqrt(v / BIAS_TWO) + ADAM_EPS)
    return p - rate * (direction + decay * p)


def gather_kernel(axis_name, grad, p, m, v, scales_in, out, m_out, v_out, p_out, g_buf, p_buf, scales,
                  scales_sem, load_sem, s_sem, r_sem, ds_sem, dr_sem):
    own = COLORS * PARTS
    rows = p.shape[1]
    tile = rows // 2
    step = min(tile // 2, ROWS)
    me = lax.axis_index(axis_name)
    deltas = [s * (1 - 2 * lax.rem(me // s, 2)) for s in STRIDES]
    partner = me + 1 - 2 * lax.rem(me, 2)
    peers = [me + d for d in deltas]

    barrier = pltpu.get_barrier_semaphore()
    for dev in (partner, *peers):
        pl.semaphore_signal(barrier, inc=1, device_id=(dev,), device_id_type=MESH_ID)

    def fetch(n):
        q, color, h = n // (2 * COLORS), n // 2 % COLORS, n % 2
        i = color * PARTS + q
        s = pl.ds(h * tile, tile)
        p_dst = p_out.at[i, s] if i < KEEP else p_buf.at[h]
        for src, dst in ((grad, g_buf.at[h]), (m, m_out.at[i, s]), (v, v_out.at[i, s]), (p, p_dst)):
            pltpu.make_async_copy(src.at[i, s], dst, load_sem.at[h]).start()

    def arrived(n):
        pltpu.make_async_copy(m.at[pl.ds(0, 2)], m_out.at[pl.ds(0, 2)], load_sem.at[n % 2]).wait()

    def across(index):
        return pltpu.make_async_remote_copy(
            src_ref=out.at[index], dst_ref=out.at[index], send_sem=ds_sem, recv_sem=dr_sem,
            device_id=(partner,), device_id_type=MESH_ID)

    def route(stage, axis):
        b1, b2 = (axis - 2) % 3, (axis - 1) % 3
        color = (axis, b2, b2, b1, b1, b1, b1)[stage]
        flips = ((), (), (b2,), (), (b1,), (b2,), (b1, b2))[stage]
        return color, sum((deltas[f] for f in flips), me)

    def push(stage, axis, q, span=None):
        color, owner = route(stage, axis)
        index = owner * own + color * PARTS + q
        place = (3 * q, 3 * q + 1, 3 * PARTS + q, 3 * q + 2)[stage] if stage < 4 else stage * PARTS + q
        ref = out.at[index] if span is None else out.at[index, span]
        return pltpu.make_async_remote_copy(
            src_ref=ref, dst_ref=ref, send_sem=s_sem, recv_sem=r_sem.at[axis * PLACES + lax.rem(place, PLACES)],
            device_id=(peers[axis],), device_id_type=MESH_ID)

    def land(stage, axis, q):
        color, owner = route(stage, axis)
        push(stage, axis, q).wait_recv()
        across((owner + deltas[axis]) * own + color * PARTS + q).start()

    def update(color, q, h, first, count):
        i = color * PARTS + q

        @pl.loop(first // step, (first + count) // step)
        def _(r):
            t = pl.ds(pl.multiple_of(r * step, step), step)
            s = pl.ds(pl.multiple_of(h * tile + r * step, step), step)
            new_m, new_v = adam_moments(g_buf[h, t, :] * scales[0:1, :], m_out[i, s, :], v_out[i, s, :])
            m_out[i, s, :] = new_m
            v_out[i, s, :] = new_v
            old_p = p_out[i, s, :] if i < KEEP else p_buf[h, t, :]
            new_p = adam_param(old_p, new_m, new_v, scales[1:2, :], WEIGHT_DECAY)
            if i < KEEP:
                p_out[i, s, :] = new_p
            out[me * own + i, s, :] = new_p.astype(jnp.bfloat16)

    def each(count, body):
        lax.fori_loop(0, count, lambda i, c: (body(i), c)[1], 0)

    scales_load = pltpu.make_async_copy(scales_in, scales, scales_sem)
    scales_load.start()
    fetch(0)
    scales_load.wait()
    fetch(1)
    for n in range(2 * own):
        q, color, h = n // (2 * COLORS), n // 2 % COLORS, n % 2
        cuts = 2 if n < 2 else 1
        arrived(n)
        for c in range(cuts):
            count = tile // cuts
            update(color, q, h, c * count, count)
            if n == 0 and c == 0:
                pl.semaphore_wait(barrier, 4)
            for k, stage in enumerate((0, 1, 3)):
                push(stage, (color + k) % 3, q, pl.ds(h * tile + c * count, count)).start()
        if h:
            across(me * own + color * PARTS + q).start()
        if n + 2 < 2 * own:
            fetch(n + 2)

    def own_stage(q):
        for axis in range(3):
            for stage in (0, 1, 3):
                land(stage, axis, q)
            push(2, (axis + 1) % 3, q).start()

    each(PARTS, own_stage)
    for stage, last in ((4, 2), (5, 4), (6, 5), (None, 6)):
        def body(q, stage=stage, last=last):
            for axis in range(3):
                if stage:
                    push(stage, axis, q).start()
                land(last, axis, q)
        each(PARTS, body)

    sent = out.at[pl.ds(0, 7 * own)]
    pltpu.make_async_remote_copy(
        src_ref=sent, dst_ref=sent, send_sem=s_sem, recv_sem=r_sem.at[0],
        device_id=(partner,), device_id_type=MESH_ID).wait_send()
    half = pltpu.make_async_remote_copy(
        src_ref=out.at[pl.ds(0, 8 * own)], dst_ref=out.at[pl.ds(0, 8 * own)], send_sem=ds_sem, recv_sem=dr_sem,
        device_id=(partner,), device_id_type=MESH_ID)
    half.wait_recv()
    half.wait_send()


def write_kernel(held, m_held, v_held, p_held, p, scales_in, g_vec, p_vec, m_vec, v_vec,
                 out, p_out, m_out, v_out, pv_out, mv_out, vv_out,
                 p_buf, vec_buf, scales, in_sem, out_sem, sem, vec_sem, vec_out_sem, scales_sem):
    own, rows, _ = p.shape
    step = min(rows, ROWS)
    span = held.shape[0] // own

    tiles = own - KEEP

    def load(n):
        return pltpu.make_async_copy(p.at[KEEP + n], p_buf.at[n % RING], in_sem.at[n % RING])

    def store(n):
        return pltpu.make_async_copy(p_buf.at[n % RING], p_out.at[KEEP + n], out_sem.at[n % RING])

    def copies(i):
        part = pl.ds(i * span, span)
        pairs = [(held.at[part], out.at[part]), (m_held.at[i], m_out.at[i]), (v_held.at[i], v_out.at[i])]
        if i < KEEP:
            pairs.append((p_held.at[i], p_out.at[i]))
        return [pltpu.make_async_copy(src, dst, sem.at[k, i % AHEAD]) for k, (src, dst) in enumerate(pairs)]

    scales_load = pltpu.make_async_copy(scales_in, scales, scales_sem)
    scales_load.start()
    vec_loads = [pltpu.make_async_copy(a, vec_buf.at[k], vec_sem.at[k])
                 for k, a in enumerate((p_vec, m_vec, v_vec, g_vec))]
    vec_stores = [pltpu.make_async_copy(vec_buf.at[k], a, vec_out_sem.at[k])
                  for k, a in enumerate((pv_out, mv_out, vv_out))]
    def vec_update():
        for copy in vec_loads:
            copy.wait()

        @pl.loop(0, g_vec.shape[1] // 1024)
        def _(i):
            s = pl.ds(pl.multiple_of(i * 1024, 1024), 1024)
            new_m, new_v = adam_moments(vec_buf[3, :, s] * scales[0:1, 0:1], vec_buf[1, :, s], vec_buf[2, :, s])
            vec_buf[1, :, s] = new_m
            vec_buf[2, :, s] = new_v
            vec_buf[0, :, s] = adam_param(vec_buf[0, :, s], new_m, new_v, scales[1:2, 0:1], 0.0)

        for copy in vec_stores:
            copy.start()

    for n in range(RING - 1):
        load(n).start()
    for copy in vec_loads:
        copy.start()
    for i in range(AHEAD):
        for copy in copies(i):
            copy.start()
    scales_load.wait()
    for n in range(tiles):
        load(n).wait()
        i = KEEP + n

        @pl.loop(0, rows // step)
        def _(r):
            s = pl.ds(pl.multiple_of(r * step, step), step)
            p_buf[n % RING, s, :] = adam_param(
                p_buf[n % RING, s, :], m_held[i, s, :], v_held[i, s, :], scales[1:2, :], WEIGHT_DECAY)

        store(n).start()
        if n + RING - 1 < tiles:
            if n:
                store(n - 1).wait()
            load(n + RING - 1).start()
        for j in range(n * (own - AHEAD) // tiles, (n + 1) * (own - AHEAD) // tiles):
            for copy in copies(j):
                copy.wait()
            for copy in copies(j + AHEAD):
                copy.start()
        if n == 0:
            vec_update()
    for n in range(tiles - RING, tiles):
        store(n).wait()
    for i in range(own - AHEAD, own):
        for copy in copies(i):
            copy.wait()
    for copy in vec_stores:
        copy.wait()


def gather_update(grad, p, m, v, scales, grad_vec, p_vec, m_vec, v_vec, axis_name, group_size):
    own = COLORS * PARTS
    piece = p.shape[0]
    n_vec = p_vec.shape[0]
    rows = piece // (own * 128)
    dma = pltpu.SemaphoreType.DMA
    any_spec = pl.BlockSpec(memory_space=pl.ANY)
    vmem_spec = pl.BlockSpec(memory_space=pltpu.VMEM)
    grad, p, m, v = (a.reshape(own, rows, 128) for a in (grad, p, m, v))
    p_vec, m_vec, v_vec = (a.reshape(1, n_vec) for a in (p_vec, m_vec, v_vec))
    full, new_m, new_v, new_p = pl.pallas_call(
        functools.partial(gather_kernel, axis_name),
        out_shape=(pltpu.VMEM((group_size * own, rows, 128), jnp.bfloat16),
                   pltpu.VMEM((own, rows, 128), jnp.float32),
                   pltpu.VMEM((own, rows, 128), jnp.float32),
                   pltpu.VMEM((KEEP, rows, 128), jnp.float32)),
        in_specs=[any_spec] * 5,
        out_specs=[vmem_spec] * 4,
        scratch_shapes=[
            pltpu.VMEM((2, rows // 2, 128), jnp.float32), pltpu.VMEM((2, rows // 2, 128), jnp.float32),
            pltpu.VMEM((2, 128), jnp.float32), dma, dma((2,)),
            dma, dma((3 * PLACES,)), dma, dma],
        compiler_params=pltpu.CompilerParams(
            collective_id=1, has_side_effects=True, vmem_limit_bytes=SMALL_VMEM),
        name="gather_update",
    )(grad, p, m, v, scales)
    flat = jax.ShapeDtypeStruct((own, rows, 128), jnp.float32)
    line = jax.ShapeDtypeStruct((1, n_vec), jnp.float32)
    full, new_p, new_m, new_v, *vecs = pl.pallas_call(
        write_kernel,
        out_shape=(jax.ShapeDtypeStruct(full.shape, full.dtype), flat, flat, flat, line, line, line),
        in_specs=[vmem_spec] * 4 + [any_spec] * 6,
        out_specs=[any_spec] * 7,
        scratch_shapes=[
            pltpu.VMEM((RING, rows, 128), jnp.float32), pltpu.VMEM((4, 1, n_vec), jnp.float32),
            pltpu.VMEM((2, 128), jnp.float32),
            dma((RING,)), dma((RING,)), dma((4, AHEAD)), dma((4,)), dma((3,)), dma],
        compiler_params=pltpu.CompilerParams(vmem_limit_bytes=SMALL_VMEM),
        name="write_out",
    )(*(pltpu.with_memory_space_constraint(a, pltpu.VMEM) for a in (full, new_m, new_v, new_p)),
      p, scales, grad_vec, p_vec, m_vec, v_vec)
    return (*(a.reshape(piece) for a in (new_p, new_m, new_v)), *(a.reshape(n_vec) for a in vecs),
            full.reshape(group_size * piece))


def solution(mesh):
    axis_name = mesh.axis_names[0]
    group_size = mesh.shape[axis_name]

    def local_step(g_mat, g_vec, p_mat, m_mat, v_mat, p_vec, m_vec, v_vec, learn_rate):
        grad_mat, grad_vec, scales = scatter_sum(g_mat, g_vec, learn_rate, axis_name, group_size)
        return gather_update(grad_mat, p_mat, m_mat, v_mat, scales, grad_vec, p_vec, m_vec, v_vec, axis_name, group_size)

    return jax.shard_map(
        local_step,
        mesh=mesh,
        in_specs=(P(axis_name, None), P(axis_name, None), P(axis_name), P(axis_name), P(axis_name), P(), P(), P(), P()),
        out_specs=(P(axis_name), P(axis_name), P(axis_name), P(), P(), P(), P()),
        check_vma=False,
    )
```

```python
import functools

import jax
import jax.numpy as jnp
from jax import lax
from jax.experimental import pallas as pl
from jax.experimental.pallas import tpu as pltpu
from jax.sharding import PartitionSpec as P

STEP = 10
ADAM_BETA1 = 0.9
ADAM_BETA2 = 0.98
ADAM_EPS = 1e-8
WEIGHT_DECAY = 0.01
MAX_NORM = 1.0
NORM_EPS = 1e-6
BIAS_ONE = 1.0 - ADAM_BETA1 ** STEP
BIAS_TWO = 1.0 - ADAM_BETA2 ** STEP

MESH_ID = pl.DeviceIdType.MESH
COLORS = 3
PARTS = 4
STRIDES = (2, 4, 8)
STEPS = 8 * PARTS
DEVICES = 16
WIDTH = 4096
ROWS = 64
SMALL_VMEM = 2048 * 1024
RING = 3
KEEP = 3
AHEAD = 3
SWAPS = 8
PLACES = 20
CUTS = 4
MEAN_SCALE = 1.0 / 16.0


def scatter_kernel(axis_name, piece, g, gv, lr, out, pg, vec_out, scale_out,
                   a_buf, b_buf, e_buf, stage, r1, r2, r3, v_in, v_full, v_acc, v_get, v_mean, n_put, n_get, squares, lr_smem, scale_buf,
                   a_sem, b_sem, e_sem, ds_sem, dr_sem, dc_sem, s1_sem, r1_sem, s2_sem, r2_sem, s3_sem, r3_sem, rc_sem, o_sem,
                   vi_sem, vs_sem, vr_sem, ns_sem, nr_sem, vo_sem, lr_sem, so_sem):
    chunk = piece // (COLORS * PARTS)
    width = min(chunk // CUTS, WIDTH)
    part = chunk // CUTS
    n_vec = gv.shape[1]
    n_half = n_vec // 2
    me = lax.axis_index(axis_name)
    core = lax.rem(me, 2)
    core_step = 1 - 2 * core
    deltas = [s * (1 - 2 * lax.rem(me // s, 2)) for s in STRIDES]
    partner = me + core_step
    peers = [me + d for d in deltas]

    barrier = pltpu.get_barrier_semaphore()
    for dev in (partner, *peers):
        pl.semaphore_signal(barrier, inc=1, device_id=(dev,), device_id_type=MESH_ID)

    def offset(color, t):
        unit = t // PARTS
        f1 = 1 - unit // 4
        f2 = 1 - lax.rem(unit // 2, 2)
        f3 = 1 - lax.rem(unit, 2)
        d1, d2, d3 = (deltas[(color + k) % 3] for k in range(3))
        owner = me + f1 * d1 + f2 * d2 + f3 * d3
        return owner * piece + (color * PARTS + lax.rem(t, PARTS)) * chunk

    def cut(ref, start):
        return ref.at[:, pl.ds(pl.multiple_of(start, 1024), chunk)]

    def swap(color, t):
        return pltpu.make_async_remote_copy(
            src_ref=cut(g, offset(color, t) + core_step * piece),
            dst_ref=cut(pg, (color * STEPS + t) * chunk),
            send_sem=ds_sem, recv_sem=dr_sem.at[color * SWAPS + lax.rem(t, SWAPS)],
            device_id=(partner,), device_id_type=MESH_ID)

    def swap_early(color, t):
        k = color * 2 + t
        return pltpu.make_async_remote_copy(
            src_ref=cut(g, offset(color, t) + core_step * piece), dst_ref=b_buf.at[k],
            send_sem=ds_sem, recv_sem=dr_sem.at[color * SWAPS + t],
            device_id=(partner,), device_id_type=MESH_ID)

    def swap_cut(color, i):
        s = pl.ds(i * part, part)
        return pltpu.make_async_remote_copy(
            src_ref=e_buf.at[color, :, s], dst_ref=b_buf.at[color * 2, :, s],
            send_sem=ds_sem, recv_sem=dc_sem.at[color * CUTS + i],
            device_id=(partner,), device_id_type=MESH_ID)

    def load_e(color):
        return pltpu.make_async_copy(
            cut(g, offset(color, 0) + core_step * piece), e_buf.at[color], e_sem.at[color])

    def push_cut(color, i):
        k, j = color * 3, color * 4 * PARTS
        s = pl.ds(i * part, part)
        return push(stage.at[k, :, s], r1.at[j, :, s], s1_sem.at[k], r1_sem.at[color * 2], color)

    def load_a(color, t):
        k = color * 2 + lax.rem(t, 2)
        return pltpu.make_async_copy(cut(g, offset(color, t)), a_buf.at[k], a_sem.at[k])

    def load_b(color, t):
        k = color * 2 + lax.rem(t, 2)
        return pltpu.make_async_copy(cut(pg, (color * STEPS + t) * chunk), b_buf.at[k], b_sem.at[k])

    def push(src, dst, send_sem, recv_sem, axis):
        return pltpu.make_async_remote_copy(
            src_ref=src, dst_ref=dst, send_sem=send_sem, recv_sem=recv_sem,
            device_id=(peers[axis],), device_id_type=MESH_ID)

    def push1(color, t):
        k = color * 3 + lax.rem(t, 3)
        j = color * 4 * PARTS + t
        return push(stage.at[k], r1.at[j], s1_sem.at[k], r1_sem.at[color * 2 + t // (2 * PARTS)], color)

    def push2(color, t):
        j = color * 2 * PARTS + t - 4 * PARTS
        return push(r1.at[color * 4 * PARTS + t - 4 * PARTS], r2.at[j], s2_sem,
                    r2_sem.at[color * 2 + t // PARTS - 4], (color + 1) % 3)

    def push3(color, t):
        j = color * PARTS + t - 6 * PARTS
        return push(r1.at[color * 4 * PARTS + t - 4 * PARTS], r3.at[j], s3_sem, r3_sem.at[j], (color + 2) % 3)

    def push3_cut(color, i):
        s = pl.ds(i * part, part)
        return push(r1.at[color * 4 * PARTS + 3 * PARTS - 1, :, s], r3.at[color * PARTS + PARTS - 1, :, s],
                    s3_sem, rc_sem.at[color * CUTS + i], (color + 2) % 3)

    def unit1(color, pair):
        span = r1.at[pl.ds((color * 2 + pair) * 2 * PARTS, 2 * PARTS)]
        return push(span, span, s2_sem, r1_sem.at[color * 2 + pair], color)

    def unit2(color, w):
        span = r2.at[pl.ds((color * 2 + w) * PARTS, PARTS)]
        return push(span, span, s2_sem, r2_sem.at[color * 2 + w], (color + 1) % 3)

    def store(color, t):
        j = color * PARTS + t - 7 * PARTS
        return pltpu.make_async_copy(r3.at[j], cut(out, j * chunk), o_sem)

    def add_up(color, t, dst, extra, last=False, span=None):
        k = color * 2 + lax.rem(t, 2)
        first, count = span or (0, chunk)

        @pl.loop(first // width, (first + count) // width)
        def _(i):
            s = pl.ds(pl.multiple_of(i * width, width), width)
            acc = a_buf[k, :, s].astype(jnp.float32) + b_buf[k, :, s].astype(jnp.float32)
            for ref, j in extra:
                acc = acc + ref[j, :, s]
            if last:
                acc = acc * MEAN_SCALE
                squares[...] += acc * acc
            dst[0][dst[1], :, s] = acc

    def half(ref, which):
        return ref.at[:, pl.ds(pl.multiple_of(which * n_half, 1024), n_half)]

    def vec_push(k):
        src = half(v_full, 1 - core) if k == 0 else half(v_mean, core) if k == 4 else v_acc.at[k]
        return pltpu.make_async_remote_copy(
            src_ref=src, dst_ref=half(v_mean, core) if k == 4 else v_get.at[k],
            send_sem=vs_sem, recv_sem=vr_sem.at[k],
            device_id=((partner, *peers, partner)[k],), device_id_type=MESH_ID)

    def norm_push(k):
        return pltpu.make_async_remote_copy(
            src_ref=n_put, dst_ref=n_get.at[me], send_sem=ns_sem, recv_sem=nr_sem,
            device_id=(lax.rem(me + k, DEVICES),), device_id_type=MESH_ID)

    def vec_loop(count, body):
        @pl.loop(0, count // 1024)
        def _(i):
            body(pl.multiple_of(i * 1024, 1024))

    def vec_turn(k):
        def body(i):
            s = pl.ds(i, 1024)
            here = pl.ds(pl.multiple_of(core * n_half + i, 1024), 1024)
            total = (v_acc[k, :, s] if k else v_full[:, here]) + v_get[k, :, s]
            if k < 3:
                v_acc[k + 1, :, s] = total
            else:
                v_mean[:, here] = total * MEAN_SCALE
        vec_push(k).wait_recv()
        vec_loop(n_half, body)
        vec_push(k + 1).start()

    def ready(color, t):
        load_a(color, t).wait()
        load_b(color, t).wait()

    def refill(color, t):
        load_a(color, t).start()
        swap(color, t).wait_recv()
        load_b(color, t).start()

    def more_swap(color, t):
        swap(color, t).start()

    for color in range(COLORS):
        load_e(color).start()
    for t in range(2):
        for color in range(COLORS):
            load_a(color, t).start()
    vec_load = pltpu.make_async_copy(gv, v_in, vi_sem)
    vec_load.start()
    lr_load = pltpu.make_async_copy(lr, lr_smem, lr_sem)
    lr_load.start()
    squares[...] = jnp.zeros_like(squares)
    for color in range(COLORS):
        load_e(color).wait()
    pl.semaphore_wait(barrier, 4)
    for i in range(CUTS):
        for color in range(COLORS):
            swap_cut(color, i).start()
    for color in range(COLORS):
        swap_early(color, 1).start()
    for t in range(2, 4):
        for color in range(COLORS):
            swap(color, t).start()
    for i in range(CUTS):
        for color in range(COLORS):
            if i == 0:
                load_a(color, 0).wait()
            swap_cut(color, i).wait_recv()
            add_up(color, 0, (stage, color * 3), (), span=(i * part, part))
            push_cut(color, i).start()
    for color in range(COLORS):
        more_swap(color, 4)
        refill(color, 2)

    def phase_one(t, first, early=False):
        for color in range(COLORS):
            if early:
                load_a(color, t).wait()
                swap_early(color, t).wait_recv()
            else:
                ready(color, t)
            if not first:
                push1(color, t - 3).wait_send()
            add_up(color, t, (stage, color * 3 + lax.rem(t, 3)), ())
            push1(color, t).start()
            more_swap(color, t + 4)
            refill(color, t + 2)

    def run(lo, hi, body):
        lax.fori_loop(lo, hi, lambda t, c: (body(t), c)[1], 0)

    phase_one(1, True, True)
    phase_one(2, True)
    vec_load.wait()

    def widen(i):
        s = pl.ds(i, 1024)
        v_full[:, s] = v_in[:, s].astype(jnp.float32)

    vec_loop(n_vec, widen)
    vec_push(0).start()
    for k in range(4):
        run(3 * k + 3, 3 * k + 6, lambda t: phase_one(t, False))
        vec_turn(k)
    run(15, 4 * PARTS, lambda t: phase_one(t, False))
    vec_push(4).wait_recv()
    vec_store = pltpu.make_async_copy(v_mean, vec_out, vo_sem)
    vec_store.start()

    def phase_two(t):
        for color in range(COLORS):
            ready(color, t)
            j = color * 4 * PARTS + t - 4 * PARTS
            add_up(color, t, (r1, j), ((r1, j),))
            push2(color, t).start()
            more_swap(color, t + 4)
            refill(color, t + 2)

    def phase_three(t, cuts):
        for color in range(COLORS):
            ready(color, t)
            j = color * 4 * PARTS + t - 4 * PARTS
            add_up(color, t, (r1, j), ((r1, j), (r2, color * 2 * PARTS + t - 6 * PARTS)))
            if cuts:
                for i in range(CUTS):
                    push3_cut(color, i).start()
            else:
                push3(color, t).start()
            more_swap(color, t + 4)
            refill(color, t + 2)

    def finish(color, t, span=None):
        j = color * PARTS + t - 7 * PARTS
        add_up(color, t, (r3, j), (
            (r1, color * 4 * PARTS + t - 4 * PARTS),
            (r2, color * 2 * PARTS + t - 6 * PARTS),
            (r3, j)), last=True, span=span)

    def phase_four(t, fill):
        for color in range(COLORS):
            ready(color, t)
            push3(color, t - PARTS).wait_recv()
            finish(color, t)
            store(color, t).start()
            if fill:
                refill(color, t + 2)

    for unit in range(4, 8):
        for color in range(COLORS):
            if unit in (4, 6):
                unit1(color, (unit - 4) // 2).wait_recv()
            if unit >= 6:
                unit2(color, unit - 6).wait_recv()
        lo = unit * PARTS
        if unit < 6:
            run(lo, lo + PARTS, phase_two)
        elif unit == 6:
            run(lo, lo + PARTS - 1, lambda t: phase_three(t, False))
            phase_three(lo + PARTS - 1, True)
        else:
            run(lo, lo + PARTS - 2, lambda t: phase_four(t, True))
            phase_four(lo + PARTS - 2, False)
    for color in range(COLORS):
        ready(color, STEPS - 1)
    for i in range(CUTS):
        for color in range(COLORS):
            push3_cut(color, i).wait_recv()
            finish(color, STEPS - 1, span=(i * part, part))
    for color in range(COLORS):
        store(color, STEPS - 1).start()

    vec_sq = jnp.sum(v_mean[...] * v_mean[...], axis=1, keepdims=True)
    mine = jnp.broadcast_to(jnp.sum(squares[...], axis=1, keepdims=True), (1, 128))
    n_put[...] = mine
    n_get[me] = mine
    for k in range(1, DEVICES):
        norm_push(k).start()
    rest = pltpu.make_async_remote_copy(
        src_ref=n_get.at[pl.ds(0, DEVICES - 1)], dst_ref=n_get.at[pl.ds(0, DEVICES - 1)],
        send_sem=ns_sem, recv_sem=nr_sem, device_id=(partner,), device_id_type=MESH_ID)
    rest.wait_recv()
    norm_sq = n_get[0]
    for k in range(1, DEVICES):
        norm_sq = norm_sq + n_get[k]
    norm_sq = norm_sq + vec_sq
    scale_buf[0:1, :] = jnp.minimum(1.0, MAX_NORM / (jnp.sqrt(norm_sq) + NORM_EPS))
    lr_load.wait()
    scale_buf[1:2, :] = jnp.full((1, 128), lr_smem[0])
    scale_store = pltpu.make_async_copy(scale_buf, scale_out, so_sem)
    scale_store.start()

    def drain(lo, hi, wait):
        def body(t):
            for color in range(COLORS):
                wait(color, t)
        run(lo, hi, body)

    drain(4 * PARTS - 3, 4 * PARTS, lambda c, t: push1(c, t).wait_send())
    push(r2, r2, s2_sem, r2_sem.at[0], 0).wait_send()
    push(r3, r3, s3_sem, r3_sem.at[0], 0).wait_send()
    pltpu.make_async_remote_copy(
        src_ref=pg, dst_ref=pg, send_sem=ds_sem, recv_sem=dr_sem.at[0],
        device_id=(partner,), device_id_type=MESH_ID).wait_send()
    pltpu.make_async_copy(out, out, o_sem).wait()
    push(v_get, v_get, vs_sem, vr_sem.at[0], 0).wait_send()
    rest.wait_send()
    vec_store.wait()
    scale_store.wait()


def scatter_sum(g_mat, g_vec, learn_rate, axis_name, group_size):
    total = g_mat.shape[1]
    n_vec = g_vec.shape[1]
    piece = total // group_size
    chunk = piece // (COLORS * PARTS)
    dma = pltpu.SemaphoreType.DMA
    any_spec = pl.BlockSpec(memory_space=pl.ANY)
    out, _, vec, scales = pl.pallas_call(
        functools.partial(scatter_kernel, axis_name, piece),
        out_shape=(jax.ShapeDtypeStruct((1, piece), jnp.float32),
                   jax.ShapeDtypeStruct((1, total // 2), jnp.bfloat16),
                   jax.ShapeDtypeStruct((1, n_vec), jnp.float32),
                   jax.ShapeDtypeStruct((2, 128), jnp.float32)),
        in_specs=[any_spec] * 3,
        out_specs=[any_spec] * 4,
        scratch_shapes=[
            pltpu.VMEM((2 * COLORS, 1, chunk), jnp.bfloat16),
            pltpu.VMEM((2 * COLORS, 1, chunk), jnp.bfloat16),
            pltpu.VMEM((COLORS, 1, chunk), jnp.bfloat16),
            pltpu.VMEM((3 * COLORS, 1, chunk), jnp.float32),
            pltpu.VMEM((4 * PARTS * COLORS, 1, chunk), jnp.float32),
            pltpu.VMEM((2 * PARTS * COLORS, 1, chunk), jnp.float32),
            pltpu.VMEM((PARTS * COLORS, 1, chunk), jnp.float32),
            pltpu.VMEM((1, n_vec), jnp.bfloat16),
            pltpu.VMEM((1, n_vec), jnp.float32),
            pltpu.VMEM((4, 1, n_vec // 2), jnp.float32),
            pltpu.VMEM((5, 1, n_vec // 2), jnp.float32),
            pltpu.VMEM((1, n_vec), jnp.float32),
            pltpu.VMEM((1, 128), jnp.float32),
            pltpu.VMEM((DEVICES, 1, 128), jnp.float32),
            pltpu.VMEM((1, min(chunk // CUTS, WIDTH)), jnp.float32),
            pltpu.SMEM((1,), jnp.float32),
            pltpu.VMEM((2, 128), jnp.float32),
            dma((2 * COLORS,)), dma((2 * COLORS,)), dma((COLORS,)),
            dma, dma((SWAPS * COLORS,)), dma((CUTS * COLORS,)),
            dma((3 * COLORS,)), dma((2 * COLORS,)), dma, dma((2 * COLORS,)),
            dma, dma((PARTS * COLORS,)), dma((CUTS * COLORS,)), dma,
            dma, dma, dma((5,)), dma, dma, dma, dma, dma,
        ],
        compiler_params=pltpu.CompilerParams(
            collective_id=0, has_side_effects=True, vmem_limit_bytes=63 * 1024 * 1024),
        name="scatter_sum",
    )(g_mat, g_vec, learn_rate.reshape(1))
    return out, vec, scales


def adam_moments(grad, m, v):
    new_m = ADAM_BETA1 * m + (1.0 - ADAM_BETA1) * grad
    new_v = ADAM_BETA2 * v + (1.0 - ADAM_BETA2) * grad * grad
    return new_m, new_v


def adam_param(p, m, v, rate, decay):
    direction = (m / BIAS_ONE) / (jnp.sqrt(v / BIAS_TWO) + ADAM_EPS)
    return p - rate * (direction + decay * p)


def gather_kernel(axis_name, grad, p, m, v, scales_in, out, m_out, v_out, p_out, g_buf, p_buf, scales,
                  scales_sem, load_sem, s_sem, r_sem, ds_sem, dr_sem):
    own = COLORS * PARTS
    rows = p.shape[1]
    tile = rows // 2
    step = min(tile // 2, ROWS)
    me = lax.axis_index(axis_name)
    deltas = [s * (1 - 2 * lax.rem(me // s, 2)) for s in STRIDES]
    partner = me + 1 - 2 * lax.rem(me, 2)
    peers = [me + d for d in deltas]

    barrier = pltpu.get_barrier_semaphore()
    for dev in (partner, *peers):
        pl.semaphore_signal(barrier, inc=1, device_id=(dev,), device_id_type=MESH_ID)

    def fetch(n):
        q, color, h = n // (2 * COLORS), n // 2 % COLORS, n % 2
        i = color * PARTS + q
        s = pl.ds(h * tile, tile)
        p_dst = p_out.at[i, s] if i < KEEP else p_buf.at[h]
        for src, dst in ((grad, g_buf.at[h]), (m, m_out.at[i, s]), (v, v_out.at[i, s]), (p, p_dst)):
            pltpu.make_async_copy(src.at[i, s], dst, load_sem.at[h]).start()

    def arrived(n):
        pltpu.make_async_copy(m.at[pl.ds(0, 2)], m_out.at[pl.ds(0, 2)], load_sem.at[n % 2]).wait()

    def across(index):
        return pltpu.make_async_remote_copy(
            src_ref=out.at[index], dst_ref=out.at[index], send_sem=ds_sem, recv_sem=dr_sem,
            device_id=(partner,), device_id_type=MESH_ID)

    def route(stage, axis):
        b1, b2 = (axis - 2) % 3, (axis - 1) % 3
        color = (axis, b2, b2, b1, b1, b1, b1)[stage]
        flips = ((), (), (b2,), (), (b1,), (b2,), (b1, b2))[stage]
        return color, sum((deltas[f] for f in flips), me)

    def push(stage, axis, q, span=None):
        color, owner = route(stage, axis)
        index = owner * own + color * PARTS + q
        place = (3 * q, 3 * q + 1, 3 * PARTS + q, 3 * q + 2)[stage] if stage < 4 else stage * PARTS + q
        ref = out.at[index] if span is None else out.at[index, span]
        return pltpu.make_async_remote_copy(
            src_ref=ref, dst_ref=ref, send_sem=s_sem, recv_sem=r_sem.at[axis * PLACES + lax.rem(place, PLACES)],
            device_id=(peers[axis],), device_id_type=MESH_ID)

    def land(stage, axis, q):
        color, owner = route(stage, axis)
        push(stage, axis, q).wait_recv()
        across((owner + deltas[axis]) * own + color * PARTS + q).start()

    def update(color, q, h, first, count):
        i = color * PARTS + q

        @pl.loop(first // step, (first + count) // step)
        def _(r):
            t = pl.ds(pl.multiple_of(r * step, step), step)
            s = pl.ds(pl.multiple_of(h * tile + r * step, step), step)
            new_m, new_v = adam_moments(g_buf[h, t, :] * scales[0:1, :], m_out[i, s, :], v_out[i, s, :])
            m_out[i, s, :] = new_m
            v_out[i, s, :] = new_v
            old_p = p_out[i, s, :] if i < KEEP else p_buf[h, t, :]
            new_p = adam_param(old_p, new_m, new_v, scales[1:2, :], WEIGHT_DECAY)
            if i < KEEP:
                p_out[i, s, :] = new_p
            out[me * own + i, s, :] = new_p.astype(jnp.bfloat16)

    def each(count, body):
        lax.fori_loop(0, count, lambda i, c: (body(i), c)[1], 0)

    scales_load = pltpu.make_async_copy(scales_in, scales, scales_sem)
    scales_load.start()
    fetch(0)
    scales_load.wait()
    fetch(1)
    for n in range(2 * own):
        q, color, h = n // (2 * COLORS), n // 2 % COLORS, n % 2
        cuts = 2 if n < 2 else 1
        arrived(n)
        for c in range(cuts):
            count = tile // cuts
            update(color, q, h, c * count, count)
            if n == 0 and c == 0:
                pl.semaphore_wait(barrier, 4)
            for k, stage in enumerate((0, 1, 3)):
                push(stage, (color + k) % 3, q, pl.ds(h * tile + c * count, count)).start()
        if h:
            across(me * own + color * PARTS + q).start()
        if n + 2 < 2 * own:
            fetch(n + 2)

    def own_stage(q):
        for axis in range(3):
            for stage in (0, 1, 3):
                land(stage, axis, q)
            push(2, (axis + 1) % 3, q).start()

    each(PARTS, own_stage)
    for stage, last in ((4, 2), (5, 4), (6, 5), (None, 6)):
        def body(q, stage=stage, last=last):
            for axis in range(3):
                if stage:
                    push(stage, axis, q).start()
                land(last, axis, q)
        each(PARTS, body)

    sent = out.at[pl.ds(0, 7 * own)]
    pltpu.make_async_remote_copy(
        src_ref=sent, dst_ref=sent, send_sem=s_sem, recv_sem=r_sem.at[0],
        device_id=(partner,), device_id_type=MESH_ID).wait_send()
    half = pltpu.make_async_remote_copy(
        src_ref=out.at[pl.ds(0, 8 * own)], dst_ref=out.at[pl.ds(0, 8 * own)], send_sem=ds_sem, recv_sem=dr_sem,
        device_id=(partner,), device_id_type=MESH_ID)
    half.wait_recv()
    half.wait_send()


def write_kernel(held, m_held, v_held, p_held, p, scales_in, g_vec, p_vec, m_vec, v_vec,
                 out, p_out, m_out, v_out, pv_out, mv_out, vv_out,
                 p_buf, vec_buf, scales, in_sem, out_sem, sem, vec_sem, vec_out_sem, scales_sem):
    own, rows, _ = p.shape
    step = min(rows, ROWS)
    span = held.shape[0] // own

    tiles = own - KEEP

    def load(n):
        return pltpu.make_async_copy(p.at[KEEP + n], p_buf.at[n % RING], in_sem.at[n % RING])

    def store(n):
        return pltpu.make_async_copy(p_buf.at[n % RING], p_out.at[KEEP + n], out_sem.at[n % RING])

    def spread(start, count, i):
        part = pl.ds(start, count)
        return pltpu.make_async_copy(held.at[part], out.at[part], sem.at[0, i % AHEAD])

    def small(i):
        pairs = [(m_held.at[i], m_out.at[i]), (v_held.at[i], v_out.at[i])]
        if i < KEEP:
            pairs.append((p_held.at[i], p_out.at[i]))
        return [pltpu.make_async_copy(src, dst, sem.at[k + 1, i % AHEAD]) for k, (src, dst) in enumerate(pairs)]

    def begin(i):
        for c in range(4):
            spread(i * span + c * (span // 4), span // 4, i).start()
        for copy in small(i):
            copy.start()

    def end(i):
        spread(i * span, span, i).wait()
        for copy in small(i):
            copy.wait()

    scales_load = pltpu.make_async_copy(scales_in, scales, scales_sem)
    scales_load.start()
    vec_loads = [pltpu.make_async_copy(a, vec_buf.at[k], vec_sem.at[k])
                 for k, a in enumerate((p_vec, m_vec, v_vec, g_vec))]
    vec_stores = [pltpu.make_async_copy(vec_buf.at[k], a, vec_out_sem.at[k])
                  for k, a in enumerate((pv_out, mv_out, vv_out))]
    def vec_update():
        for copy in vec_loads:
            copy.wait()

        @pl.loop(0, g_vec.shape[1] // 1024)
        def _(i):
            s = pl.ds(pl.multiple_of(i * 1024, 1024), 1024)
            new_m, new_v = adam_moments(vec_buf[3, :, s] * scales[0:1, 0:1], vec_buf[1, :, s], vec_buf[2, :, s])
            vec_buf[1, :, s] = new_m
            vec_buf[2, :, s] = new_v
            vec_buf[0, :, s] = adam_param(vec_buf[0, :, s], new_m, new_v, scales[1:2, 0:1], 0.0)

        for copy in vec_stores:
            copy.start()

    for n in range(RING - 1):
        load(n).start()
    for copy in vec_loads:
        copy.start()
    for i in range(AHEAD):
        begin(i)
    scales_load.wait()
    for n in range(tiles):
        load(n).wait()
        i = KEEP + n

        @pl.loop(0, rows // step)
        def _(r):
            s = pl.ds(pl.multiple_of(r * step, step), step)
            p_buf[n % RING, s, :] = adam_param(
                p_buf[n % RING, s, :], m_held[i, s, :], v_held[i, s, :], scales[1:2, :], WEIGHT_DECAY)

        store(n).start()
        if n + RING - 1 < tiles:
            if n:
                store(n - 1).wait()
            load(n + RING - 1).start()
        for j in range(n * (own - AHEAD) // tiles, (n + 1) * (own - AHEAD) // tiles):
            end(j)
            begin(j + AHEAD)
        if n == 0:
            vec_update()
    for n in range(tiles - RING, tiles):
        store(n).wait()
    for i in range(own - AHEAD, own):
        end(i)
    for copy in vec_stores:
        copy.wait()


def gather_update(grad, p, m, v, scales, grad_vec, p_vec, m_vec, v_vec, axis_name, group_size):
    own = COLORS * PARTS
    piece = p.shape[0]
    n_vec = p_vec.shape[0]
    rows = piece // (own * 128)
    dma = pltpu.SemaphoreType.DMA
    any_spec = pl.BlockSpec(memory_space=pl.ANY)
    vmem_spec = pl.BlockSpec(memory_space=pltpu.VMEM)
    grad, p, m, v = (a.reshape(own, rows, 128) for a in (grad, p, m, v))
    p_vec, m_vec, v_vec = (a.reshape(1, n_vec) for a in (p_vec, m_vec, v_vec))
    full, new_m, new_v, new_p = pl.pallas_call(
        functools.partial(gather_kernel, axis_name),
        out_shape=(pltpu.VMEM((group_size * own, rows, 128), jnp.bfloat16),
                   pltpu.VMEM((own, rows, 128), jnp.float32),
                   pltpu.VMEM((own, rows, 128), jnp.float32),
                   pltpu.VMEM((KEEP, rows, 128), jnp.float32)),
        in_specs=[any_spec] * 5,
        out_specs=[vmem_spec] * 4,
        scratch_shapes=[
            pltpu.VMEM((2, rows // 2, 128), jnp.float32), pltpu.VMEM((2, rows // 2, 128), jnp.float32),
            pltpu.VMEM((2, 128), jnp.float32), dma, dma((2,)),
            dma, dma((3 * PLACES,)), dma, dma],
        compiler_params=pltpu.CompilerParams(
            collective_id=1, has_side_effects=True, vmem_limit_bytes=SMALL_VMEM),
        name="gather_update",
    )(grad, p, m, v, scales)
    flat = jax.ShapeDtypeStruct((own, rows, 128), jnp.float32)
    line = jax.ShapeDtypeStruct((1, n_vec), jnp.float32)
    full, new_p, new_m, new_v, *vecs = pl.pallas_call(
        write_kernel,
        out_shape=(jax.ShapeDtypeStruct(full.shape, full.dtype), flat, flat, flat, line, line, line),
        in_specs=[vmem_spec] * 4 + [any_spec] * 6,
        out_specs=[any_spec] * 7,
        scratch_shapes=[
            pltpu.VMEM((RING, rows, 128), jnp.float32), pltpu.VMEM((4, 1, n_vec), jnp.float32),
            pltpu.VMEM((2, 128), jnp.float32),
            dma((RING,)), dma((RING,)), dma((4, AHEAD)), dma((4,)), dma((3,)), dma],
        compiler_params=pltpu.CompilerParams(vmem_limit_bytes=SMALL_VMEM),
        name="write_out",
    )(*(pltpu.with_memory_space_constraint(a, pltpu.VMEM) for a in (full, new_m, new_v, new_p)),
      p, scales, grad_vec, p_vec, m_vec, v_vec)
    return (*(a.reshape(piece) for a in (new_p, new_m, new_v)), *(a.reshape(n_vec) for a in vecs),
            full.reshape(group_size * piece))


def solution(mesh):
    axis_name = mesh.axis_names[0]
    group_size = mesh.shape[axis_name]

    def local_step(g_mat, g_vec, p_mat, m_mat, v_mat, p_vec, m_vec, v_vec, learn_rate):
        grad_mat, grad_vec, scales = scatter_sum(g_mat, g_vec, learn_rate, axis_name, group_size)
        return gather_update(grad_mat, p_mat, m_mat, v_mat, scales, grad_vec, p_vec, m_vec, v_vec, axis_name, group_size)

    return jax.shard_map(
        local_step,
        mesh=mesh,
        in_specs=(P(axis_name, None), P(axis_name, None), P(axis_name), P(axis_name), P(axis_name), P(), P(), P(), P()),
        out_specs=(P(axis_name), P(axis_name), P(axis_name), P(), P(), P(), P()),
        check_vma=False,
    )
```

```python
import functools

import jax
import jax.numpy as jnp
from jax import lax
from jax.experimental import pallas as pl
from jax.experimental.pallas import tpu as pltpu
from jax.sharding import PartitionSpec as P

STEP = 10
ADAM_BETA1 = 0.9
ADAM_BETA2 = 0.98
ADAM_EPS = 1e-8
WEIGHT_DECAY = 0.01
MAX_NORM = 1.0
NORM_EPS = 1e-6
BIAS_ONE = 1.0 - ADAM_BETA1 ** STEP
BIAS_TWO = 1.0 - ADAM_BETA2 ** STEP

MESH_ID = pl.DeviceIdType.MESH
COLORS = 3
PARTS = 4
STRIDES = (2, 4, 8)
STEPS = 8 * PARTS
DEVICES = 16
WIDTH = 4096
ROWS = 64
SMALL_VMEM = 2048 * 1024
RING = 3
KEEP = 3
AHEAD = 3
SWAPS = 8
PLACES = 20
CUTS = 4
MEAN_SCALE = 1.0 / 16.0


def scatter_kernel(axis_name, piece, g, gv, lr, out, pg, vec_out, scale_out,
                   a_buf, b_buf, e_buf, stage, r1, r2, r3, v_in, v_full, v_acc, v_get, v_mean, n_put, n_get, squares, lr_smem, scale_buf,
                   a_sem, b_sem, e_sem, ds_sem, dr_sem, dc_sem, s1_sem, r1_sem, s2_sem, r2_sem, s3_sem, r3_sem, rc_sem, o_sem,
                   vi_sem, vs_sem, vr_sem, ns_sem, nr_sem, vo_sem, lr_sem, so_sem):
    chunk = piece // (COLORS * PARTS)
    width = min(chunk // CUTS, WIDTH)
    part = chunk // CUTS
    n_vec = gv.shape[1]
    n_half = n_vec // 2
    me = lax.axis_index(axis_name)
    core = lax.rem(me, 2)
    core_step = 1 - 2 * core
    deltas = [s * (1 - 2 * lax.rem(me // s, 2)) for s in STRIDES]
    partner = me + core_step
    peers = [me + d for d in deltas]

    barrier = pltpu.get_barrier_semaphore()
    for dev in (partner, *peers):
        pl.semaphore_signal(barrier, inc=1, device_id=(dev,), device_id_type=MESH_ID)

    def offset(color, t):
        unit = t // PARTS
        f1 = 1 - unit // 4
        f2 = 1 - lax.rem(unit // 2, 2)
        f3 = 1 - lax.rem(unit, 2)
        d1, d2, d3 = (deltas[(color + k) % 3] for k in range(3))
        owner = me + f1 * d1 + f2 * d2 + f3 * d3
        return owner * piece + (color * PARTS + lax.rem(t, PARTS)) * chunk

    def cut(ref, start):
        return ref.at[:, pl.ds(pl.multiple_of(start, 1024), chunk)]

    def swap(color, t):
        return pltpu.make_async_remote_copy(
            src_ref=cut(g, offset(color, t) + core_step * piece),
            dst_ref=cut(pg, (color * STEPS + t) * chunk),
            send_sem=ds_sem, recv_sem=dr_sem.at[color * SWAPS + lax.rem(t, SWAPS)],
            device_id=(partner,), device_id_type=MESH_ID)

    def swap_early(color, t):
        k = color * 2 + t
        return pltpu.make_async_remote_copy(
            src_ref=cut(g, offset(color, t) + core_step * piece), dst_ref=b_buf.at[k],
            send_sem=ds_sem, recv_sem=dr_sem.at[color * SWAPS + t],
            device_id=(partner,), device_id_type=MESH_ID)

    def swap_cut(color, i):
        s = pl.ds(i * part, part)
        return pltpu.make_async_remote_copy(
            src_ref=e_buf.at[color, :, s], dst_ref=b_buf.at[color * 2, :, s],
            send_sem=ds_sem, recv_sem=dc_sem.at[color * CUTS + i],
            device_id=(partner,), device_id_type=MESH_ID)

    def load_e(color):
        return pltpu.make_async_copy(
            cut(g, offset(color, 0) + core_step * piece), e_buf.at[color], e_sem.at[color])

    def push_cut(color, i):
        k, j = color * 3, color * 4 * PARTS
        s = pl.ds(i * part, part)
        return push(stage.at[k, :, s], r1.at[j, :, s], s1_sem.at[k], r1_sem.at[color * 2], color)

    def load_a(color, t):
        k = color * 2 + lax.rem(t, 2)
        return pltpu.make_async_copy(cut(g, offset(color, t)), a_buf.at[k], a_sem.at[k])

    def load_b(color, t):
        k = color * 2 + lax.rem(t, 2)
        return pltpu.make_async_copy(cut(pg, (color * STEPS + t) * chunk), b_buf.at[k], b_sem.at[k])

    def push(src, dst, send_sem, recv_sem, axis):
        return pltpu.make_async_remote_copy(
            src_ref=src, dst_ref=dst, send_sem=send_sem, recv_sem=recv_sem,
            device_id=(peers[axis],), device_id_type=MESH_ID)

    def push1(color, t):
        k = color * 3 + lax.rem(t, 3)
        j = color * 4 * PARTS + t
        return push(stage.at[k], r1.at[j], s1_sem.at[k], r1_sem.at[color * 2 + t // (2 * PARTS)], color)

    def push2(color, t):
        j = color * 2 * PARTS + t - 4 * PARTS
        return push(r1.at[color * 4 * PARTS + t - 4 * PARTS], r2.at[j], s2_sem,
                    r2_sem.at[color * 2 + t // PARTS - 4], (color + 1) % 3)

    def push3(color, t):
        j = color * PARTS + t - 6 * PARTS
        return push(r1.at[color * 4 * PARTS + t - 4 * PARTS], r3.at[j], s3_sem, r3_sem.at[j], (color + 2) % 3)

    def push3_cut(color, i):
        s = pl.ds(i * part, part)
        return push(r1.at[color * 4 * PARTS + 3 * PARTS - 1, :, s], r3.at[color * PARTS + PARTS - 1, :, s],
                    s3_sem, rc_sem.at[color * CUTS + i], (color + 2) % 3)

    def unit1(color, pair):
        span = r1.at[pl.ds((color * 2 + pair) * 2 * PARTS, 2 * PARTS)]
        return push(span, span, s2_sem, r1_sem.at[color * 2 + pair], color)

    def unit2(color, w):
        span = r2.at[pl.ds((color * 2 + w) * PARTS, PARTS)]
        return push(span, span, s2_sem, r2_sem.at[color * 2 + w], (color + 1) % 3)

    def store(color, t):
        j = color * PARTS + t - 7 * PARTS
        return pltpu.make_async_copy(r3.at[j], cut(out, j * chunk), o_sem)

    def add_up(color, t, dst, extra, last=False, span=None):
        k = color * 2 + lax.rem(t, 2)
        first, count = span or (0, chunk)

        @pl.loop(first // width, (first + count) // width)
        def _(i):
            s = pl.ds(pl.multiple_of(i * width, width), width)
            acc = a_buf[k, :, s].astype(jnp.float32) + b_buf[k, :, s].astype(jnp.float32)
            for ref, j in extra:
                acc = acc + ref[j, :, s]
            if last:
                acc = acc * MEAN_SCALE
                squares[...] += acc * acc
            dst[0][dst[1], :, s] = acc

    def half(ref, which):
        return ref.at[:, pl.ds(pl.multiple_of(which * n_half, 1024), n_half)]

    def vec_push(k):
        src = half(v_full, 1 - core) if k == 0 else half(v_mean, core) if k == 4 else v_acc.at[k]
        return pltpu.make_async_remote_copy(
            src_ref=src, dst_ref=half(v_mean, core) if k == 4 else v_get.at[k],
            send_sem=vs_sem, recv_sem=vr_sem.at[k],
            device_id=((partner, *peers, partner)[k],), device_id_type=MESH_ID)

    def norm_push(k):
        return pltpu.make_async_remote_copy(
            src_ref=n_put, dst_ref=n_get.at[me], send_sem=ns_sem, recv_sem=nr_sem,
            device_id=(lax.rem(me + k, DEVICES),), device_id_type=MESH_ID)

    def vec_loop(count, body):
        @pl.loop(0, count // 1024)
        def _(i):
            body(pl.multiple_of(i * 1024, 1024))

    def vec_turn(k):
        def body(i):
            s = pl.ds(i, 1024)
            here = pl.ds(pl.multiple_of(core * n_half + i, 1024), 1024)
            total = (v_acc[k, :, s] if k else v_full[:, here]) + v_get[k, :, s]
            if k < 3:
                v_acc[k + 1, :, s] = total
            else:
                v_mean[:, here] = total * MEAN_SCALE
        vec_push(k).wait_recv()
        vec_loop(n_half, body)
        vec_push(k + 1).start()

    def ready(color, t):
        load_a(color, t).wait()
        load_b(color, t).wait()

    def refill(color, t):
        load_a(color, t).start()
        swap(color, t).wait_recv()
        load_b(color, t).start()

    def more_swap(color, t):
        swap(color, t).start()

    for color in range(COLORS):
        load_e(color).start()
    for t in range(2):
        for color in range(COLORS):
            load_a(color, t).start()
    vec_load = pltpu.make_async_copy(gv, v_in, vi_sem)
    vec_load.start()
    lr_load = pltpu.make_async_copy(lr, lr_smem, lr_sem)
    lr_load.start()
    squares[...] = jnp.zeros_like(squares)
    for color in range(COLORS):
        load_e(color).wait()
    pl.semaphore_wait(barrier, 4)
    for i in range(CUTS):
        for color in range(COLORS):
            swap_cut(color, i).start()
    for color in range(COLORS):
        swap_early(color, 1).start()
    for t in range(2, 4):
        for color in range(COLORS):
            swap(color, t).start()
    for i in range(CUTS):
        for color in range(COLORS):
            if i == 0:
                load_a(color, 0).wait()
            swap_cut(color, i).wait_recv()
            add_up(color, 0, (stage, color * 3), (), span=(i * part, part))
            push_cut(color, i).start()
    for color in range(COLORS):
        more_swap(color, 4)
        refill(color, 2)

    def phase_one(t, first, early=False):
        for color in range(COLORS):
            if early:
                load_a(color, t).wait()
                swap_early(color, t).wait_recv()
            else:
                ready(color, t)
            if not first:
                push1(color, t - 3).wait_send()
            add_up(color, t, (stage, color * 3 + lax.rem(t, 3)), ())
            push1(color, t).start()
            more_swap(color, t + 4)
            refill(color, t + 2)

    def run(lo, hi, body):
        lax.fori_loop(lo, hi, lambda t, c: (body(t), c)[1], 0)

    phase_one(1, True, True)
    phase_one(2, True)
    vec_load.wait()

    def widen(i):
        s = pl.ds(i, 1024)
        v_full[:, s] = v_in[:, s].astype(jnp.float32)

    vec_loop(n_vec, widen)
    vec_push(0).start()
    for k in range(4):
        run(3 * k + 3, 3 * k + 6, lambda t: phase_one(t, False))
        vec_turn(k)
    run(15, 4 * PARTS, lambda t: phase_one(t, False))
    vec_push(4).wait_recv()
    vec_store = pltpu.make_async_copy(v_mean, vec_out, vo_sem)
    vec_store.start()

    def phase_two(t):
        for color in range(COLORS):
            ready(color, t)
            j = color * 4 * PARTS + t - 4 * PARTS
            add_up(color, t, (r1, j), ((r1, j),))
            push2(color, t).start()
            more_swap(color, t + 4)
            refill(color, t + 2)

    def phase_three(t, cuts):
        for color in range(COLORS):
            ready(color, t)
            j = color * 4 * PARTS + t - 4 * PARTS
            add_up(color, t, (r1, j), ((r1, j), (r2, color * 2 * PARTS + t - 6 * PARTS)))
            if cuts:
                for i in range(CUTS):
                    push3_cut(color, i).start()
            else:
                push3(color, t).start()
            more_swap(color, t + 4)
            refill(color, t + 2)

    def finish(color, t, span=None):
        j = color * PARTS + t - 7 * PARTS
        add_up(color, t, (r3, j), (
            (r1, color * 4 * PARTS + t - 4 * PARTS),
            (r2, color * 2 * PARTS + t - 6 * PARTS),
            (r3, j)), last=True, span=span)

    def phase_four(t, fill):
        for color in range(COLORS):
            ready(color, t)
            push3(color, t - PARTS).wait_recv()
            finish(color, t)
            store(color, t).start()
            if fill:
                refill(color, t + 2)

    for unit in range(4, 8):
        for color in range(COLORS):
            if unit in (4, 6):
                unit1(color, (unit - 4) // 2).wait_recv()
            if unit >= 6:
                unit2(color, unit - 6).wait_recv()
        lo = unit * PARTS
        if unit < 6:
            run(lo, lo + PARTS, phase_two)
        elif unit == 6:
            run(lo, lo + PARTS - 1, lambda t: phase_three(t, False))
            phase_three(lo + PARTS - 1, True)
        else:
            run(lo, lo + PARTS - 2, lambda t: phase_four(t, True))
            phase_four(lo + PARTS - 2, False)
    for color in range(COLORS):
        ready(color, STEPS - 1)
    for i in range(CUTS):
        for color in range(COLORS):
            push3_cut(color, i).wait_recv()
            finish(color, STEPS - 1, span=(i * part, part))
    for color in range(COLORS):
        store(color, STEPS - 1).start()

    vec_sq = jnp.sum(v_mean[...] * v_mean[...], axis=1, keepdims=True)
    mine = jnp.broadcast_to(jnp.sum(squares[...], axis=1, keepdims=True), (1, 128))
    n_put[...] = mine
    n_get[me] = mine
    for k in range(1, DEVICES):
        norm_push(k).start()
    rest = pltpu.make_async_remote_copy(
        src_ref=n_get.at[pl.ds(0, DEVICES - 1)], dst_ref=n_get.at[pl.ds(0, DEVICES - 1)],
        send_sem=ns_sem, recv_sem=nr_sem, device_id=(partner,), device_id_type=MESH_ID)
    rest.wait_recv()
    norm_sq = n_get[0]
    for k in range(1, DEVICES):
        norm_sq = norm_sq + n_get[k]
    norm_sq = norm_sq + vec_sq
    scale_buf[0:1, :] = jnp.minimum(1.0, MAX_NORM / (jnp.sqrt(norm_sq) + NORM_EPS))
    lr_load.wait()
    scale_buf[1:2, :] = jnp.full((1, 128), lr_smem[0])
    scale_store = pltpu.make_async_copy(scale_buf, scale_out, so_sem)
    scale_store.start()

    def drain(lo, hi, wait):
        def body(t):
            for color in range(COLORS):
                wait(color, t)
        run(lo, hi, body)

    drain(4 * PARTS - 3, 4 * PARTS, lambda c, t: push1(c, t).wait_send())
    push(r2, r2, s2_sem, r2_sem.at[0], 0).wait_send()
    push(r3, r3, s3_sem, r3_sem.at[0], 0).wait_send()
    pltpu.make_async_remote_copy(
        src_ref=pg, dst_ref=pg, send_sem=ds_sem, recv_sem=dr_sem.at[0],
        device_id=(partner,), device_id_type=MESH_ID).wait_send()
    pltpu.make_async_copy(out, out, o_sem).wait()
    push(v_get, v_get, vs_sem, vr_sem.at[0], 0).wait_send()
    rest.wait_send()
    vec_store.wait()
    scale_store.wait()


def scatter_sum(g_mat, g_vec, learn_rate, axis_name, group_size):
    total = g_mat.shape[1]
    n_vec = g_vec.shape[1]
    piece = total // group_size
    chunk = piece // (COLORS * PARTS)
    dma = pltpu.SemaphoreType.DMA
    any_spec = pl.BlockSpec(memory_space=pl.ANY)
    out, _, vec, scales = pl.pallas_call(
        functools.partial(scatter_kernel, axis_name, piece),
        out_shape=(jax.ShapeDtypeStruct((1, piece), jnp.float32),
                   jax.ShapeDtypeStruct((1, total // 2), jnp.bfloat16),
                   jax.ShapeDtypeStruct((1, n_vec), jnp.float32),
                   jax.ShapeDtypeStruct((2, 128), jnp.float32)),
        in_specs=[any_spec] * 3,
        out_specs=[any_spec] * 4,
        scratch_shapes=[
            pltpu.VMEM((2 * COLORS, 1, chunk), jnp.bfloat16),
            pltpu.VMEM((2 * COLORS, 1, chunk), jnp.bfloat16),
            pltpu.VMEM((COLORS, 1, chunk), jnp.bfloat16),
            pltpu.VMEM((3 * COLORS, 1, chunk), jnp.float32),
            pltpu.VMEM((4 * PARTS * COLORS, 1, chunk), jnp.float32),
            pltpu.VMEM((2 * PARTS * COLORS, 1, chunk), jnp.float32),
            pltpu.VMEM((PARTS * COLORS, 1, chunk), jnp.float32),
            pltpu.VMEM((1, n_vec), jnp.bfloat16),
            pltpu.VMEM((1, n_vec), jnp.float32),
            pltpu.VMEM((4, 1, n_vec // 2), jnp.float32),
            pltpu.VMEM((5, 1, n_vec // 2), jnp.float32),
            pltpu.VMEM((1, n_vec), jnp.float32),
            pltpu.VMEM((1, 128), jnp.float32),
            pltpu.VMEM((DEVICES, 1, 128), jnp.float32),
            pltpu.VMEM((1, min(chunk // CUTS, WIDTH)), jnp.float32),
            pltpu.SMEM((1,), jnp.float32),
            pltpu.VMEM((2, 128), jnp.float32),
            dma((2 * COLORS,)), dma((2 * COLORS,)), dma((COLORS,)),
            dma, dma((SWAPS * COLORS,)), dma((CUTS * COLORS,)),
            dma((3 * COLORS,)), dma((2 * COLORS,)), dma, dma((2 * COLORS,)),
            dma, dma((PARTS * COLORS,)), dma((CUTS * COLORS,)), dma,
            dma, dma, dma((5,)), dma, dma, dma, dma, dma,
        ],
        compiler_params=pltpu.CompilerParams(
            collective_id=0, has_side_effects=True, vmem_limit_bytes=63 * 1024 * 1024),
        name="scatter_sum",
    )(g_mat, g_vec, learn_rate.reshape(1))
    return out, vec, scales


def adam_moments(grad, m, v):
    new_m = ADAM_BETA1 * m + (1.0 - ADAM_BETA1) * grad
    new_v = ADAM_BETA2 * v + (1.0 - ADAM_BETA2) * grad * grad
    return new_m, new_v


def adam_param(p, m, v, rate, decay):
    direction = (m / BIAS_ONE) / (jnp.sqrt(v / BIAS_TWO) + ADAM_EPS)
    return p - rate * (direction + decay * p)


def gather_kernel(axis_name, grad, p, m, v, scales_in, out, m_out, v_out, p_out, g_buf, p_buf, scales,
                  scales_sem, load_sem, s_sem, r_sem, t_sem, ds_sem, dr_sem):
    own = COLORS * PARTS
    rows = p.shape[1]
    tile = rows // 2
    step = min(tile // 2, ROWS)
    me = lax.axis_index(axis_name)
    deltas = [s * (1 - 2 * lax.rem(me // s, 2)) for s in STRIDES]
    partner = me + 1 - 2 * lax.rem(me, 2)
    peers = [me + d for d in deltas]

    barrier = pltpu.get_barrier_semaphore()
    for dev in (partner, *peers):
        pl.semaphore_signal(barrier, inc=1, device_id=(dev,), device_id_type=MESH_ID)

    def fetch(n):
        q, color, h = n // (2 * COLORS), n // 2 % COLORS, n % 2
        i = color * PARTS + q
        s = pl.ds(h * tile, tile)
        p_dst = p_out.at[i, s] if i < KEEP else p_buf.at[h]
        for src, dst in ((grad, g_buf.at[h]), (m, m_out.at[i, s]), (v, v_out.at[i, s]), (p, p_dst)):
            pltpu.make_async_copy(src.at[i, s], dst, load_sem.at[h]).start()

    def arrived(n):
        pltpu.make_async_copy(m.at[pl.ds(0, 2)], m_out.at[pl.ds(0, 2)], load_sem.at[n % 2]).wait()

    def across(index, span=None):
        ref = out.at[index] if span is None else out.at[index, span]
        return pltpu.make_async_remote_copy(
            src_ref=ref, dst_ref=ref, send_sem=ds_sem, recv_sem=dr_sem,
            device_id=(partner,), device_id_type=MESH_ID)

    def route(stage, axis):
        b1, b2 = (axis - 2) % 3, (axis - 1) % 3
        color = (axis, b2, b2, b1, b1, b1, b1)[stage]
        flips = ((), (), (b2,), (), (b1,), (b2,), (b1, b2))[stage]
        return color, sum((deltas[f] for f in flips), me)

    def push(stage, axis, q, span=None):
        color, owner = route(stage, axis)
        index = owner * own + color * PARTS + q
        place = (3 * q, 3 * q + 1, 3 * PARTS + q, 3 * q + 2)[stage] if stage < 4 else stage * PARTS + q
        ref = out.at[index] if span is None else out.at[index, span]
        return pltpu.make_async_remote_copy(
            src_ref=ref, dst_ref=ref, send_sem=s_sem, recv_sem=r_sem.at[axis * PLACES + lax.rem(place, PLACES)],
            device_id=(peers[axis],), device_id_type=MESH_ID)

    def tail(axis, c):
        color, owner = route(6, axis)
        index = color * PARTS + PARTS - 1
        span = pl.ds(c * (rows // CUTS), rows // CUTS)
        ref = out.at[owner * own + index, span]
        copy = pltpu.make_async_remote_copy(
            src_ref=ref, dst_ref=ref, send_sem=s_sem, recv_sem=t_sem.at[axis * CUTS + c],
            device_id=(peers[axis],), device_id_type=MESH_ID)
        return copy, across((owner + deltas[axis]) * own + index, span)

    def land(stage, axis, q):
        color, owner = route(stage, axis)
        push(stage, axis, q).wait_recv()
        across((owner + deltas[axis]) * own + color * PARTS + q).start()

    def update(color, q, h, first, count):
        i = color * PARTS + q

        @pl.loop(first // step, (first + count) // step)
        def _(r):
            t = pl.ds(pl.multiple_of(r * step, step), step)
            s = pl.ds(pl.multiple_of(h * tile + r * step, step), step)
            new_m, new_v = adam_moments(g_buf[h, t, :] * scales[0:1, :], m_out[i, s, :], v_out[i, s, :])
            m_out[i, s, :] = new_m
            v_out[i, s, :] = new_v
            old_p = p_out[i, s, :] if i < KEEP else p_buf[h, t, :]
            new_p = adam_param(old_p, new_m, new_v, scales[1:2, :], WEIGHT_DECAY)
            if i < KEEP:
                p_out[i, s, :] = new_p
            out[me * own + i, s, :] = new_p.astype(jnp.bfloat16)

    def each(count, body):
        lax.fori_loop(0, count, lambda i, c: (body(i), c)[1], 0)

    scales_load = pltpu.make_async_copy(scales_in, scales, scales_sem)
    scales_load.start()
    fetch(0)
    scales_load.wait()
    fetch(1)
    for n in range(2 * own):
        q, color, h = n // (2 * COLORS), n // 2 % COLORS, n % 2
        cuts = 2 if n < 2 else 1
        arrived(n)
        for c in range(cuts):
            count = tile // cuts
            update(color, q, h, c * count, count)
            if n == 0 and c == 0:
                pl.semaphore_wait(barrier, 4)
            for k, stage in enumerate((0, 1, 3)):
                push(stage, (color + k) % 3, q, pl.ds(h * tile + c * count, count)).start()
        if h:
            across(me * own + color * PARTS + q).start()
        if n + 2 < 2 * own:
            fetch(n + 2)

    def own_stage(q):
        for axis in range(3):
            for stage in (0, 1, 3):
                land(stage, axis, q)
            push(2, (axis + 1) % 3, q).start()

    each(PARTS, own_stage)
    for stage, last, count in ((4, 2, PARTS), (5, 4, PARTS), (6, 5, PARTS - 1)):
        def body(q, stage=stage, last=last):
            for axis in range(3):
                push(stage, axis, q).start()
                land(last, axis, q)
        each(count, body)
    tails = [tail(axis, c) for c in range(CUTS) for axis in range(3)]
    for copy, _ in tails:
        copy.start()
    for axis in range(3):
        land(5, axis, PARTS - 1)

    def last_stage(q):
        for axis in range(3):
            land(6, axis, q)

    each(PARTS - 1, last_stage)
    for copy, onward in tails:
        copy.wait_recv()
        onward.start()

    sent = out.at[pl.ds(0, 7 * own)]
    pltpu.make_async_remote_copy(
        src_ref=sent, dst_ref=sent, send_sem=s_sem, recv_sem=r_sem.at[0],
        device_id=(partner,), device_id_type=MESH_ID).wait_send()
    half = pltpu.make_async_remote_copy(
        src_ref=out.at[pl.ds(0, 8 * own)], dst_ref=out.at[pl.ds(0, 8 * own)], send_sem=ds_sem, recv_sem=dr_sem,
        device_id=(partner,), device_id_type=MESH_ID)
    half.wait_recv()
    half.wait_send()


def write_kernel(held, m_held, v_held, p_held, p, scales_in, g_vec, p_vec, m_vec, v_vec,
                 out, p_out, m_out, v_out, pv_out, mv_out, vv_out,
                 p_buf, vec_buf, scales, in_sem, out_sem, sem, vec_sem, vec_out_sem, scales_sem):
    own, rows, _ = p.shape
    step = min(rows, ROWS)
    span = held.shape[0] // own

    tiles = own - KEEP

    def load(n):
        return pltpu.make_async_copy(p.at[KEEP + n], p_buf.at[n % RING], in_sem.at[n % RING])

    def store(n):
        return pltpu.make_async_copy(p_buf.at[n % RING], p_out.at[KEEP + n], out_sem.at[n % RING])

    def spread(start, count, i):
        part = pl.ds(start, count)
        return pltpu.make_async_copy(held.at[part], out.at[part], sem.at[0, i % AHEAD])

    def small(i):
        pairs = [(m_held.at[i], m_out.at[i]), (v_held.at[i], v_out.at[i])]
        if i < KEEP:
            pairs.append((p_held.at[i], p_out.at[i]))
        return [pltpu.make_async_copy(src, dst, sem.at[k + 1, i % AHEAD]) for k, (src, dst) in enumerate(pairs)]

    def begin(i):
        for c in range(4):
            spread(i * span + c * (span // 4), span // 4, i).start()
        for copy in small(i):
            copy.start()

    def end(i):
        spread(i * span, span, i).wait()
        for copy in small(i):
            copy.wait()

    scales_load = pltpu.make_async_copy(scales_in, scales, scales_sem)
    scales_load.start()
    vec_loads = [pltpu.make_async_copy(a, vec_buf.at[k], vec_sem.at[k])
                 for k, a in enumerate((p_vec, m_vec, v_vec, g_vec))]
    vec_stores = [pltpu.make_async_copy(vec_buf.at[k], a, vec_out_sem.at[k])
                  for k, a in enumerate((pv_out, mv_out, vv_out))]
    def vec_update():
        for copy in vec_loads:
            copy.wait()

        @pl.loop(0, g_vec.shape[1] // 1024)
        def _(i):
            s = pl.ds(pl.multiple_of(i * 1024, 1024), 1024)
            new_m, new_v = adam_moments(vec_buf[3, :, s] * scales[0:1, 0:1], vec_buf[1, :, s], vec_buf[2, :, s])
            vec_buf[1, :, s] = new_m
            vec_buf[2, :, s] = new_v
            vec_buf[0, :, s] = adam_param(vec_buf[0, :, s], new_m, new_v, scales[1:2, 0:1], 0.0)

        for copy in vec_stores:
            copy.start()

    for n in range(RING - 1):
        load(n).start()
    for copy in vec_loads:
        copy.start()
    for i in range(AHEAD):
        begin(i)
    scales_load.wait()
    for n in range(tiles):
        load(n).wait()
        i = KEEP + n

        @pl.loop(0, rows // step)
        def _(r):
            s = pl.ds(pl.multiple_of(r * step, step), step)
            p_buf[n % RING, s, :] = adam_param(
                p_buf[n % RING, s, :], m_held[i, s, :], v_held[i, s, :], scales[1:2, :], WEIGHT_DECAY)

        store(n).start()
        if n + RING - 1 < tiles:
            if n:
                store(n - 1).wait()
            load(n + RING - 1).start()
        for j in range(n * (own - AHEAD) // tiles, (n + 1) * (own - AHEAD) // tiles):
            end(j)
            begin(j + AHEAD)
        if n == 0:
            vec_update()
    for n in range(tiles - RING, tiles):
        store(n).wait()
    for i in range(own - AHEAD, own):
        end(i)
    for copy in vec_stores:
        copy.wait()


def gather_update(grad, p, m, v, scales, grad_vec, p_vec, m_vec, v_vec, axis_name, group_size):
    own = COLORS * PARTS
    piece = p.shape[0]
    n_vec = p_vec.shape[0]
    rows = piece // (own * 128)
    dma = pltpu.SemaphoreType.DMA
    any_spec = pl.BlockSpec(memory_space=pl.ANY)
    vmem_spec = pl.BlockSpec(memory_space=pltpu.VMEM)
    grad, p, m, v = (a.reshape(own, rows, 128) for a in (grad, p, m, v))
    p_vec, m_vec, v_vec = (a.reshape(1, n_vec) for a in (p_vec, m_vec, v_vec))
    full, new_m, new_v, new_p = pl.pallas_call(
        functools.partial(gather_kernel, axis_name),
        out_shape=(pltpu.VMEM((group_size * own, rows, 128), jnp.bfloat16),
                   pltpu.VMEM((own, rows, 128), jnp.float32),
                   pltpu.VMEM((own, rows, 128), jnp.float32),
                   pltpu.VMEM((KEEP, rows, 128), jnp.float32)),
        in_specs=[any_spec] * 5,
        out_specs=[vmem_spec] * 4,
        scratch_shapes=[
            pltpu.VMEM((2, rows // 2, 128), jnp.float32), pltpu.VMEM((2, rows // 2, 128), jnp.float32),
            pltpu.VMEM((2, 128), jnp.float32), dma, dma((2,)),
            dma, dma((3 * PLACES,)), dma((3 * CUTS,)), dma, dma],
        compiler_params=pltpu.CompilerParams(
            collective_id=1, has_side_effects=True, vmem_limit_bytes=SMALL_VMEM),
        name="gather_update",
    )(grad, p, m, v, scales)
    flat = jax.ShapeDtypeStruct((own, rows, 128), jnp.float32)
    line = jax.ShapeDtypeStruct((1, n_vec), jnp.float32)
    full, new_p, new_m, new_v, *vecs = pl.pallas_call(
        write_kernel,
        out_shape=(jax.ShapeDtypeStruct(full.shape, full.dtype), flat, flat, flat, line, line, line),
        in_specs=[vmem_spec] * 4 + [any_spec] * 6,
        out_specs=[any_spec] * 7,
        scratch_shapes=[
            pltpu.VMEM((RING, rows, 128), jnp.float32), pltpu.VMEM((4, 1, n_vec), jnp.float32),
            pltpu.VMEM((2, 128), jnp.float32),
            dma((RING,)), dma((RING,)), dma((4, AHEAD)), dma((4,)), dma((3,)), dma],
        compiler_params=pltpu.CompilerParams(vmem_limit_bytes=SMALL_VMEM),
        name="write_out",
    )(*(pltpu.with_memory_space_constraint(a, pltpu.VMEM) for a in (full, new_m, new_v, new_p)),
      p, scales, grad_vec, p_vec, m_vec, v_vec)
    return (*(a.reshape(piece) for a in (new_p, new_m, new_v)), *(a.reshape(n_vec) for a in vecs),
            full.reshape(group_size * piece))


def solution(mesh):
    axis_name = mesh.axis_names[0]
    group_size = mesh.shape[axis_name]

    def local_step(g_mat, g_vec, p_mat, m_mat, v_mat, p_vec, m_vec, v_vec, learn_rate):
        grad_mat, grad_vec, scales = scatter_sum(g_mat, g_vec, learn_rate, axis_name, group_size)
        return gather_update(grad_mat, p_mat, m_mat, v_mat, scales, grad_vec, p_vec, m_vec, v_vec, axis_name, group_size)

    return jax.shard_map(
        local_step,
        mesh=mesh,
        in_specs=(P(axis_name, None), P(axis_name, None), P(axis_name), P(axis_name), P(axis_name), P(), P(), P(), P()),
        out_specs=(P(axis_name), P(axis_name), P(axis_name), P(), P(), P(), P()),
        check_vma=False,
    )
```
